32 devices in a mesh: frag: 4 (over x, y), dev: 8 (over z, core).
Axes of the slice: x: 2, y: 2, z: 4, core: 2. Of those that a mesh axis runs over, the one named last changes fastest.
Arguments:
- ao_ints: bfloat16 [256, 64, 64, 64], P(('frag', 'dev')), parts along dimension 0
- coeffs: bfloat16 [256, 64], P('frag'), parts along dimension 0
Outputs:
- output: float32 [256, 64, 4096], P('frag', None, 'dev'), parts along dimension 0
There are 4 independent parts. The reference program is written for one: setup_inputs(seed, part) draws one part's arguments, and reference() takes and returns one part's arrays. A program takes and returns all parts, laid end to end along the dimension named above; each array names one.
All inputs are finite; a program needn't handle non-finite values.
Results may differ from the reference program's by a relative error of at most 0.001.
Values are sent between devices in bfloat16 or wider.
A program may use at most 1 GiB of HBM per device.

```python
import jax
import jax.numpy as jnp
from jax import lax

NBASIS = 64


def setup_inputs(seed: int = 0, part: int = 0) -> dict:
    part_key = jax.random.fold_in(jax.random.key(seed), part)
    key_ints, key_coef = jax.random.split(part_key)
    ao_ints = jax.random.normal(key_ints, (NBASIS, NBASIS, NBASIS, NBASIS), jnp.float32).astype(jnp.bfloat16)
    coeffs = (jax.random.normal(key_coef, (NBASIS, NBASIS), jnp.float32) * NBASIS ** -0.5).astype(jnp.bfloat16)
    return {"ao_ints": ao_ints, "coeffs": coeffs}


def reference(ao_ints, coeffs):
    n_basis = coeffs.shape[0]
    coeffs_t = coeffs.T

    def row_transform(a_row):
        a_qsr = jnp.transpose(a_row, (0, 2, 1)).reshape(n_basis * n_basis, n_basis)
        t_one = jnp.dot(a_qsr, coeffs, preferred_element_type=jnp.float32).astype(jnp.bfloat16)
        t_qjs = jnp.transpose(t_one.reshape(n_basis, n_basis, n_basis), (0, 2, 1)).reshape(n_basis * n_basis, n_basis)
        h_row = jnp.dot(t_qjs, coeffs, preferred_element_type=jnp.float32).astype(jnp.bfloat16)
        return jnp.dot(coeffs_t, h_row.reshape(n_basis, n_basis * n_basis), preferred_element_type=jnp.float32).astype(jnp.bfloat16)

    g_all = lax.map(row_transform, ao_ints)
    mo_ints = jnp.dot(coeffs_t, g_all.reshape(n_basis, n_basis ** 3), preferred_element_type=jnp.float32)
    return mo_ints.reshape(n_basis, n_basis, n_basis * n_basis)
```

```python
import functools

import jax
import jax.numpy as jnp
from jax import lax
from jax.experimental import pallas as pl
from jax.experimental.pallas import tpu as pltpu
from jax.sharding import PartitionSpec as P

N = 64
DEV = 8
ROWS = N // DEV
COLS = N * N // DEV
BF16 = jnp.bfloat16
F32 = jnp.float32


def iota(shape, dim):
    return lax.broadcasted_iota(jnp.int32, shape, dim)


def exchange_kernel(a_hbm, c_hbm, g_ref, l4_ref, a_vm, c_vm, l_vm, b4_vm, ct_vm, send, recv, a_sem, c_sem, send_sem, recv_sem):
    me = lax.axis_index("dev")
    chip = me // 2
    core = me % 2

    load_c = pltpu.make_async_copy(c_hbm, c_vm, c_sem)
    load_c.start()

    def load_row(p):
        return pltpu.make_async_copy(a_hbm.at[p], a_vm.at[p], a_sem.at[p])

    for p in range(ROWS):
        load_row(p).start()

    barrier = pltpu.get_barrier_semaphore()
    for k in range(1, DEV):
        pl.semaphore_signal(barrier, inc=1, device_id={"dev": (me + k) % DEV}, device_id_type=pl.DeviceIdType.MESH)

    load_c.wait()
    c = c_vm[...]
    spread = (iota((8 * N, N), 0) // 8 == iota((8 * N, N), 1)).astype(BF16)
    nt = (((1,), (1,)), ((), ()))
    rows = lax.dot_general(spread, c, nt, preferred_element_type=F32)
    wide = (8 * N, 8 * N)
    pair = jnp.concatenate([rows, rows], axis=1)
    tiled = jnp.concatenate([pair] * 4, axis=1)
    l_vm[...] = jnp.where(iota(wide, 0) % 8 == iota(wide, 1) // N, tiled, 0.0).astype(BF16)
    widen = (iota((N, 8 * N), 0) == iota((N, 8 * N), 1) // 8).astype(BF16)
    full = jnp.dot(rows.astype(BF16), widen, preferred_element_type=F32)
    l4_ref[...] = jnp.where(iota(wide, 0) % 8 == iota(wide, 1) % 8, full, 0.0).astype(BF16)
    cf = c.astype(F32)
    cpair = jnp.concatenate([cf, cf], axis=1)
    c4 = jnp.concatenate([cpair, cpair], axis=1)
    c44 = jnp.concatenate([c4] * 4, axis=0)
    quad = (4 * N, 4 * N)
    b4_vm[...] = jnp.where(iota(quad, 0) // N == iota(quad, 1) // N, c44, 0.0).astype(BF16)
    eye = (iota((N, N), 0) == iota((N, N), 1)).astype(BF16)
    ct_vm[...] = lax.dot_general(eye, c, nt, preferred_element_type=F32).astype(BF16)

    pl.semaphore_wait(barrier, DEV - 1)

    def block(p, dest):
        return pltpu.make_async_remote_copy(
            src_ref=send.at[dest, p],
            dst_ref=recv.at[me, p],
            send_sem=send_sem.at[dest, p],
            recv_sem=recv_sem.at[me, p],
            device_id={"dev": dest},
            device_id_type=pl.DeviceIdType.MESH,
        )

    low = iota((32, 8, 128), 2) < N

    def half_row(p, h):
        a = a_vm[p, pl.ds(32 * h, 32)].reshape(4, 8 * N, N)
        left = jnp.concatenate([a[0], a[1]], axis=1)
        right = jnp.concatenate([a[2], a[3]], axis=1)
        a4 = jnp.concatenate([left, right], axis=1)
        t_one = jnp.dot(l_vm[...], a4, preferred_element_type=F32).astype(BF16)
        half = jnp.dot(t_one, b4_vm[...], preferred_element_type=F32)
        pairs = half.reshape(32, 2, 8, 256)
        for t in range(2):
            even = pairs[:, 0, :, 128 * t:128 * t + 128]
            odd = pairs[:, 1, :, 128 * t:128 * t + 128]
            first = jnp.where(low, even, pltpu.roll(odd, N, 2))
            second = jnp.where(low, pltpu.roll(even, N, 2), odd)
            both = jnp.concatenate([first, second], axis=1).astype(BF16)
            for jp in range(32):
                send[jp // 4, p, pl.ds(32 * h + 16 * t, 16), pl.ds(128 * (jp % 4), 128)] = both[jp]

    is_edge = jnp.logical_or(chip == 0, chip == 3)
    inward = jnp.where(chip < 2, 1, -1)
    edge_near = chip + inward
    mid_cross, mid_far, mid_back = chip + inward, chip + 2 * inward, chip - inward

    def send_row(p):
        block(p, 2 * chip + 1 - core).start()

        @pl.when(is_edge)
        def _():
            for k in range(2):
                block(p, 2 * edge_near + k).start()

        @pl.when(jnp.logical_not(is_edge))
        def _():
            for other in (mid_cross, mid_far, mid_back):
                for k in range(2):
                    block(p, 2 * other + k).start()

    def make_row(p, carry):
        load_row(p).wait()
        for h in range(2):
            half_row(p, h)
        send_row(p)
        return carry

    lax.fori_loop(0, ROWS, make_row, 0)

    @pl.when(is_edge)
    def _():
        def far_row(p, carry):
            for step in (2, 3):
                for k in range(2):
                    block(p, 2 * (chip + step * inward) + k).start()
            return carry

        lax.fori_loop(0, ROWS, far_row, 0)

    def third(src, p, first, second):
        g0 = jnp.dot(ct_vm[...], first, preferred_element_type=F32).reshape(8, 8, COLS)
        g1 = jnp.dot(ct_vm[...], second, preferred_element_type=F32).reshape(8, 8, COLS)
        at = pl.multiple_of(N * src + 8 * p, 16)
        g_ref[:, pl.ds(at, 16), :] = jnp.concatenate([g0, g1], axis=1).astype(BF16)

    def own(t, carry):
        third(me, 2 * t, send[me, 2 * t], send[me, 2 * t + 1])
        return carry

    lax.fori_loop(0, ROWS // 2, own, 0)

    def arrived(src, p):
        pltpu.make_async_remote_copy(
            src_ref=send.at[src, p],
            dst_ref=recv.at[src, p],
            send_sem=send_sem.at[src, p],
            recv_sem=recv_sem.at[src, p],
            device_id={"dev": src},
            device_id_type=pl.DeviceIdType.MESH,
        ).wait_recv()

    def take(src):
        def body(t, carry):
            arrived(src, 2 * t)
            arrived(src, 2 * t + 1)
            third(src, 2 * t, recv[src, 2 * t], recv[src, 2 * t + 1])
            return carry

        lax.fori_loop(0, ROWS // 2, body, 0)

    take(2 * chip + 1 - core)
    order = [
        jnp.where(is_edge, chip + inward, chip - inward),
        jnp.where(is_edge, chip + 2 * inward, chip + inward),
        jnp.where(is_edge, chip + 3 * inward, chip + 2 * inward),
    ]
    for other in order:
        for k in range(2):
            take(2 * other + k)

    def sent(p, carry):
        for k in range(1, DEV):
            block(p, (me + k) % DEV).wait_send()
        return carry

    lax.fori_loop(0, ROWS, sent, 0)


def fourth_kernel(g_ref, l4_ref, v_hbm, v_vm, v_sem):
    def put(ag):
        return pltpu.make_async_copy(v_vm.at[ag], v_hbm.at[:, pl.ds(8 * ag, 8), :], v_sem.at[ag])

    for ag in range(8):
        v_vm[ag] = jnp.dot(l4_ref[...], g_ref[ag], preferred_element_type=F32).reshape(N, 8, COLS)
        put(ag).start()
    for ag in range(8):
        put(ag).wait()


def solution(mesh):
    def local_transform(ao_rows, coeffs):
        vmem = pl.BlockSpec(memory_space=pltpu.VMEM)
        anywhere = pl.BlockSpec(memory_space=pltpu.HBM)
        g, l4 = pl.pallas_call(
            exchange_kernel,
            out_shape=(
                jax.ShapeDtypeStruct((8, 8 * N, COLS), BF16),
                jax.ShapeDtypeStruct((8 * N, 8 * N), BF16),
            ),
            in_specs=[anywhere, anywhere],
            out_specs=(vmem, vmem),
            scratch_shapes=[
                pltpu.VMEM((ROWS, N, N, N), BF16),
                pltpu.VMEM((N, N), BF16),
                pltpu.VMEM((8 * N, 8 * N), BF16),
                pltpu.VMEM((4 * N, 4 * N), BF16),
                pltpu.VMEM((N, N), BF16),
                pltpu.VMEM((DEV, ROWS, N, COLS), BF16),
                pltpu.VMEM((DEV, ROWS, N, COLS), BF16),
                pltpu.SemaphoreType.DMA((ROWS,)),
                pltpu.SemaphoreType.DMA,
                pltpu.SemaphoreType.DMA((DEV, ROWS)),
                pltpu.SemaphoreType.DMA((DEV, ROWS)),
            ],
            compiler_params=pltpu.CompilerParams(collective_id=0, has_side_effects=True, vmem_limit_bytes=56 * 2**20),
            name="exchange",
        )(ao_rows, coeffs)
        return pl.pallas_call(
            fourth_kernel,
            out_shape=jax.ShapeDtypeStruct((N, N, COLS), F32),
            in_specs=[vmem, vmem],
            out_specs=anywhere,
            scratch_shapes=[pltpu.VMEM((8, N, 8, COLS), F32), pltpu.SemaphoreType.DMA((8,))],
            compiler_params=pltpu.CompilerParams(vmem_limit_bytes=24 * 2**20),
            name="fourth",
        )(g, l4)

    return jax.shard_map(local_transform, mesh=mesh, in_specs=(P(('frag', 'dev')), P('frag')), out_specs=P('frag', None, 'dev'), check_vma=False)
```

```python
import functools

import jax
import jax.numpy as jnp
from jax import lax
from jax.experimental import pallas as pl
from jax.experimental.pallas import tpu as pltpu
from jax.sharding import PartitionSpec as P

N = 64
DEV = 8
ROWS = N // DEV
COLS = N * N // DEV
BF16 = jnp.bfloat16
F32 = jnp.float32


def iota(shape, dim):
    return lax.broadcasted_iota(jnp.int32, shape, dim)


def exchange_kernel(a_hbm, c_hbm, g_ref, l4_ref, a_vm, c_vm, l_vm, b4_vm, ct_vm, send, recv, a_sem, c_sem, send_sem, recv_sem):
    me = lax.axis_index("dev")
    chip = me // 2
    core = me % 2

    load_c = pltpu.make_async_copy(c_hbm, c_vm, c_sem)
    load_c.start()

    def load_row(p):
        return pltpu.make_async_copy(a_hbm.at[p], a_vm.at[p], a_sem.at[p])

    for p in range(ROWS):
        load_row(p).start()

    barrier = pltpu.get_barrier_semaphore()
    for k in range(1, DEV):
        pl.semaphore_signal(barrier, inc=1, device_id={"dev": (me + k) % DEV}, device_id_type=pl.DeviceIdType.MESH)

    load_c.wait()
    c = c_vm[...]
    spread = (iota((8 * N, N), 0) // 8 == iota((8 * N, N), 1)).astype(BF16)
    nt = (((1,), (1,)), ((), ()))
    rows = lax.dot_general(spread, c, nt, preferred_element_type=F32)
    wide = (8 * N, 8 * N)
    pair = jnp.concatenate([rows, rows], axis=1)
    tiled = jnp.concatenate([pair] * 4, axis=1)
    l_vm[...] = jnp.where(iota(wide, 0) % 8 == iota(wide, 1) // N, tiled, 0.0).astype(BF16)
    widen = (iota((N, 8 * N), 0) == iota((N, 8 * N), 1) // 8).astype(BF16)
    full = jnp.dot(rows.astype(BF16), widen, preferred_element_type=F32)
    l4_ref[...] = jnp.where(iota(wide, 0) % 8 == iota(wide, 1) % 8, full, 0.0).astype(BF16)
    cf = c.astype(F32)
    cpair = jnp.concatenate([cf, cf], axis=1)
    c4 = jnp.concatenate([cpair, cpair], axis=1)
    c44 = jnp.concatenate([c4] * 4, axis=0)
    quad = (4 * N, 4 * N)
    b4_vm[...] = jnp.where(iota(quad, 0) // N == iota(quad, 1) // N, c44, 0.0).astype(BF16)
    eye = (iota((N, N), 0) == iota((N, N), 1)).astype(BF16)
    ct_vm[...] = lax.dot_general(eye, c, nt, preferred_element_type=F32).astype(BF16)

    pl.semaphore_wait(barrier, DEV - 1)

    def block(p, dest):
        return pltpu.make_async_remote_copy(
            src_ref=send.at[dest, p],
            dst_ref=recv.at[me, p],
            send_sem=send_sem.at[dest, p],
            recv_sem=recv_sem.at[me, p],
            device_id={"dev": dest},
            device_id_type=pl.DeviceIdType.MESH,
        )

    low = iota((32, 8, 128), 2) < N

    def half_row(p, h):
        a = a_vm[p, pl.ds(32 * h, 32)].reshape(4, 8 * N, N)
        left = jnp.concatenate([a[0], a[1]], axis=1)
        right = jnp.concatenate([a[2], a[3]], axis=1)
        a4 = jnp.concatenate([left, right], axis=1)
        t_one = jnp.dot(l_vm[...], a4, preferred_element_type=F32).astype(BF16)
        half = jnp.dot(t_one, b4_vm[...], preferred_element_type=F32)
        pairs = half.reshape(32, 2, 8, 256)
        for t in range(2):
            even = pairs[:, 0, :, 128 * t:128 * t + 128]
            odd = pairs[:, 1, :, 128 * t:128 * t + 128]
            first = jnp.where(low, even, pltpu.roll(odd, N, 2))
            second = jnp.where(low, pltpu.roll(even, N, 2), odd)
            both = jnp.concatenate([first, second], axis=1).astype(BF16)
            for jp in range(32):
                send[jp // 4, p, pl.ds(32 * h + 16 * t, 16), pl.ds(128 * (jp % 4), 128)] = both[jp]

    is_edge = jnp.logical_or(chip == 0, chip == 3)
    inward = jnp.where(chip < 2, 1, -1)
    edge_near = chip + inward
    mid_cross, mid_far, mid_back = chip + inward, chip + 2 * inward, chip - inward

    def send_row(p):
        block(p, 2 * chip + 1 - core).start()

        @pl.when(is_edge)
        def _():
            for k in range(2):
                block(p, 2 * edge_near + k).start()

        @pl.when(jnp.logical_not(is_edge))
        def _():
            for other in (mid_cross, mid_far, mid_back):
                for k in range(2):
                    block(p, 2 * other + k).start()

    def make_row(p, carry):
        load_row(p).wait()
        for h in range(2):
            half_row(p, h)
        send_row(p)
        return carry

    lax.fori_loop(0, ROWS, make_row, 0)

    def far_rows(dest):
        return pltpu.make_async_remote_copy(
            src_ref=send.at[dest],
            dst_ref=recv.at[me],
            send_sem=send_sem.at[dest, 0],
            recv_sem=recv_sem.at[me, 0],
            device_id={"dev": dest},
            device_id_type=pl.DeviceIdType.MESH,
        )

    @pl.when(is_edge)
    def _():
        for step in (2, 3):
            for k in range(2):
                far_rows(2 * (chip + step * inward) + k).start()

    def third(src, p, first, second):
        g0 = jnp.dot(ct_vm[...], first, preferred_element_type=F32).reshape(8, 8, COLS)
        g1 = jnp.dot(ct_vm[...], second, preferred_element_type=F32).reshape(8, 8, COLS)
        at = pl.multiple_of(N * src + 8 * p, 16)
        g_ref[:, pl.ds(at, 16), :] = jnp.concatenate([g0, g1], axis=1).astype(BF16)

    def own(t, carry):
        third(me, 2 * t, send[me, 2 * t], send[me, 2 * t + 1])
        return carry

    lax.fori_loop(0, ROWS // 2, own, 0)

    def arrived(src, p):
        pltpu.make_async_remote_copy(
            src_ref=send.at[src, p],
            dst_ref=recv.at[src, p],
            send_sem=send_sem.at[src, p],
            recv_sem=recv_sem.at[src, p],
            device_id={"dev": src},
            device_id_type=pl.DeviceIdType.MESH,
        ).wait_recv()

    def take(src):
        def body(t, carry):
            arrived(src, 2 * t)
            arrived(src, 2 * t + 1)
            third(src, 2 * t, recv[src, 2 * t], recv[src, 2 * t + 1])
            return carry

        lax.fori_loop(0, ROWS // 2, body, 0)

    take(2 * chip + 1 - core)
    order = [
        jnp.where(is_edge, chip + inward, chip - inward),
        jnp.where(is_edge, chip + 2 * inward, chip + inward),
        jnp.where(is_edge, chip + 3 * inward, chip + 2 * inward),
    ]
    for other in order[:2]:
        for k in range(2):
            take(2 * other + k)

    def take_far(src):
        pltpu.make_async_remote_copy(
            src_ref=send.at[src],
            dst_ref=recv.at[src],
            send_sem=send_sem.at[src, 0],
            recv_sem=recv_sem.at[src, 0],
            device_id={"dev": src},
            device_id_type=pl.DeviceIdType.MESH,
        ).wait_recv()

        def body(t, carry):
            third(src, 2 * t, recv[src, 2 * t], recv[src, 2 * t + 1])
            return carry

        lax.fori_loop(0, ROWS // 2, body, 0)

    for k in range(2):
        take_far(2 * order[2] + k)

    def sent_row(p, carry):
        block(p, 2 * chip + 1 - core).wait_send()

        @pl.when(is_edge)
        def _():
            for k in range(2):
                block(p, 2 * edge_near + k).wait_send()

        @pl.when(jnp.logical_not(is_edge))
        def _():
            for other in (mid_cross, mid_far, mid_back):
                for k in range(2):
                    block(p, 2 * other + k).wait_send()

        return carry

    lax.fori_loop(0, ROWS, sent_row, 0)

    @pl.when(is_edge)
    def _():
        for step in (2, 3):
            for k in range(2):
                far_rows(2 * (chip + step * inward) + k).wait_send()


def fourth_kernel(g_ref, l4_ref, v_hbm, v_vm, v_sem):
    def put(ag):
        return pltpu.make_async_copy(v_vm.at[ag], v_hbm.at[:, pl.ds(8 * ag, 8), :], v_sem.at[ag])

    for ag in range(8):
        v_vm[ag] = jnp.dot(l4_ref[...], g_ref[ag], preferred_element_type=F32).reshape(N, 8, COLS)
        put(ag).start()
    for ag in range(8):
        put(ag).wait()


def solution(mesh):
    def local_transform(ao_rows, coeffs):
        vmem = pl.BlockSpec(memory_space=pltpu.VMEM)
        anywhere = pl.BlockSpec(memory_space=pltpu.HBM)
        g, l4 = pl.pallas_call(
            exchange_kernel,
            out_shape=(
                jax.ShapeDtypeStruct((8, 8 * N, COLS), BF16),
                jax.ShapeDtypeStruct((8 * N, 8 * N), BF16),
            ),
            in_specs=[anywhere, anywhere],
            out_specs=(vmem, vmem),
            scratch_shapes=[
                pltpu.VMEM((ROWS, N, N, N), BF16),
                pltpu.VMEM((N, N), BF16),
                pltpu.VMEM((8 * N, 8 * N), BF16),
                pltpu.VMEM((4 * N, 4 * N), BF16),
                pltpu.VMEM((N, N), BF16),
                pltpu.VMEM((DEV, ROWS, N, COLS), BF16),
                pltpu.VMEM((DEV, ROWS, N, COLS), BF16),
                pltpu.SemaphoreType.DMA((ROWS,)),
                pltpu.SemaphoreType.DMA,
                pltpu.SemaphoreType.DMA((DEV, ROWS)),
                pltpu.SemaphoreType.DMA((DEV, ROWS)),
            ],
            compiler_params=pltpu.CompilerParams(collective_id=0, has_side_effects=True, vmem_limit_bytes=53 * 2**20),
            name="exchange",
        )(ao_rows, coeffs)
        return pl.pallas_call(
            fourth_kernel,
            out_shape=jax.ShapeDtypeStruct((N, N, COLS), F32),
            in_specs=[vmem, vmem],
            out_specs=anywhere,
            scratch_shapes=[pltpu.VMEM((8, N, 8, COLS), F32), pltpu.SemaphoreType.DMA((8,))],
            compiler_params=pltpu.CompilerParams(vmem_limit_bytes=24 * 2**20),
            name="fourth",
        )(g, l4)

    return jax.shard_map(local_transform, mesh=mesh, in_specs=(P(('frag', 'dev')), P('frag')), out_specs=P('frag', None, 'dev'), check_vma=False)
```

```python
import functools

import jax
import jax.numpy as jnp
from jax import lax
from jax.experimental import pallas as pl
from jax.experimental.pallas import tpu as pltpu
from jax.sharding import PartitionSpec as P

N = 64
DEV = 8
ROWS = N // DEV
COLS = N * N // DEV
BF16 = jnp.bfloat16
F32 = jnp.float32


def iota(shape, dim):
    return lax.broadcasted_iota(jnp.int32, shape, dim)


def exchange_kernel(a_hbm, c_hbm, g_ref, l4_ref, a_vm, c_vm, l_vm, b4_vm, ct_vm, send, recv, a_sem, c_sem, send_sem, recv_sem):
    me = lax.axis_index("dev")
    chip = me // 2
    core = me % 2

    load_c = pltpu.make_async_copy(c_hbm, c_vm, c_sem)
    load_c.start()

    def load_row(p):
        return pltpu.make_async_copy(a_hbm.at[p], a_vm.at[p], a_sem.at[p])

    for p in range(ROWS):
        load_row(p).start()

    barrier = pltpu.get_barrier_semaphore()
    for k in range(1, DEV):
        pl.semaphore_signal(barrier, inc=1, device_id={"dev": (me + k) % DEV}, device_id_type=pl.DeviceIdType.MESH)

    load_c.wait()
    c = c_vm[...]
    spread = (iota((8 * N, N), 0) // 8 == iota((8 * N, N), 1)).astype(BF16)
    nt = (((1,), (1,)), ((), ()))
    rows = lax.dot_general(spread, c, nt, preferred_element_type=F32)
    wide = (8 * N, 8 * N)
    pair = jnp.concatenate([rows, rows], axis=1)
    tiled = jnp.concatenate([pair] * 4, axis=1)
    l_vm[...] = jnp.where(iota(wide, 0) % 8 == iota(wide, 1) // N, tiled, 0.0).astype(BF16)
    widen = (iota((N, 8 * N), 0) == iota((N, 8 * N), 1) // 8).astype(BF16)
    full = jnp.dot(rows.astype(BF16), widen, preferred_element_type=F32)
    l4_ref[...] = jnp.where(iota(wide, 0) % 8 == iota(wide, 1) % 8, full, 0.0).astype(BF16)
    cf = c.astype(F32)
    cpair = jnp.concatenate([cf, cf], axis=1)
    c4 = jnp.concatenate([cpair, cpair], axis=1)
    c44 = jnp.concatenate([c4] * 4, axis=0)
    quad = (4 * N, 4 * N)
    b4_vm[...] = jnp.where(iota(quad, 0) // N == iota(quad, 1) // N, c44, 0.0).astype(BF16)
    eye = (iota((N, N), 0) == iota((N, N), 1)).astype(BF16)
    ct_vm[...] = lax.dot_general(eye, c, nt, preferred_element_type=F32).astype(BF16)

    pl.semaphore_wait(barrier, DEV - 1)

    def block(p, dest):
        return pltpu.make_async_remote_copy(
            src_ref=send.at[dest, p],
            dst_ref=recv.at[me, p],
            send_sem=send_sem.at[dest, p],
            recv_sem=recv_sem.at[me, p],
            device_id={"dev": dest},
            device_id_type=pl.DeviceIdType.MESH,
        )

    low = iota((32, 8, 128), 2) < N

    def half_row(p, h):
        a = a_vm[p, pl.ds(32 * h, 32)].reshape(4, 8 * N, N)
        left = jnp.concatenate([a[0], a[1]], axis=1)
        right = jnp.concatenate([a[2], a[3]], axis=1)
        a4 = jnp.concatenate([left, right], axis=1)
        t_one = jnp.dot(l_vm[...], a4, preferred_element_type=F32).astype(BF16)
        half = jnp.dot(t_one, b4_vm[...], preferred_element_type=F32)
        pairs = half.reshape(32, 2, 8, 256)
        for t in range(2):
            even = pairs[:, 0, :, 128 * t:128 * t + 128]
            odd = pairs[:, 1, :, 128 * t:128 * t + 128]
            first = jnp.where(low, even, pltpu.roll(odd, N, 2))
            second = jnp.where(low, pltpu.roll(even, N, 2), odd)
            both = jnp.concatenate([first, second], axis=1).astype(BF16)
            for jp in range(32):
                send[jp // 4, p, pl.ds(32 * h + 16 * t, 16), pl.ds(128 * (jp % 4), 128)] = both[jp]

    is_edge = jnp.logical_or(chip == 0, chip == 3)
    inward = jnp.where(chip < 2, 1, -1)
    edge_near = chip + inward
    mid_cross, mid_far, mid_back = chip + inward, chip + 2 * inward, chip - inward

    def send_row(p):
        block(p, 2 * chip + 1 - core).start()

        @pl.when(is_edge)
        def _():
            for k in range(2):
                block(p, 2 * edge_near + k).start()

        @pl.when(jnp.logical_not(is_edge))
        def _():
            for other in (mid_cross, mid_far, mid_back):
                for k in range(2):
                    block(p, 2 * other + k).start()

    def make_row(p, carry):
        load_row(p).wait()
        for h in range(2):
            half_row(p, h)
        send_row(p)
        return carry

    lax.fori_loop(0, ROWS, make_row, 0)

    def far_rows(dest):
        return pltpu.make_async_remote_copy(
            src_ref=send.at[dest],
            dst_ref=recv.at[me],
            send_sem=send_sem.at[dest, 0],
            recv_sem=recv_sem.at[me, 0],
            device_id={"dev": dest},
            device_id_type=pl.DeviceIdType.MESH,
        )

    @pl.when(is_edge)
    def _():
        for step in (2, 3):
            for k in range(2):
                far_rows(2 * (chip + step * inward) + k).start()

    def third(src, p, first, second):
        g0 = jnp.dot(ct_vm[...], first, preferred_element_type=F32).reshape(8, 8, COLS)
        g1 = jnp.dot(ct_vm[...], second, preferred_element_type=F32).reshape(8, 8, COLS)
        at = pl.multiple_of(N * src + 8 * p, 16)
        g_ref[:, pl.ds(at, 16), :] = jnp.concatenate([g0, g1], axis=1).astype(BF16)

    def own(t, carry):
        third(me, 2 * t, send[me, 2 * t], send[me, 2 * t + 1])
        return carry

    lax.fori_loop(0, ROWS // 2, own, 0)

    def arrived(src, p):
        pltpu.make_async_remote_copy(
            src_ref=send.at[src, p],
            dst_ref=recv.at[src, p],
            send_sem=send_sem.at[src, p],
            recv_sem=recv_sem.at[src, p],
            device_id={"dev": src},
            device_id_type=pl.DeviceIdType.MESH,
        ).wait_recv()

    def take(src):
        def body(t, carry):
            arrived(src, 2 * t)
            arrived(src, 2 * t + 1)
            third(src, 2 * t, recv[src, 2 * t], recv[src, 2 * t + 1])
            return carry

        lax.fori_loop(0, ROWS // 2, body, 0)

    take(2 * chip + 1 - core)
    order = [
        jnp.where(is_edge, chip + inward, chip - inward),
        jnp.where(is_edge, chip + 2 * inward, chip + inward),
        jnp.where(is_edge, chip + 3 * inward, chip + 2 * inward),
    ]
    for other in order[:2]:
        for k in range(2):
            take(2 * other + k)

    def take_far(src):
        pltpu.make_async_remote_copy(
            src_ref=send.at[src],
            dst_ref=recv.at[src],
            send_sem=send_sem.at[src, 0],
            recv_sem=recv_sem.at[src, 0],
            device_id={"dev": src},
            device_id_type=pl.DeviceIdType.MESH,
        ).wait_recv()

        def body(t, carry):
            third(src, 2 * t, recv[src, 2 * t], recv[src, 2 * t + 1])
            return carry

        lax.fori_loop(0, ROWS // 2, body, 0)

    for k in range(2):
        take_far(2 * order[2] + k)

    def sent_row(p, carry):
        block(p, 2 * chip + 1 - core).wait_send()

        @pl.when(is_edge)
        def _():
            for k in range(2):
                block(p, 2 * edge_near + k).wait_send()

        @pl.when(jnp.logical_not(is_edge))
        def _():
            for other in (mid_cross, mid_far, mid_back):
                for k in range(2):
                    block(p, 2 * other + k).wait_send()

        return carry

    lax.fori_loop(0, ROWS, sent_row, 0)

    @pl.when(is_edge)
    def _():
        for step in (2, 3):
            for k in range(2):
                far_rows(2 * (chip + step * inward) + k).wait_send()


def fourth_kernel(g_ref, l4_ref, v_hbm, v_vm, v_sem):
    def put(ag):
        return pltpu.make_async_copy(v_vm.at[ag], v_hbm.at[:, pl.ds(8 * ag, 8), :], v_sem.at[ag])

    for ag in range(8):
        v_vm[ag] = jnp.dot(l4_ref[...], g_ref[ag], preferred_element_type=F32).reshape(N, 8, COLS)
        put(ag).start()
    for ag in range(8):
        put(ag).wait()


def solution(mesh):
    def local_transform(ao_rows, coeffs):
        vmem = pl.BlockSpec(memory_space=pltpu.VMEM)
        anywhere = pl.BlockSpec(memory_space=pltpu.HBM)
        g, l4 = pl.pallas_call(
            exchange_kernel,
            out_shape=(
                jax.ShapeDtypeStruct((8, 8 * N, COLS), BF16),
                jax.ShapeDtypeStruct((8 * N, 8 * N), BF16),
            ),
            in_specs=[anywhere, anywhere],
            out_specs=(vmem, vmem),
            scratch_shapes=[
                pltpu.VMEM((ROWS, N, N, N), BF16),
                pltpu.VMEM((N, N), BF16),
                pltpu.VMEM((8 * N, 8 * N), BF16),
                pltpu.VMEM((4 * N, 4 * N), BF16),
                pltpu.VMEM((N, N), BF16),
                pltpu.VMEM((DEV, ROWS, N, COLS), BF16),
                pltpu.VMEM((DEV, ROWS, N, COLS), BF16),
                pltpu.SemaphoreType.DMA((ROWS,)),
                pltpu.SemaphoreType.DMA,
                pltpu.SemaphoreType.DMA((DEV, ROWS)),
                pltpu.SemaphoreType.DMA((DEV, ROWS)),
            ],
            compiler_params=pltpu.CompilerParams(collective_id=0, has_side_effects=True, vmem_limit_bytes=48 * 2**20),
            name="exchange",
        )(pltpu.with_memory_space_constraint(ao_rows, pltpu.HBM), pltpu.with_memory_space_constraint(coeffs, pltpu.HBM))
        return pl.pallas_call(
            fourth_kernel,
            out_shape=jax.ShapeDtypeStruct((N, N, COLS), F32),
            in_specs=[vmem, vmem],
            out_specs=anywhere,
            scratch_shapes=[pltpu.VMEM((8, N, 8, COLS), F32), pltpu.SemaphoreType.DMA((8,))],
            compiler_params=pltpu.CompilerParams(vmem_limit_bytes=24 * 2**20),
            name="fourth",
        )(g, l4)

    return jax.shard_map(local_transform, mesh=mesh, in_specs=(P(('frag', 'dev')), P('frag')), out_specs=P('frag', None, 'dev'), check_vma=False)
```

```python
import functools

import jax
import jax.numpy as jnp
from jax import lax
from jax.experimental import pallas as pl
from jax.experimental.pallas import tpu as pltpu
from jax.sharding import PartitionSpec as P

N = 64
DEV = 8
ROWS = N // DEV
COLS = N * N // DEV
BF16 = jnp.bfloat16
F32 = jnp.float32


def iota(shape, dim):
    return lax.broadcasted_iota(jnp.int32, shape, dim)


def exchange_kernel(a_hbm, c_hbm, g_ref, l4_ref, a_vm, c_vm, l_vm, b4_vm, ct_vm, send, recv, a_sem, c_sem, send_sem, recv_sem):
    me = lax.axis_index("dev")
    chip = me // 2
    core = me % 2

    load_c = pltpu.make_async_copy(c_hbm, c_vm, c_sem)
    load_c.start()

    def load_row(p):
        return pltpu.make_async_copy(a_hbm.at[p], a_vm.at[p], a_sem.at[p])

    for p in range(ROWS):
        load_row(p).start()

    barrier = pltpu.get_barrier_semaphore()
    for k in range(1, DEV):
        pl.semaphore_signal(barrier, inc=1, device_id={"dev": (me + k) % DEV}, device_id_type=pl.DeviceIdType.MESH)

    load_c.wait()
    c = c_vm[...]
    spread = (iota((8 * N, N), 0) // 8 == iota((8 * N, N), 1)).astype(BF16)
    nt = (((1,), (1,)), ((), ()))
    rows = lax.dot_general(spread, c, nt, preferred_element_type=F32)
    wide = (8 * N, 8 * N)
    pair = jnp.concatenate([rows, rows], axis=1)
    tiled = jnp.concatenate([pair] * 4, axis=1)
    l_vm[...] = jnp.where(iota(wide, 0) % 8 == iota(wide, 1) // N, tiled, 0.0).astype(BF16)
    widen = (iota((N, 8 * N), 0) == iota((N, 8 * N), 1) // 8).astype(BF16)
    full = jnp.dot(rows.astype(BF16), widen, preferred_element_type=F32)
    l4_ref[...] = jnp.where(iota(wide, 0) % 8 == iota(wide, 1) % 8, full, 0.0).astype(BF16)
    cf = c.astype(F32)
    cpair = jnp.concatenate([cf, cf], axis=1)
    c4 = jnp.concatenate([cpair, cpair], axis=1)
    c44 = jnp.concatenate([c4] * 4, axis=0)
    quad = (4 * N, 4 * N)
    b4_vm[...] = jnp.where(iota(quad, 0) // N == iota(quad, 1) // N, c44, 0.0).astype(BF16)
    eye = (iota((N, N), 0) == iota((N, N), 1)).astype(BF16)
    ct_vm[...] = lax.dot_general(eye, c, nt, preferred_element_type=F32).astype(BF16)

    pl.semaphore_wait(barrier, DEV - 1)

    def block(p, dest):
        return pltpu.make_async_remote_copy(
            src_ref=send.at[dest, p],
            dst_ref=recv.at[me, p],
            send_sem=send_sem.at[dest, p],
            recv_sem=recv_sem.at[me, p],
            device_id={"dev": dest},
            device_id_type=pl.DeviceIdType.MESH,
        )

    low = iota((32, 8, 128), 2) < N

    def half_row(p, h):
        a = a_vm[p, pl.ds(32 * h, 32)].reshape(4, 8 * N, N)
        left = jnp.concatenate([a[0], a[1]], axis=1)
        right = jnp.concatenate([a[2], a[3]], axis=1)
        a4 = jnp.concatenate([left, right], axis=1)
        t_one = jnp.dot(l_vm[...], a4, preferred_element_type=F32).astype(BF16)
        half = jnp.dot(t_one, b4_vm[...], preferred_element_type=F32)
        pairs = half.reshape(32, 2, 8, 256)
        for t in range(2):
            even = pairs[:, 0, :, 128 * t:128 * t + 128]
            odd = pairs[:, 1, :, 128 * t:128 * t + 128]
            first = jnp.where(low, even, pltpu.roll(odd, N, 2))
            second = jnp.where(low, pltpu.roll(even, N, 2), odd)
            both = jnp.concatenate([first, second], axis=1).astype(BF16)
            for jp in range(32):
                send[jp // 4, p, pl.ds(32 * h + 16 * t, 16), pl.ds(128 * (jp % 4), 128)] = both[jp]

    is_edge = jnp.logical_or(chip == 0, chip == 3)
    inward = jnp.where(chip < 2, 1, -1)
    partner = 2 * chip + 1 - core
    near = chip + inward
    far = chip + 2 * inward
    last = chip + 3 * inward
    outward = chip - inward

    def send_row(p):
        block(p, partner).start()
        for k in range(2):
            block(p, 2 * near + k).start()

        @pl.when(jnp.logical_not(is_edge))
        def _():
            for k in range(2):
                block(p, 2 * outward + k).start()

    def make_row(p, carry):
        load_row(p).wait()
        for h in range(2):
            half_row(p, h)
        send_row(p)
        return carry

    lax.fori_loop(0, ROWS, make_row, 0)

    def rows(dest, src):
        return pltpu.make_async_remote_copy(
            src_ref=send.at[dest],
            dst_ref=recv.at[src],
            send_sem=send_sem.at[dest, 0],
            recv_sem=recv_sem.at[src, 0],
            device_id={"dev": dest},
            device_id_type=pl.DeviceIdType.MESH,
        )

    def third(src, p, first, second):
        g0 = jnp.dot(ct_vm[...], first, preferred_element_type=F32).reshape(8, 8, COLS)
        g1 = jnp.dot(ct_vm[...], second, preferred_element_type=F32).reshape(8, 8, COLS)
        at = pl.multiple_of(N * src + 8 * p, 16)
        g_ref[:, pl.ds(at, 16), :] = jnp.concatenate([g0, g1], axis=1).astype(BF16)

    def own(t, carry):
        third(me, 2 * t, send[me, 2 * t], send[me, 2 * t + 1])
        return carry

    lax.fori_loop(0, ROWS // 2, own, 0)

    def await_rows(src):
        def body(p, carry):
            pltpu.make_async_remote_copy(
                src_ref=send.at[src, p],
                dst_ref=recv.at[src, p],
                send_sem=send_sem.at[src, p],
                recv_sem=recv_sem.at[src, p],
                device_id={"dev": src},
                device_id_type=pl.DeviceIdType.MESH,
            ).wait_recv()
            return carry

        lax.fori_loop(0, ROWS, body, 0)

    def third_rows(src):
        def body(t, carry):
            third(src, 2 * t, recv[src, 2 * t], recv[src, 2 * t + 1])
            return carry

        lax.fori_loop(0, ROWS // 2, body, 0)

    def sent_rows(dest):
        def body(p, carry):
            block(p, dest).wait_send()
            return carry

        lax.fori_loop(0, ROWS, body, 0)

    await_rows(partner)
    third_rows(partner)

    for k in range(2):
        sent_rows(2 * near + k)
    for k in range(2):
        rows(2 * far + k, me).start()

    beside = jnp.where(is_edge, near, outward)
    for k in range(2):
        await_rows(2 * beside + k)
        third_rows(2 * beside + k)

    @pl.when(is_edge)
    def _():
        for k in range(2):
            rows(2 * far + k, me).wait_send()
        for k in range(2):
            rows(2 * last + k, me).start()
        for k in range(2):
            rows(2 * far + k, 2 * far + k).wait_recv()

    @pl.when(jnp.logical_not(is_edge))
    def _():
        for k in range(2):
            await_rows(2 * near + k)

    second = jnp.where(is_edge, far, near)
    for k in range(2):
        third_rows(2 * second + k)

    third_chip = jnp.where(is_edge, last, far)
    for k in range(2):
        rows(2 * third_chip + k, 2 * third_chip + k).wait_recv()
        third_rows(2 * third_chip + k)

    sent_rows(partner)

    @pl.when(is_edge)
    def _():
        for k in range(2):
            rows(2 * last + k, me).wait_send()

    @pl.when(jnp.logical_not(is_edge))
    def _():
        for k in range(2):
            rows(2 * far + k, me).wait_send()
            sent_rows(2 * outward + k)


def fourth_kernel(g_ref, l4_ref, v_hbm, v_vm, v_sem):
    def put(ag):
        return pltpu.make_async_copy(v_vm.at[ag], v_hbm.at[:, pl.ds(8 * ag, 8), :], v_sem.at[ag])

    for ag in range(8):
        v_vm[ag] = jnp.dot(l4_ref[...], g_ref[ag], preferred_element_type=F32).reshape(N, 8, COLS)
        put(ag).start()
    for ag in range(8):
        put(ag).wait()


def solution(mesh):
    def local_transform(ao_rows, coeffs):
        vmem = pl.BlockSpec(memory_space=pltpu.VMEM)
        anywhere = pl.BlockSpec(memory_space=pltpu.HBM)
        g, l4 = pl.pallas_call(
            exchange_kernel,
            out_shape=(
                jax.ShapeDtypeStruct((8, 8 * N, COLS), BF16),
                jax.ShapeDtypeStruct((8 * N, 8 * N), BF16),
            ),
            in_specs=[anywhere, anywhere],
            out_specs=(vmem, vmem),
            scratch_shapes=[
                pltpu.VMEM((ROWS, N, N, N), BF16),
                pltpu.VMEM((N, N), BF16),
                pltpu.VMEM((8 * N, 8 * N), BF16),
                pltpu.VMEM((4 * N, 4 * N), BF16),
                pltpu.VMEM((N, N), BF16),
                pltpu.VMEM((DEV, ROWS, N, COLS), BF16),
                pltpu.VMEM((DEV, ROWS, N, COLS), BF16),
                pltpu.SemaphoreType.DMA((ROWS,)),
                pltpu.SemaphoreType.DMA,
                pltpu.SemaphoreType.DMA((DEV, ROWS)),
                pltpu.SemaphoreType.DMA((DEV, ROWS)),
            ],
            compiler_params=pltpu.CompilerParams(collective_id=0, has_side_effects=True, vmem_limit_bytes=48 * 2**20),
            name="exchange",
        )(pltpu.with_memory_space_constraint(ao_rows, pltpu.HBM), pltpu.with_memory_space_constraint(coeffs, pltpu.HBM))
        return pl.pallas_call(
            fourth_kernel,
            out_shape=jax.ShapeDtypeStruct((N, N, COLS), F32),
            in_specs=[vmem, vmem],
            out_specs=anywhere,
            scratch_shapes=[pltpu.VMEM((8, N, 8, COLS), F32), pltpu.SemaphoreType.DMA((8,))],
            compiler_params=pltpu.CompilerParams(vmem_limit_bytes=24 * 2**20),
            name="fourth",
        )(g, l4)

    return jax.shard_map(local_transform, mesh=mesh, in_specs=(P(('frag', 'dev')), P('frag')), out_specs=P('frag', None, 'dev'), check_vma=False)
```

```python
import functools

import jax
import jax.numpy as jnp
from jax import lax
from jax.experimental import pallas as pl
from jax.experimental.pallas import tpu as pltpu
from jax.sharding import PartitionSpec as P

N = 64
DEV = 8
ROWS = N // DEV
COLS = N * N // DEV
BF16 = jnp.bfloat16
F32 = jnp.float32


def iota(shape, dim):
    return lax.broadcasted_iota(jnp.int32, shape, dim)


def exchange_kernel(a_hbm, c_hbm, g_ref, l4_ref, a_vm, c_vm, l_vm, b4_vm, ct_vm, send, recv, a_sem, c_sem, send_sem, recv_sem):
    me = lax.axis_index("dev")
    chip = me // 2
    core = me % 2

    load_c = pltpu.make_async_copy(c_hbm, c_vm, c_sem)
    load_c.start()

    def load_row(p):
        return pltpu.make_async_copy(a_hbm.at[p], a_vm.at[p], a_sem.at[p])

    for p in range(ROWS):
        load_row(p).start()

    barrier = pltpu.get_barrier_semaphore()
    for k in range(1, DEV):
        pl.semaphore_signal(barrier, inc=1, device_id={"dev": (me + k) % DEV}, device_id_type=pl.DeviceIdType.MESH)

    load_c.wait()
    c = c_vm[...]
    spread = (iota((8 * N, N), 0) // 8 == iota((8 * N, N), 1)).astype(BF16)
    nt = (((1,), (1,)), ((), ()))
    rows = lax.dot_general(spread, c, nt, preferred_element_type=F32)
    wide = (8 * N, 8 * N)
    pair = jnp.concatenate([rows, rows], axis=1)
    tiled = jnp.concatenate([pair] * 4, axis=1)
    l_vm[...] = jnp.where(iota(wide, 0) % 8 == iota(wide, 1) // N, tiled, 0.0).astype(BF16)
    widen = (iota((N, 8 * N), 0) == iota((N, 8 * N), 1) // 8).astype(BF16)
    full = jnp.dot(rows.astype(BF16), widen, preferred_element_type=F32)
    l4_ref[...] = jnp.where(iota(wide, 0) % 8 == iota(wide, 1) % 8, full, 0.0).astype(BF16)
    cf = c.astype(F32)
    cpair = jnp.concatenate([cf, cf], axis=1)
    c4 = jnp.concatenate([cpair, cpair], axis=1)
    c44 = jnp.concatenate([c4] * 4, axis=0)
    quad = (4 * N, 4 * N)
    b4_vm[...] = jnp.where(iota(quad, 0) // N == iota(quad, 1) // N, c44, 0.0).astype(BF16)
    eye = (iota((N, N), 0) == iota((N, N), 1)).astype(BF16)
    ct_vm[...] = lax.dot_general(eye, c, nt, preferred_element_type=F32).astype(BF16)

    pl.semaphore_wait(barrier, DEV - 1)

    def block(p, dest):
        return pltpu.make_async_remote_copy(
            src_ref=send.at[dest, p],
            dst_ref=recv.at[me, p],
            send_sem=send_sem.at[dest, p],
            recv_sem=recv_sem.at[me, p],
            device_id={"dev": dest},
            device_id_type=pl.DeviceIdType.MESH,
        )

    low = iota((32, 8, 128), 2) < N

    def half_row(p, h):
        a = a_vm[p, pl.ds(32 * h, 32)].reshape(4, 8 * N, N)
        left = jnp.concatenate([a[0], a[1]], axis=1)
        right = jnp.concatenate([a[2], a[3]], axis=1)
        a4 = jnp.concatenate([left, right], axis=1)
        t_one = jnp.dot(l_vm[...], a4, preferred_element_type=F32).astype(BF16)
        half = jnp.dot(t_one, b4_vm[...], preferred_element_type=F32)
        pairs = half.reshape(32, 2, 8, 256)
        for t in range(2):
            even = pairs[:, 0, :, 128 * t:128 * t + 128]
            odd = pairs[:, 1, :, 128 * t:128 * t + 128]
            first = jnp.where(low, even, pltpu.roll(odd, N, 2))
            second = jnp.where(low, pltpu.roll(even, N, 2), odd)
            both = jnp.concatenate([first, second], axis=1).astype(BF16)
            for jp in range(32):
                send[jp // 4, p, pl.ds(32 * h + 16 * t, 16), pl.ds(128 * (jp % 4), 128)] = both[jp]

    is_edge = jnp.logical_or(chip == 0, chip == 3)
    inward = jnp.where(chip < 2, 1, -1)
    partner = 2 * chip + 1 - core
    near = chip + inward
    far = chip + 2 * inward
    last = chip + 3 * inward
    outward = chip - inward
    third_chip = jnp.where(is_edge, last, outward)

    def make_row(p, carry):
        load_row(p).wait()
        for h in range(2):
            half_row(p, h)
        for other in (third_chip, far):
            for k in range(2):
                block(p, 2 * other + k).start()
        block(p, partner).start()
        return carry

    lax.fori_loop(0, ROWS, make_row, 0)

    def near_row(p, carry):
        for k in range(2):
            block(p, 2 * near + k).start()
        return carry

    lax.fori_loop(0, ROWS, near_row, 0)

    def third(src, p, first, second):
        g0 = jnp.dot(ct_vm[...], first, preferred_element_type=F32).reshape(8, 8, COLS)
        g1 = jnp.dot(ct_vm[...], second, preferred_element_type=F32).reshape(8, 8, COLS)
        at = pl.multiple_of(N * src + 8 * p, 16)
        g_ref[:, pl.ds(at, 16), :] = jnp.concatenate([g0, g1], axis=1).astype(BF16)

    def own(t, carry):
        third(me, 2 * t, send[me, 2 * t], send[me, 2 * t + 1])
        return carry

    lax.fori_loop(0, ROWS // 2, own, 0)

    def arrived(src, p):
        pltpu.make_async_remote_copy(
            src_ref=send.at[src, p],
            dst_ref=recv.at[src, p],
            send_sem=send_sem.at[src, p],
            recv_sem=recv_sem.at[src, p],
            device_id={"dev": src},
            device_id_type=pl.DeviceIdType.MESH,
        ).wait_recv()

    def take(sources):
        def body(t, carry):
            for src in sources:
                arrived(src, 2 * t)
                arrived(src, 2 * t + 1)
                third(src, 2 * t, recv[src, 2 * t], recv[src, 2 * t + 1])
            return carry

        lax.fori_loop(0, ROWS // 2, body, 0)

    take([partner])
    for other in (third_chip, far, near):
        take([2 * other, 2 * other + 1])

    def sent_row(p, carry):
        for k in range(1, DEV):
            block(p, (me + k) % DEV).wait_send()
        return carry

    lax.fori_loop(0, ROWS, sent_row, 0)


def fourth_kernel(g_ref, l4_ref, v_hbm, v_vm, v_sem):
    def put(ag):
        return pltpu.make_async_copy(v_vm.at[ag], v_hbm.at[:, pl.ds(8 * ag, 8), :], v_sem.at[ag])

    for ag in range(8):
        v_vm[ag] = jnp.dot(l4_ref[...], g_ref[ag], preferred_element_type=F32).reshape(N, 8, COLS)
        put(ag).start()
    for ag in range(8):
        put(ag).wait()


def solution(mesh):
    def local_transform(ao_rows, coeffs):
        vmem = pl.BlockSpec(memory_space=pltpu.VMEM)
        anywhere = pl.BlockSpec(memory_space=pltpu.HBM)
        g, l4 = pl.pallas_call(
            exchange_kernel,
            out_shape=(
                jax.ShapeDtypeStruct((8, 8 * N, COLS), BF16),
                jax.ShapeDtypeStruct((8 * N, 8 * N), BF16),
            ),
            in_specs=[anywhere, anywhere],
            out_specs=(vmem, vmem),
            scratch_shapes=[
                pltpu.VMEM((ROWS, N, N, N), BF16),
                pltpu.VMEM((N, N), BF16),
                pltpu.VMEM((8 * N, 8 * N), BF16),
                pltpu.VMEM((4 * N, 4 * N), BF16),
                pltpu.VMEM((N, N), BF16),
                pltpu.VMEM((DEV, ROWS, N, COLS), BF16),
                pltpu.VMEM((DEV, ROWS, N, COLS), BF16),
                pltpu.SemaphoreType.DMA((ROWS,)),
                pltpu.SemaphoreType.DMA,
                pltpu.SemaphoreType.DMA((DEV, ROWS)),
                pltpu.SemaphoreType.DMA((DEV, ROWS)),
            ],
            compiler_params=pltpu.CompilerParams(collective_id=0, has_side_effects=True, vmem_limit_bytes=48 * 2**20),
            name="exchange",
        )(pltpu.with_memory_space_constraint(ao_rows, pltpu.HBM), pltpu.with_memory_space_constraint(coeffs, pltpu.HBM))
        return pl.pallas_call(
            fourth_kernel,
            out_shape=jax.ShapeDtypeStruct((N, N, COLS), F32),
            in_specs=[vmem, vmem],
            out_specs=anywhere,
            scratch_shapes=[pltpu.VMEM((8, N, 8, COLS), F32), pltpu.SemaphoreType.DMA((8,))],
            compiler_params=pltpu.CompilerParams(vmem_limit_bytes=24 * 2**20),
            name="fourth",
        )(g, l4)

    return jax.shard_map(local_transform, mesh=mesh, in_specs=(P(('frag', 'dev')), P('frag')), out_specs=P('frag', None, 'dev'), check_vma=False)
```

```python
import functools

import jax
import jax.numpy as jnp
from jax import lax
from jax.experimental import pallas as pl
from jax.experimental.pallas import tpu as pltpu
from jax.sharding import PartitionSpec as P

N = 64
DEV = 8
ROWS = N // DEV
COLS = N * N // DEV
BF16 = jnp.bfloat16
F32 = jnp.float32


def iota(shape, dim):
    return lax.broadcasted_iota(jnp.int32, shape, dim)


def exchange_kernel(a_hbm, c_hbm, g_ref, l4_ref, a_vm, c_vm, l_vm, b4_vm, ct_vm, send, recv, a_sem, c_sem, send_sem, recv_sem):
    me = lax.axis_index("dev")
    chip = me // 2
    core = me % 2

    load_c = pltpu.make_async_copy(c_hbm, c_vm, c_sem)
    load_c.start()

    def load_row(p):
        return pltpu.make_async_copy(a_hbm.at[p], a_vm.at[p], a_sem.at[p])

    for p in range(ROWS):
        load_row(p).start()

    barrier = pltpu.get_barrier_semaphore()
    for k in range(1, DEV):
        pl.semaphore_signal(barrier, inc=1, device_id={"dev": (me + k) % DEV}, device_id_type=pl.DeviceIdType.MESH)

    load_c.wait()
    c = c_vm[...]
    spread = (iota((8 * N, N), 0) // 8 == iota((8 * N, N), 1)).astype(BF16)
    nt = (((1,), (1,)), ((), ()))
    rows = lax.dot_general(spread, c, nt, preferred_element_type=F32)
    wide = (8 * N, 8 * N)
    pair = jnp.concatenate([rows, rows], axis=1)
    tiled = jnp.concatenate([pair] * 4, axis=1)
    l_vm[...] = jnp.where(iota(wide, 0) % 8 == iota(wide, 1) // N, tiled, 0.0).astype(BF16)
    widen = (iota((N, 8 * N), 0) == iota((N, 8 * N), 1) // 8).astype(BF16)
    full = jnp.dot(rows.astype(BF16), widen, preferred_element_type=F32)
    l4_ref[...] = jnp.where(iota(wide, 0) % 8 == iota(wide, 1) % 8, full, 0.0).astype(BF16)
    cf = c.astype(F32)
    cpair = jnp.concatenate([cf, cf], axis=1)
    c4 = jnp.concatenate([cpair, cpair], axis=1)
    c44 = jnp.concatenate([c4] * 4, axis=0)
    quad = (4 * N, 4 * N)
    b4_vm[...] = jnp.where(iota(quad, 0) // N == iota(quad, 1) // N, c44, 0.0).astype(BF16)
    eye = (iota((N, N), 0) == iota((N, N), 1)).astype(BF16)
    ct_vm[...] = lax.dot_general(eye, c, nt, preferred_element_type=F32).astype(BF16)

    pl.semaphore_wait(barrier, DEV - 1)

    def block(p, dest):
        return pltpu.make_async_remote_copy(
            src_ref=send.at[dest, p],
            dst_ref=recv.at[me, p],
            send_sem=send_sem.at[dest, p],
            recv_sem=recv_sem.at[me, p],
            device_id={"dev": dest},
            device_id_type=pl.DeviceIdType.MESH,
        )

    low = iota((32, 8, 128), 2) < N

    def half_row(p, h):
        a = a_vm[p, pl.ds(32 * h, 32)].reshape(4, 8 * N, N)
        left = jnp.concatenate([a[0], a[1]], axis=1)
        right = jnp.concatenate([a[2], a[3]], axis=1)
        a4 = jnp.concatenate([left, right], axis=1)
        t_one = jnp.dot(l_vm[...], a4, preferred_element_type=F32).astype(BF16)
        half = jnp.dot(t_one, b4_vm[...], preferred_element_type=F32)
        pairs = half.reshape(32, 2, 8, 256)
        for t in range(2):
            even = pairs[:, 0, :, 128 * t:128 * t + 128]
            odd = pairs[:, 1, :, 128 * t:128 * t + 128]
            first = jnp.where(low, even, pltpu.roll(odd, N, 2))
            second = jnp.where(low, pltpu.roll(even, N, 2), odd)
            both = jnp.concatenate([first, second], axis=1).astype(BF16)
            for jp in range(32):
                send[jp // 4, p, pl.ds(32 * h + 16 * t, 16), pl.ds(128 * (jp % 4), 128)] = both[jp]

    is_edge = jnp.logical_or(chip == 0, chip == 3)
    inward = jnp.where(chip < 2, 1, -1)
    partner = 2 * chip + 1 - core
    near = chip + inward
    far = chip + 2 * inward
    last = chip + 3 * inward
    outward = chip - inward
    third_chip = jnp.where(is_edge, last, outward)

    def make_row(p, carry):
        load_row(p).wait()
        for h in range(2):
            half_row(p, h)
        for other in (third_chip, far):
            for mine in (core, 1 - core):
                block(p, 2 * other + mine).start()
        block(p, partner).start()
        return carry

    lax.fori_loop(0, ROWS, make_row, 0)

    def near_row(p, carry):
        for mine in (core, 1 - core):
            block(p, 2 * near + mine).start()
        return carry

    lax.fori_loop(0, ROWS, near_row, 0)

    def third(src, p, first, second):
        g0 = jnp.dot(ct_vm[...], first, preferred_element_type=F32).reshape(8, 8, COLS)
        g1 = jnp.dot(ct_vm[...], second, preferred_element_type=F32).reshape(8, 8, COLS)
        at = pl.multiple_of(N * src + 8 * p, 16)
        g_ref[:, pl.ds(at, 16), :] = jnp.concatenate([g0, g1], axis=1).astype(BF16)

    def own(t, carry):
        third(me, 2 * t, send[me, 2 * t], send[me, 2 * t + 1])
        return carry

    lax.fori_loop(0, ROWS // 2, own, 0)

    def arrived(src, p):
        pltpu.make_async_remote_copy(
            src_ref=send.at[src, p],
            dst_ref=recv.at[src, p],
            send_sem=send_sem.at[src, p],
            recv_sem=recv_sem.at[src, p],
            device_id={"dev": src},
            device_id_type=pl.DeviceIdType.MESH,
        ).wait_recv()

    def take(sources):
        def body(t, carry):
            for src in sources:
                arrived(src, 2 * t)
                arrived(src, 2 * t + 1)
                third(src, 2 * t, recv[src, 2 * t], recv[src, 2 * t + 1])
            return carry

        lax.fori_loop(0, ROWS // 2, body, 0)

    take([partner])
    for other in (third_chip, far, near):
        take([2 * other, 2 * other + 1])

    def sent_row(p, carry):
        for k in range(1, DEV):
            block(p, (me + k) % DEV).wait_send()
        return carry

    lax.fori_loop(0, ROWS, sent_row, 0)


def fourth_kernel(g_ref, l4_ref, v_hbm, v_vm, v_sem):
    def put(ag):
        return pltpu.make_async_copy(v_vm.at[ag], v_hbm.at[:, pl.ds(8 * ag, 8), :], v_sem.at[ag])

    for ag in range(8):
        v_vm[ag] = jnp.dot(l4_ref[...], g_ref[ag], preferred_element_type=F32).reshape(N, 8, COLS)
        put(ag).start()
    for ag in range(8):
        put(ag).wait()


def solution(mesh):
    def local_transform(ao_rows, coeffs):
        vmem = pl.BlockSpec(memory_space=pltpu.VMEM)
        anywhere = pl.BlockSpec(memory_space=pltpu.HBM)
        g, l4 = pl.pallas_call(
            exchange_kernel,
            out_shape=(
                jax.ShapeDtypeStruct((8, 8 * N, COLS), BF16),
                jax.ShapeDtypeStruct((8 * N, 8 * N), BF16),
            ),
            in_specs=[anywhere, anywhere],
            out_specs=(vmem, vmem),
            scratch_shapes=[
                pltpu.VMEM((ROWS, N, N, N), BF16),
                pltpu.VMEM((N, N), BF16),
                pltpu.VMEM((8 * N, 8 * N), BF16),
                pltpu.VMEM((4 * N, 4 * N), BF16),
                pltpu.VMEM((N, N), BF16),
                pltpu.VMEM((DEV, ROWS, N, COLS), BF16),
                pltpu.VMEM((DEV, ROWS, N, COLS), BF16),
                pltpu.SemaphoreType.DMA((ROWS,)),
                pltpu.SemaphoreType.DMA,
                pltpu.SemaphoreType.DMA((DEV, ROWS)),
                pltpu.SemaphoreType.DMA((DEV, ROWS)),
            ],
            compiler_params=pltpu.CompilerParams(collective_id=0, has_side_effects=True, vmem_limit_bytes=48 * 2**20),
            name="exchange",
        )(pltpu.with_memory_space_constraint(ao_rows, pltpu.HBM), pltpu.with_memory_space_constraint(coeffs, pltpu.HBM))
        return pl.pallas_call(
            fourth_kernel,
            out_shape=jax.ShapeDtypeStruct((N, N, COLS), F32),
            in_specs=[vmem, vmem],
            out_specs=anywhere,
            scratch_shapes=[pltpu.VMEM((8, N, 8, COLS), F32), pltpu.SemaphoreType.DMA((8,))],
            compiler_params=pltpu.CompilerParams(vmem_limit_bytes=24 * 2**20),
            name="fourth",
        )(g, l4)

    return jax.shard_map(local_transform, mesh=mesh, in_specs=(P(('frag', 'dev')), P('frag')), out_specs=P('frag', None, 'dev'), check_vma=False)
```

```python
import functools

import jax
import jax.numpy as jnp
from jax import lax
from jax.experimental import pallas as pl
from jax.experimental.pallas import tpu as pltpu
from jax.sharding import PartitionSpec as P

N = 64
DEV = 8
ROWS = N // DEV
COLS = N * N // DEV
BF16 = jnp.bfloat16
F32 = jnp.float32


def iota(shape, dim):
    return lax.broadcasted_iota(jnp.int32, shape, dim)


def exchange_kernel(a_hbm, c_hbm, g_ref, l4_ref, a_vm, c_vm, l_vm, b4_vm, ct_vm, send, recv, a_sem, c_sem, send_sem, recv_sem):
    me = lax.axis_index("dev")
    chip = me // 2
    core = me % 2

    load_c = pltpu.make_async_copy(c_hbm, c_vm, c_sem)
    load_c.start()

    def load_row(p):
        return pltpu.make_async_copy(a_hbm.at[p], a_vm.at[p], a_sem.at[p])

    load_row(0).start()

    barrier = pltpu.get_barrier_semaphore()
    for k in range(1, DEV):
        pl.semaphore_signal(barrier, inc=1, device_id={"dev": (me + k) % DEV}, device_id_type=pl.DeviceIdType.MESH)

    load_c.wait()
    c = c_vm[...]
    spread = (iota((8 * N, N), 0) // 8 == iota((8 * N, N), 1)).astype(BF16)
    nt = (((1,), (1,)), ((), ()))
    rows = lax.dot_general(spread, c, nt, preferred_element_type=F32)
    wide = (8 * N, 8 * N)
    pair = jnp.concatenate([rows, rows], axis=1)
    tiled = jnp.concatenate([pair] * 4, axis=1)
    l_vm[...] = jnp.where(iota(wide, 0) % 8 == iota(wide, 1) // N, tiled, 0.0).astype(BF16)
    cf = c.astype(F32)
    cpair = jnp.concatenate([cf, cf], axis=1)
    c4 = jnp.concatenate([cpair, cpair], axis=1)
    c44 = jnp.concatenate([c4] * 4, axis=0)
    quad = (4 * N, 4 * N)
    b4_vm[...] = jnp.where(iota(quad, 0) // N == iota(quad, 1) // N, c44, 0.0).astype(BF16)

    pl.semaphore_wait(barrier, DEV - 1)

    def block(p, dest):
        return pltpu.make_async_remote_copy(
            src_ref=send.at[dest, p],
            dst_ref=recv.at[me, p],
            send_sem=send_sem.at[dest, p],
            recv_sem=recv_sem.at[me, p],
            device_id={"dev": dest},
            device_id_type=pl.DeviceIdType.MESH,
        )

    low = iota((32, 8, 128), 2) < N

    def half_row(p, h):
        a = a_vm[p, pl.ds(32 * h, 32)].reshape(4, 8 * N, N)
        left = jnp.concatenate([a[0], a[1]], axis=1)
        right = jnp.concatenate([a[2], a[3]], axis=1)
        a4 = jnp.concatenate([left, right], axis=1)
        t_one = jnp.dot(l_vm[...], a4, preferred_element_type=F32).astype(BF16)
        half = jnp.dot(t_one, b4_vm[...], preferred_element_type=F32)
        pairs = half.reshape(32, 2, 8, 256)
        for t in range(2):
            even = pairs[:, 0, :, 128 * t:128 * t + 128]
            odd = pairs[:, 1, :, 128 * t:128 * t + 128]
            first = jnp.where(low, even, pltpu.roll(odd, N, 2))
            second = jnp.where(low, pltpu.roll(even, N, 2), odd)
            both = jnp.concatenate([first, second], axis=1).astype(BF16)
            for jp in range(32):
                send[jp // 4, p, pl.ds(32 * h + 16 * t, 16), pl.ds(128 * (jp % 4), 128)] = both[jp]

    is_edge = jnp.logical_or(chip == 0, chip == 3)
    inward = jnp.where(chip < 2, 1, -1)
    partner = 2 * chip + 1 - core
    near = chip + inward
    far = chip + 2 * inward
    last = chip + 3 * inward
    outward = chip - inward
    third_chip = jnp.where(is_edge, last, outward)

    def make_row(p, carry):
        load_row(p).wait()

        @pl.when(p == 0)
        def _():
            for later in range(1, ROWS):
                load_row(later).start()

        for h in range(2):
            half_row(p, h)
        for other in (third_chip, far):
            for mine in (core, 1 - core):
                block(p, 2 * other + mine).start()
        block(p, partner).start()
        return carry

    lax.fori_loop(0, ROWS, make_row, 0)

    def near_row(p, carry):
        for mine in (core, 1 - core):
            block(p, 2 * near + mine).start()
        return carry

    lax.fori_loop(0, ROWS, near_row, 0)

    c = c_vm[...]
    rows = lax.dot_general(spread, c, nt, preferred_element_type=F32)
    widen = (iota((N, 8 * N), 0) == iota((N, 8 * N), 1) // 8).astype(BF16)
    full = jnp.dot(rows.astype(BF16), widen, preferred_element_type=F32)
    l4_ref[...] = jnp.where(iota(wide, 0) % 8 == iota(wide, 1) % 8, full, 0.0).astype(BF16)
    eye = (iota((N, N), 0) == iota((N, N), 1)).astype(BF16)
    ct_vm[...] = lax.dot_general(eye, c, nt, preferred_element_type=F32).astype(BF16)

    def third(src, p, first, second):
        g0 = jnp.dot(ct_vm[...], first, preferred_element_type=F32).reshape(8, 8, COLS)
        g1 = jnp.dot(ct_vm[...], second, preferred_element_type=F32).reshape(8, 8, COLS)
        at = pl.multiple_of(N * src + 8 * p, 16)
        g_ref[:, pl.ds(at, 16), :] = jnp.concatenate([g0, g1], axis=1).astype(BF16)

    def own(t, carry):
        third(me, 2 * t, send[me, 2 * t], send[me, 2 * t + 1])
        return carry

    lax.fori_loop(0, ROWS // 2, own, 0)

    def arrived(src, p):
        pltpu.make_async_remote_copy(
            src_ref=send.at[src, p],
            dst_ref=recv.at[src, p],
            send_sem=send_sem.at[src, p],
            recv_sem=recv_sem.at[src, p],
            device_id={"dev": src},
            device_id_type=pl.DeviceIdType.MESH,
        ).wait_recv()

    def take(sources):
        def body(t, carry):
            for src in sources:
                arrived(src, 2 * t)
                arrived(src, 2 * t + 1)
                third(src, 2 * t, recv[src, 2 * t], recv[src, 2 * t + 1])
            return carry

        lax.fori_loop(0, ROWS // 2, body, 0)

    take([partner])
    for other in (third_chip, far, near):
        take([2 * other, 2 * other + 1])

    def sent_row(p, carry):
        for k in range(1, DEV):
            block(p, (me + k) % DEV).wait_send()
        return carry

    lax.fori_loop(0, ROWS, sent_row, 0)


def fourth_kernel(g_ref, l4_ref, v_hbm, v_vm, v_sem):
    def put(ag):
        return pltpu.make_async_copy(v_vm.at[ag], v_hbm.at[:, pl.ds(8 * ag, 8), :], v_sem.at[ag])

    for ag in range(8):
        v_vm[ag] = jnp.dot(l4_ref[...], g_ref[ag], preferred_element_type=F32).reshape(N, 8, COLS)
        put(ag).start()
    for ag in range(8):
        put(ag).wait()


def solution(mesh):
    def local_transform(ao_rows, coeffs):
        vmem = pl.BlockSpec(memory_space=pltpu.VMEM)
        anywhere = pl.BlockSpec(memory_space=pltpu.HBM)
        g, l4 = pl.pallas_call(
            exchange_kernel,
            out_shape=(
                jax.ShapeDtypeStruct((8, 8 * N, COLS), BF16),
                jax.ShapeDtypeStruct((8 * N, 8 * N), BF16),
            ),
            in_specs=[anywhere, anywhere],
            out_specs=(vmem, vmem),
            scratch_shapes=[
                pltpu.VMEM((ROWS, N, N, N), BF16),
                pltpu.VMEM((N, N), BF16),
                pltpu.VMEM((8 * N, 8 * N), BF16),
                pltpu.VMEM((4 * N, 4 * N), BF16),
                pltpu.VMEM((N, N), BF16),
                pltpu.VMEM((DEV, ROWS, N, COLS), BF16),
                pltpu.VMEM((DEV, ROWS, N, COLS), BF16),
                pltpu.SemaphoreType.DMA((ROWS,)),
                pltpu.SemaphoreType.DMA,
                pltpu.SemaphoreType.DMA((DEV, ROWS)),
                pltpu.SemaphoreType.DMA((DEV, ROWS)),
            ],
            compiler_params=pltpu.CompilerParams(collective_id=0, has_side_effects=True, vmem_limit_bytes=48 * 2**20),
            name="exchange",
        )(pltpu.with_memory_space_constraint(ao_rows, pltpu.HBM), pltpu.with_memory_space_constraint(coeffs, pltpu.HBM))
        return pl.pallas_call(
            fourth_kernel,
            out_shape=jax.ShapeDtypeStruct((N, N, COLS), F32),
            in_specs=[vmem, vmem],
            out_specs=anywhere,
            scratch_shapes=[pltpu.VMEM((8, N, 8, COLS), F32), pltpu.SemaphoreType.DMA((8,))],
            compiler_params=pltpu.CompilerParams(vmem_limit_bytes=24 * 2**20),
            name="fourth",
        )(g, l4)

    return jax.shard_map(local_transform, mesh=mesh, in_specs=(P(('frag', 'dev')), P('frag')), out_specs=P('frag', None, 'dev'), check_vma=False)
```

```python
import functools

import jax
import jax.numpy as jnp
from jax import lax
from jax.experimental import pallas as pl
from jax.experimental.pallas import tpu as pltpu
from jax.sharding import PartitionSpec as P

N = 64
DEV = 8
ROWS = N // DEV
COLS = N * N // DEV
NEAR_GROUPS = ((0, 4), (4, 2), (6, 2))
BF16 = jnp.bfloat16
F32 = jnp.float32


def iota(shape, dim):
    return lax.broadcasted_iota(jnp.int32, shape, dim)


def exchange_kernel(a_hbm, c_hbm, g_ref, l4_ref, a_vm, c_vm, l_vm, b4_vm, ct_vm, send, recv, a_sem, c_sem, send_sem, recv_sem):
    me = lax.axis_index("dev")
    chip = me // 2
    core = me % 2

    load_c = pltpu.make_async_copy(c_hbm, c_vm, c_sem)
    load_c.start()

    def load_row(p):
        return pltpu.make_async_copy(a_hbm.at[p], a_vm.at[p], a_sem.at[p])

    load_row(0).start()

    barrier = pltpu.get_barrier_semaphore()
    for k in range(1, DEV):
        pl.semaphore_signal(barrier, inc=1, device_id={"dev": (me + k) % DEV}, device_id_type=pl.DeviceIdType.MESH)

    load_c.wait()
    c = c_vm[...]
    spread = (iota((8 * N, N), 0) // 8 == iota((8 * N, N), 1)).astype(BF16)
    nt = (((1,), (1,)), ((), ()))
    rows = lax.dot_general(spread, c, nt, preferred_element_type=F32)
    wide = (8 * N, 8 * N)
    pair = jnp.concatenate([rows, rows], axis=1)
    tiled = jnp.concatenate([pair] * 4, axis=1)
    l_vm[...] = jnp.where(iota(wide, 0) % 8 == iota(wide, 1) // N, tiled, 0.0).astype(BF16)
    cf = c.astype(F32)
    cpair = jnp.concatenate([cf, cf], axis=1)
    c4 = jnp.concatenate([cpair, cpair], axis=1)
    c44 = jnp.concatenate([c4] * 4, axis=0)
    quad = (4 * N, 4 * N)
    b4_vm[...] = jnp.where(iota(quad, 0) // N == iota(quad, 1) // N, c44, 0.0).astype(BF16)

    pl.semaphore_wait(barrier, DEV - 1)

    def block(p, dest):
        return pltpu.make_async_remote_copy(
            src_ref=send.at[dest, p],
            dst_ref=recv.at[me, p],
            send_sem=send_sem.at[dest, p],
            recv_sem=recv_sem.at[me, p],
            device_id={"dev": dest},
            device_id_type=pl.DeviceIdType.MESH,
        )

    low = iota((32, 8, 128), 2) < N

    def half_row(p, h):
        a = a_vm[p, pl.ds(32 * h, 32)].reshape(4, 8 * N, N)
        left = jnp.concatenate([a[0], a[1]], axis=1)
        right = jnp.concatenate([a[2], a[3]], axis=1)
        a4 = jnp.concatenate([left, right], axis=1)
        t_one = jnp.dot(l_vm[...], a4, preferred_element_type=F32).astype(BF16)
        half = jnp.dot(t_one, b4_vm[...], preferred_element_type=F32)
        pairs = half.reshape(32, 2, 8, 256)
        for t in range(2):
            even = pairs[:, 0, :, 128 * t:128 * t + 128]
            odd = pairs[:, 1, :, 128 * t:128 * t + 128]
            first = jnp.where(low, even, pltpu.roll(odd, N, 2))
            second = jnp.where(low, pltpu.roll(even, N, 2), odd)
            both = jnp.concatenate([first, second], axis=1).astype(BF16)
            for jp in range(32):
                send[jp // 4, p, pl.ds(32 * h + 16 * t, 16), pl.ds(128 * (jp % 4), 128)] = both[jp]

    is_edge = jnp.logical_or(chip == 0, chip == 3)
    inward = jnp.where(chip < 2, 1, -1)
    partner = 2 * chip + 1 - core
    near = chip + inward
    far = chip + 2 * inward
    last = chip + 3 * inward
    outward = chip - inward
    third_chip = jnp.where(is_edge, last, outward)

    def make_row(p, carry):
        load_row(p).wait()

        @pl.when(p == 0)
        def _():
            for later in range(1, ROWS):
                load_row(later).start()

        for h in range(2):
            half_row(p, h)
        for other in (third_chip, far):
            for mine in (core, 1 - core):
                block(p, 2 * other + mine).start()
        block(p, partner).start()
        return carry

    lax.fori_loop(0, ROWS, make_row, 0)

    def group(first, count, dest, src):
        part = pl.ds(first, count)
        return pltpu.make_async_remote_copy(
            src_ref=send.at[dest, part],
            dst_ref=recv.at[src, part],
            send_sem=send_sem.at[dest, first],
            recv_sem=recv_sem.at[src, first],
            device_id={"dev": dest},
            device_id_type=pl.DeviceIdType.MESH,
        )

    @pl.when(is_edge)
    def _():
        def near_row(p, carry):
            for mine in (core, 1 - core):
                block(p, 2 * near + mine).start()
            return carry

        lax.fori_loop(0, ROWS, near_row, 0)

    @pl.when(jnp.logical_not(is_edge))
    def _():
        for first, count in NEAR_GROUPS:
            for mine in (core, 1 - core):
                group(first, count, 2 * near + mine, me).start()

    c = c_vm[...]
    rows = lax.dot_general(spread, c, nt, preferred_element_type=F32)
    widen = (iota((N, 8 * N), 0) == iota((N, 8 * N), 1) // 8).astype(BF16)
    full = jnp.dot(rows.astype(BF16), widen, preferred_element_type=F32)
    l4_ref[...] = jnp.where(iota(wide, 0) % 8 == iota(wide, 1) % 8, full, 0.0).astype(BF16)
    eye = (iota((N, N), 0) == iota((N, N), 1)).astype(BF16)
    ct_vm[...] = lax.dot_general(eye, c, nt, preferred_element_type=F32).astype(BF16)

    def third(src, p, first, second):
        g0 = jnp.dot(ct_vm[...], first, preferred_element_type=F32).reshape(8, 8, COLS)
        g1 = jnp.dot(ct_vm[...], second, preferred_element_type=F32).reshape(8, 8, COLS)
        at = pl.multiple_of(N * src + 8 * p, 16)
        g_ref[:, pl.ds(at, 16), :] = jnp.concatenate([g0, g1], axis=1).astype(BF16)

    def own(t, carry):
        third(me, 2 * t, send[me, 2 * t], send[me, 2 * t + 1])
        return carry

    lax.fori_loop(0, ROWS // 2, own, 0)

    def arrived(src, p):
        pltpu.make_async_remote_copy(
            src_ref=send.at[src, p],
            dst_ref=recv.at[src, p],
            send_sem=send_sem.at[src, p],
            recv_sem=recv_sem.at[src, p],
            device_id={"dev": src},
            device_id_type=pl.DeviceIdType.MESH,
        ).wait_recv()

    def take(sources):
        def body(t, carry):
            for src in sources:
                arrived(src, 2 * t)
                arrived(src, 2 * t + 1)
                third(src, 2 * t, recv[src, 2 * t], recv[src, 2 * t + 1])
            return carry

        lax.fori_loop(0, ROWS // 2, body, 0)

    take([partner])
    for other in (third_chip, far):
        take([2 * other, 2 * other + 1])

    @pl.when(is_edge)
    def _():
        take([2 * near, 2 * near + 1])

    @pl.when(jnp.logical_not(is_edge))
    def _():
        for first, count in NEAR_GROUPS:
            for k in range(2):
                src = 2 * near + k
                group(first, count, src, src).wait_recv()
                for p in range(first, first + count, 2):
                    third(src, p, recv[src, p], recv[src, p + 1])

    def sent_row(p, carry):
        block(p, partner).wait_send()
        for other in (third_chip, far):
            for k in range(2):
                block(p, 2 * other + k).wait_send()
        return carry

    lax.fori_loop(0, ROWS, sent_row, 0)

    @pl.when(is_edge)
    def _():
        def near_sent(p, carry):
            for k in range(2):
                block(p, 2 * near + k).wait_send()
            return carry

        lax.fori_loop(0, ROWS, near_sent, 0)

    @pl.when(jnp.logical_not(is_edge))
    def _():
        for first, count in NEAR_GROUPS:
            for k in range(2):
                group(first, count, 2 * near + k, me).wait_send()


def fourth_kernel(g_ref, l4_ref, v_hbm, v_vm, v_sem):
    def put(ag):
        return pltpu.make_async_copy(v_vm.at[ag], v_hbm.at[:, pl.ds(8 * ag, 8), :], v_sem.at[ag])

    for ag in range(8):
        v_vm[ag] = jnp.dot(l4_ref[...], g_ref[ag], preferred_element_type=F32).reshape(N, 8, COLS)
        put(ag).start()
    for ag in range(8):
        put(ag).wait()


def solution(mesh):
    def local_transform(ao_rows, coeffs):
        vmem = pl.BlockSpec(memory_space=pltpu.VMEM)
        anywhere = pl.BlockSpec(memory_space=pltpu.HBM)
        g, l4 = pl.pallas_call(
            exchange_kernel,
            out_shape=(
                jax.ShapeDtypeStruct((8, 8 * N, COLS), BF16),
                jax.ShapeDtypeStruct((8 * N, 8 * N), BF16),
            ),
            in_specs=[anywhere, anywhere],
            out_specs=(vmem, vmem),
            scratch_shapes=[
                pltpu.VMEM((ROWS, N, N, N), BF16),
                pltpu.VMEM((N, N), BF16),
                pltpu.VMEM((8 * N, 8 * N), BF16),
                pltpu.VMEM((4 * N, 4 * N), BF16),
                pltpu.VMEM((N, N), BF16),
                pltpu.VMEM((DEV, ROWS, N, COLS), BF16),
                pltpu.VMEM((DEV, ROWS, N, COLS), BF16),
                pltpu.SemaphoreType.DMA((ROWS,)),
                pltpu.SemaphoreType.DMA,
                pltpu.SemaphoreType.DMA((DEV, ROWS)),
                pltpu.SemaphoreType.DMA((DEV, ROWS)),
            ],
            compiler_params=pltpu.CompilerParams(collective_id=0, has_side_effects=True, vmem_limit_bytes=48 * 2**20),
            name="exchange",
        )(pltpu.with_memory_space_constraint(ao_rows, pltpu.HBM), pltpu.with_memory_space_constraint(coeffs, pltpu.HBM))
        return pl.pallas_call(
            fourth_kernel,
            out_shape=jax.ShapeDtypeStruct((N, N, COLS), F32),
            in_specs=[vmem, vmem],
            out_specs=anywhere,
            scratch_shapes=[pltpu.VMEM((8, N, 8, COLS), F32), pltpu.SemaphoreType.DMA((8,))],
            compiler_params=pltpu.CompilerParams(vmem_limit_bytes=24 * 2**20),
            name="fourth",
        )(g, l4)

    return jax.shard_map(local_transform, mesh=mesh, in_specs=(P(('frag', 'dev')), P('frag')), out_specs=P('frag', None, 'dev'), check_vma=False)
```

```python
import functools

import jax
import jax.numpy as jnp
from jax import lax
from jax.experimental import pallas as pl
from jax.experimental.pallas import tpu as pltpu
from jax.sharding import PartitionSpec as P


N = 64
DEV = 8
ROWS = N // DEV
COLS = N * N // DEV
CHUNKS = COLS // 128
BF16 = jnp.bfloat16
F32 = jnp.float32


def iota(shape, dim):
    return lax.broadcasted_iota(jnp.int32, shape, dim)


def exchange_kernel(a_hbm, c_hbm, g_ref, l4_ref, l4n_ref, ct_ref, *refs):
    near_refs = refs[:2 * CHUNKS]
    a_vm, c_vm, l_vm, b4_vm, ct_vm, send, recv, a_sem, c_sem, send_sem, recv_sem = refs[2 * CHUNKS:]
    me = lax.axis_index("dev")
    chip = me // 2
    core = me % 2

    load_c = pltpu.make_async_copy(c_hbm, c_vm, c_sem)
    load_c.start()

    def load_row(p):
        return pltpu.make_async_copy(a_hbm.at[p], a_vm.at[p], a_sem.at[p])

    load_row(0).start()

    barrier = pltpu.get_barrier_semaphore()
    for k in range(1, DEV):
        pl.semaphore_signal(barrier, inc=1, device_id={"dev": (me + k) % DEV}, device_id_type=pl.DeviceIdType.MESH)

    load_c.wait()
    c = c_vm[...]
    spread = (iota((8 * N, N), 0) // 8 == iota((8 * N, N), 1)).astype(BF16)
    nt = (((1,), (1,)), ((), ()))
    rows = lax.dot_general(spread, c, nt, preferred_element_type=F32)
    wide = (8 * N, 8 * N)
    pair = jnp.concatenate([rows, rows], axis=1)
    tiled = jnp.concatenate([pair] * 4, axis=1)
    l_vm[...] = jnp.where(iota(wide, 0) % 8 == iota(wide, 1) // N, tiled, 0.0).astype(BF16)
    cf = c.astype(F32)
    cpair = jnp.concatenate([cf, cf], axis=1)
    c4 = jnp.concatenate([cpair, cpair], axis=1)
    c44 = jnp.concatenate([c4] * 4, axis=0)
    quad = (4 * N, 4 * N)
    b4_vm[...] = jnp.where(iota(quad, 0) // N == iota(quad, 1) // N, c44, 0.0).astype(BF16)

    pl.semaphore_wait(barrier, DEV - 1)

    def block(p, dest):
        return pltpu.make_async_remote_copy(
            src_ref=send.at[dest, p],
            dst_ref=recv.at[me, p],
            send_sem=send_sem.at[dest, p],
            recv_sem=recv_sem.at[me, p],
            device_id={"dev": dest},
            device_id_type=pl.DeviceIdType.MESH,
        )

    low = iota((32, 8, 128), 2) < N

    def half_row(p, h):
        a = a_vm[p, pl.ds(32 * h, 32)].reshape(4, 8 * N, N)
        left = jnp.concatenate([a[0], a[1]], axis=1)
        right = jnp.concatenate([a[2], a[3]], axis=1)
        a4 = jnp.concatenate([left, right], axis=1)
        t_one = jnp.dot(l_vm[...], a4, preferred_element_type=F32).astype(BF16)
        half = jnp.dot(t_one, b4_vm[...], preferred_element_type=F32)
        pairs = half.reshape(32, 2, 8, 256)
        for t in range(2):
            even = pairs[:, 0, :, 128 * t:128 * t + 128]
            odd = pairs[:, 1, :, 128 * t:128 * t + 128]
            first = jnp.where(low, even, pltpu.roll(odd, N, 2))
            second = jnp.where(low, pltpu.roll(even, N, 2), odd)
            both = jnp.concatenate([first, second], axis=1).astype(BF16)
            for jp in range(32):
                send[jp // 4, p, pl.ds(32 * h + 16 * t, 16), pl.ds(128 * (jp % 4), 128)] = both[jp]

    is_edge = jnp.logical_or(chip == 0, chip == 3)
    inward = jnp.where(chip < 2, 1, -1)
    partner = 2 * chip + 1 - core
    near = chip + inward
    far = chip + 2 * inward
    last = chip + 3 * inward
    outward = chip - inward
    beside = jnp.where(is_edge, near, outward)

    def make_row(p, carry):
        load_row(p).wait()

        @pl.when(p == 0)
        def _():
            for later in range(1, ROWS):
                load_row(later).start()

        for h in range(2):
            half_row(p, h)
        for k in range(2):
            block(p, 2 * beside + k).start()

        @pl.when(jnp.logical_not(is_edge))
        def _():
            for k in range(2):
                block(p, 2 * far + k).start()

        block(p, partner).start()
        return carry

    lax.fori_loop(0, ROWS, make_row, 0)

    @pl.when(is_edge)
    def _():
        for other in (far, last):
            def far_row(p, carry):
                for k in range(2):
                    block(p, 2 * other + k).start()
                return carry

            lax.fori_loop(0, ROWS, far_row, 0)

    for side, dest in ((0, 2 * near + core), (1, 2 * near + 1 - core)):
        for chunk in range(CHUNKS):
            near_refs[side * CHUNKS + chunk][...] = send[dest, :, :, pl.ds(128 * chunk, 128)]

    c = c_vm[...]
    rows = lax.dot_general(spread, c, nt, preferred_element_type=F32)
    widen = (iota((N, 8 * N), 0) == iota((N, 8 * N), 1) // 8).astype(BF16)
    full = jnp.dot(rows.astype(BF16), widen, preferred_element_type=F32)
    l4_ref[...] = jnp.where(iota(wide, 0) % 8 == iota(wide, 1) % 8, full, 0.0).astype(BF16)
    l4n_ref[...] = l4_ref[:, pl.ds(pl.multiple_of(128 * near, 128), 128)]
    eye = (iota((N, N), 0) == iota((N, N), 1)).astype(BF16)
    ct_vm[...] = lax.dot_general(eye, c, nt, preferred_element_type=F32).astype(BF16)
    ct_ref[...] = ct_vm[...]

    def third(src, p, first, second):
        g0 = jnp.dot(ct_vm[...], first, preferred_element_type=F32).reshape(8, 8, COLS)
        g1 = jnp.dot(ct_vm[...], second, preferred_element_type=F32).reshape(8, 8, COLS)
        at = pl.multiple_of(N * src + 8 * p, 16)
        g_ref[:, pl.ds(at, 16), :] = jnp.concatenate([g0, g1], axis=1).astype(BF16)

    def own(t, carry):
        third(me, 2 * t, send[me, 2 * t], send[me, 2 * t + 1])
        return carry

    lax.fori_loop(0, ROWS // 2, own, 0)

    def arrived(src, p):
        pltpu.make_async_remote_copy(
            src_ref=send.at[src, p],
            dst_ref=recv.at[src, p],
            send_sem=send_sem.at[src, p],
            recv_sem=recv_sem.at[src, p],
            device_id={"dev": src},
            device_id_type=pl.DeviceIdType.MESH,
        ).wait_recv()

    def take(sources):
        def body(t, carry):
            for src in sources:
                arrived(src, 2 * t)
                arrived(src, 2 * t + 1)
                third(src, 2 * t, recv[src, 2 * t], recv[src, 2 * t + 1])
            return carry

        lax.fori_loop(0, ROWS // 2, body, 0)

    take([partner])

    @pl.when(jnp.logical_not(is_edge))
    def _():
        g_ref[:, pl.ds(pl.multiple_of(2 * N * near, 16), 2 * N), :] = jnp.zeros((8, 2 * N, COLS), BF16)

    take([2 * beside, 2 * beside + 1])
    take([2 * far, 2 * far + 1])

    @pl.when(is_edge)
    def _():
        take([2 * last, 2 * last + 1])

    def sent_row(p, carry):
        block(p, partner).wait_send()
        for other in (beside, far):
            for k in range(2):
                block(p, 2 * other + k).wait_send()

        @pl.when(is_edge)
        def _():
            for k in range(2):
                block(p, 2 * last + k).wait_send()

        return carry

    lax.fori_loop(0, ROWS, sent_row, 0)


def most_kernel(g_ref, l4_ref, v_ref):
    for ag in range(8):
        v_ref[ag] = jnp.dot(l4_ref[...], g_ref[ag], preferred_element_type=F32)


def chunk_kernel(chunk, same_ref, other_ref, ct_ref, l4n_ref, most_ref, *refs):
    v_hbm, g_vm, v_vm, v_sem = refs[-4:]
    core = lax.axis_index("dev") % 2
    for side, ref in ((core, same_ref), (1 - core, other_ref)):
        for p in range(0, ROWS, 2):
            g0 = jnp.dot(ct_ref[...], ref[p], preferred_element_type=F32).reshape(8, 8, 128)
            g1 = jnp.dot(ct_ref[...], ref[p + 1], preferred_element_type=F32).reshape(8, 8, 128)
            at = pl.multiple_of(N * side + 8 * p, 16)
            g_vm[:, pl.ds(at, 16), :] = jnp.concatenate([g0, g1], axis=1).astype(BF16)

    def put(ag):
        return pltpu.make_async_copy(v_vm.at[ag], v_hbm.at[:, pl.ds(8 * ag, 8), pl.ds(128 * chunk, 128)], v_sem.at[ag])

    for ag in range(8):
        part = jnp.dot(l4n_ref[...], g_vm[ag], preferred_element_type=F32)
        v_vm[ag] = (part + most_ref[ag, :, 128 * chunk:128 * chunk + 128]).reshape(N, 8, 128)
        put(ag).start()
    for ag in range(8):
        put(ag).wait()


def solution(mesh):
    def local_transform(ao_rows, coeffs):
        vmem = pl.BlockSpec(memory_space=pltpu.VMEM)
        anywhere = pl.BlockSpec(memory_space=pltpu.HBM)
        sds = jax.ShapeDtypeStruct
        outs = (
            sds((8, 8 * N, COLS), BF16),
            sds((8 * N, 8 * N), BF16),
            sds((8 * N, 2 * N), BF16),
            sds((N, N), BF16),
        ) + (sds((ROWS, N, 128), BF16),) * (2 * CHUNKS)
        g, l4, l4n, ct, *near = pl.pallas_call(
            exchange_kernel,
            out_shape=outs,
            in_specs=[anywhere, anywhere],
            out_specs=(vmem,) * len(outs),
            scratch_shapes=[
                pltpu.VMEM((ROWS, N, N, N), BF16),
                pltpu.VMEM((N, N), BF16),
                pltpu.VMEM((8 * N, 8 * N), BF16),
                pltpu.VMEM((4 * N, 4 * N), BF16),
                pltpu.VMEM((N, N), BF16),
                pltpu.VMEM((DEV, ROWS, N, COLS), BF16),
                pltpu.VMEM((DEV, ROWS, N, COLS), BF16),
                pltpu.SemaphoreType.DMA((ROWS,)),
                pltpu.SemaphoreType.DMA,
                pltpu.SemaphoreType.DMA((DEV, ROWS)),
                pltpu.SemaphoreType.DMA((DEV, ROWS)),
            ],
            compiler_params=pltpu.CompilerParams(collective_id=0, has_side_effects=True, vmem_limit_bytes=40 * 2**20),
            name="exchange",
        )(pltpu.with_memory_space_constraint(ao_rows, pltpu.HBM), pltpu.with_memory_space_constraint(coeffs, pltpu.HBM))
        same = [(2, 4), (3, 5), (4, 2), (5, 3)]
        other = [(2, 5), (3, 4), (4, 3), (5, 2)]
        arrived = []
        for chunk in range(CHUNKS):
            pair = []
            for side, perm in enumerate((same, other)):
                pair.append(lax.ppermute(near[side * CHUNKS + chunk], "dev", perm))
            arrived.append(pair)
        most = pl.pallas_call(
            most_kernel,
            out_shape=sds((8, 8 * N, COLS), F32),
            in_specs=[vmem, vmem],
            out_specs=vmem,
            compiler_params=pltpu.CompilerParams(vmem_limit_bytes=12 * 2**20),
            cost_estimate=pl.CostEstimate(flops=2 * 8 * 512**3, bytes_accessed=12 * 2**20, transcendentals=0),
            name="most",
        )(g, l4)
        v = None
        for chunk in range(CHUNKS):
            operands = (*arrived[chunk], ct, l4n, most) + (() if v is None else (v,))
            v = pl.pallas_call(
                functools.partial(chunk_kernel, chunk),
                out_shape=sds((N, N, COLS), F32),
                in_specs=[vmem] * 5 + ([] if v is None else [anywhere]),
                out_specs=anywhere,
                scratch_shapes=[
                    pltpu.VMEM((8, 2 * N, 128), BF16),
                    pltpu.VMEM((8, N, 8, 128), F32),
                    pltpu.SemaphoreType.DMA((8,)),
                ],
                input_output_aliases={} if v is None else {5: 0},
                compiler_params=pltpu.CompilerParams(vmem_limit_bytes=12 * 2**20),
                cost_estimate=pl.CostEstimate(flops=2 * 8 * 512 * 128 * 128, bytes_accessed=4 * 2**20, transcendentals=0),
            )(*operands)
        return v

    return jax.shard_map(local_transform, mesh=mesh, in_specs=(P(('frag', 'dev')), P('frag')), out_specs=P('frag', None, 'dev'), check_vma=False)
```

```python
import functools

import jax
import jax.numpy as jnp
from jax import lax
from jax.experimental import pallas as pl
from jax.experimental.pallas import tpu as pltpu
from jax.sharding import PartitionSpec as P


N = 64
DEV = 8
ROWS = N // DEV
COLS = N * N // DEV
CHUNKS = COLS // 128
BF16 = jnp.bfloat16
F32 = jnp.float32


def iota(shape, dim):
    return lax.broadcasted_iota(jnp.int32, shape, dim)


def exchange_kernel(a_hbm, c_hbm, g_ref, l4_ref, l4n_ref, ct_ref, *refs):
    near_refs = refs[:2 * CHUNKS]
    a_vm, c_vm, l_vm, b4_vm, ct_vm, send, recv, a_sem, c_sem, send_sem, recv_sem = refs[2 * CHUNKS:]
    me = lax.axis_index("dev")
    chip = me // 2
    core = me % 2

    load_c = pltpu.make_async_copy(c_hbm, c_vm, c_sem)
    load_c.start()

    def load_row(p):
        return pltpu.make_async_copy(a_hbm.at[p], a_vm.at[p], a_sem.at[p])

    def load_half(h):
        half = pl.ds(32 * h, 32)
        return pltpu.make_async_copy(a_hbm.at[0, half], a_vm.at[0, half], a_sem.at[ROWS * h])

    for h in range(2):
        load_half(h).start()

    barrier = pltpu.get_barrier_semaphore()
    for k in range(1, DEV):
        pl.semaphore_signal(barrier, inc=1, device_id={"dev": (me + k) % DEV}, device_id_type=pl.DeviceIdType.MESH)

    load_c.wait()
    c = c_vm[...]
    spread = (iota((8 * N, N), 0) // 8 == iota((8 * N, N), 1)).astype(BF16)
    nt = (((1,), (1,)), ((), ()))
    rows = lax.dot_general(spread, c, nt, preferred_element_type=F32)
    wide = (8 * N, 8 * N)
    pair = jnp.concatenate([rows, rows], axis=1)
    tiled = jnp.concatenate([pair] * 4, axis=1)
    l_vm[...] = jnp.where(iota(wide, 0) % 8 == iota(wide, 1) // N, tiled, 0.0).astype(BF16)
    cf = c.astype(F32)
    cpair = jnp.concatenate([cf, cf], axis=1)
    c4 = jnp.concatenate([cpair, cpair], axis=1)
    c44 = jnp.concatenate([c4] * 4, axis=0)
    quad = (4 * N, 4 * N)
    b4_vm[...] = jnp.where(iota(quad, 0) // N == iota(quad, 1) // N, c44, 0.0).astype(BF16)

    pl.semaphore_wait(barrier, DEV - 1)

    def block(p, dest):
        return pltpu.make_async_remote_copy(
            src_ref=send.at[dest, p],
            dst_ref=recv.at[me, p],
            send_sem=send_sem.at[dest, p],
            recv_sem=recv_sem.at[me, p],
            device_id={"dev": dest},
            device_id_type=pl.DeviceIdType.MESH,
        )

    low = iota((32, 8, 128), 2) < N

    def pieces(p, h, first, count, put):
        a = a_vm[p, pl.ds(32 * h, 32)].reshape(4, 8 * N, N)
        left = jnp.concatenate([a[0], a[1]], axis=1)
        right = jnp.concatenate([a[2], a[3]], axis=1)
        a4 = jnp.concatenate([left, right], axis=1)
        lhs = l_vm[pl.ds(first, 16 * count), :]
        t_one = jnp.dot(lhs, a4, preferred_element_type=F32).astype(BF16)
        half = jnp.dot(t_one, b4_vm[...], preferred_element_type=F32)
        pairs = half.reshape(count, 2, 8, 256)
        for t in range(2):
            even = pairs[:, 0, :, 128 * t:128 * t + 128]
            odd = pairs[:, 1, :, 128 * t:128 * t + 128]
            first_rows = jnp.where(low[:count], even, pltpu.roll(odd, N, 2))
            second_rows = jnp.where(low[:count], pltpu.roll(even, N, 2), odd)
            both = jnp.concatenate([first_rows, second_rows], axis=1).astype(BF16)
            for jp in range(count):
                put(jp // 4, pl.ds(32 * h + 16 * t, 16), pl.ds(128 * (jp % 4), 128), both[jp])

    def half_row(p, h):
        def put(dest, q, columns, value):
            send[dest, p, q, columns] = value

        pieces(p, h, 0, 32, put)

    def chip_piece(to):
        def put(dest, q, columns, value):
            send[2 * to + dest, 0, q, columns] = value

        for h in range(2):
            pieces(0, h, pl.multiple_of(128 * to, 128), 8, put)

    is_edge = jnp.logical_or(chip == 0, chip == 3)
    inward = jnp.where(chip < 2, 1, -1)
    partner = 2 * chip + 1 - core
    near = chip + inward
    far = chip + 2 * inward
    last = chip + 3 * inward
    outward = chip - inward
    beside = jnp.where(is_edge, near, outward)

    for h in range(2):
        load_half(h).wait()
    for later in range(1, ROWS):
        load_row(later).start()
    chip_piece(jnp.where(is_edge, near, far))
    for k in range(2):
        block(0, 2 * jnp.where(is_edge, near, far) + k).start()
    chip_piece(jnp.where(is_edge, far, outward))

    @pl.when(jnp.logical_not(is_edge))
    def _():
        for k in range(2):
            block(0, 2 * outward + k).start()

    chip_piece(jnp.where(is_edge, last, near))
    chip_piece(chip)
    block(0, partner).start()

    def make_row(p, carry):
        load_row(p).wait()
        for h in range(2):
            half_row(p, h)
        for k in range(2):
            block(p, 2 * beside + k).start()

        @pl.when(jnp.logical_not(is_edge))
        def _():
            for k in range(2):
                block(p, 2 * far + k).start()

        block(p, partner).start()
        return carry

    lax.fori_loop(1, ROWS, make_row, 0)

    @pl.when(is_edge)
    def _():
        for other in (far, last):
            def far_row(p, carry):
                for k in range(2):
                    block(p, 2 * other + k).start()
                return carry

            lax.fori_loop(0, ROWS, far_row, 0)

    for side, dest in ((0, 2 * near + core), (1, 2 * near + 1 - core)):
        for chunk in range(CHUNKS):
            near_refs[side * CHUNKS + chunk][...] = send[dest, :, :, pl.ds(128 * chunk, 128)]

    c = c_vm[...]
    rows = lax.dot_general(spread, c, nt, preferred_element_type=F32)
    widen = (iota((N, 8 * N), 0) == iota((N, 8 * N), 1) // 8).astype(BF16)
    full = jnp.dot(rows.astype(BF16), widen, preferred_element_type=F32)
    l4_ref[...] = jnp.where(iota(wide, 0) % 8 == iota(wide, 1) % 8, full, 0.0).astype(BF16)
    l4n_ref[...] = l4_ref[:, pl.ds(pl.multiple_of(128 * near, 128), 128)]
    eye = (iota((N, N), 0) == iota((N, N), 1)).astype(BF16)
    ct_vm[...] = lax.dot_general(eye, c, nt, preferred_element_type=F32).astype(BF16)
    ct_ref[...] = ct_vm[...]

    def third(src, p, first, second):
        g0 = jnp.dot(ct_vm[...], first, preferred_element_type=F32).reshape(8, 8, COLS)
        g1 = jnp.dot(ct_vm[...], second, preferred_element_type=F32).reshape(8, 8, COLS)
        at = pl.multiple_of(N * src + 8 * p, 16)
        g_ref[:, pl.ds(at, 16), :] = jnp.concatenate([g0, g1], axis=1).astype(BF16)

    def own(t, carry):
        third(me, 2 * t, send[me, 2 * t], send[me, 2 * t + 1])
        return carry

    lax.fori_loop(0, ROWS // 2, own, 0)

    def arrived(src, p):
        pltpu.make_async_remote_copy(
            src_ref=send.at[src, p],
            dst_ref=recv.at[src, p],
            send_sem=send_sem.at[src, p],
            recv_sem=recv_sem.at[src, p],
            device_id={"dev": src},
            device_id_type=pl.DeviceIdType.MESH,
        ).wait_recv()

    def take(sources):
        def body(t, carry):
            for src in sources:
                arrived(src, 2 * t)
                arrived(src, 2 * t + 1)
                third(src, 2 * t, recv[src, 2 * t], recv[src, 2 * t + 1])
            return carry

        lax.fori_loop(0, ROWS // 2, body, 0)

    take([partner])

    @pl.when(jnp.logical_not(is_edge))
    def _():
        g_ref[:, pl.ds(pl.multiple_of(2 * N * near, 16), 2 * N), :] = jnp.zeros((8, 2 * N, COLS), BF16)

    take([2 * beside, 2 * beside + 1])
    take([2 * far, 2 * far + 1])

    @pl.when(is_edge)
    def _():
        take([2 * last, 2 * last + 1])

    def sent_row(p, carry):
        block(p, partner).wait_send()
        for other in (beside, far):
            for k in range(2):
                block(p, 2 * other + k).wait_send()

        @pl.when(is_edge)
        def _():
            for k in range(2):
                block(p, 2 * last + k).wait_send()

        return carry

    lax.fori_loop(0, ROWS, sent_row, 0)


def most_kernel(g_ref, l4_ref, v_ref):
    for ag in range(8):
        v_ref[ag] = jnp.dot(l4_ref[...], g_ref[ag], preferred_element_type=F32)


def chunk_kernel(chunk, same_ref, other_ref, ct_ref, l4n_ref, most_ref, *refs):
    v_hbm, g_vm, v_vm, v_sem = refs[-4:]
    core = lax.axis_index("dev") % 2
    for side, ref in ((core, same_ref), (1 - core, other_ref)):
        for p in range(0, ROWS, 2):
            both = jnp.concatenate([ref[p], ref[p + 1]], axis=1)
            g = jnp.dot(ct_ref[...], both, preferred_element_type=F32)
            g0 = g[:, :128].reshape(8, 8, 128)
            g1 = g[:, 128:].reshape(8, 8, 128)
            g = jnp.concatenate([g0, g1], axis=1).astype(BF16)
            at = pl.multiple_of(N * side + 8 * p, 16)
            for ag in range(8):
                g_vm[pl.ds(at, 16), 128 * ag:128 * ag + 128] = g[ag]

    def put(ag):
        return pltpu.make_async_copy(v_vm.at[ag], v_hbm.at[:, pl.ds(8 * ag, 8), pl.ds(128 * chunk, 128)], v_sem.at[ag])

    for pair in range(4):
        part = jnp.dot(l4n_ref[...], g_vm[:, 256 * pair:256 * pair + 256], preferred_element_type=F32)
        for k in range(2):
            ag = 2 * pair + k
            v_vm[ag] = (part[:, 128 * k:128 * k + 128] + most_ref[ag, :, 128 * chunk:128 * chunk + 128]).reshape(N, 8, 128)
            put(ag).start()
    for ag in range(8):
        put(ag).wait()


def solution(mesh):
    def local_transform(ao_rows, coeffs):
        vmem = pl.BlockSpec(memory_space=pltpu.VMEM)
        anywhere = pl.BlockSpec(memory_space=pltpu.HBM)
        sds = jax.ShapeDtypeStruct
        outs = (
            sds((8, 8 * N, COLS), BF16),
            sds((8 * N, 8 * N), BF16),
            sds((8 * N, 2 * N), BF16),
            sds((N, N), BF16),
        ) + (sds((ROWS, N, 128), BF16),) * (2 * CHUNKS)
        g, l4, l4n, ct, *near = pl.pallas_call(
            exchange_kernel,
            out_shape=outs,
            in_specs=[anywhere, anywhere],
            out_specs=(vmem,) * len(outs),
            scratch_shapes=[
                pltpu.VMEM((ROWS, N, N, N), BF16),
                pltpu.VMEM((N, N), BF16),
                pltpu.VMEM((8 * N, 8 * N), BF16),
                pltpu.VMEM((4 * N, 4 * N), BF16),
                pltpu.VMEM((N, N), BF16),
                pltpu.VMEM((DEV, ROWS, N, COLS), BF16),
                pltpu.VMEM((DEV, ROWS, N, COLS), BF16),
                pltpu.SemaphoreType.DMA((ROWS + 1,)),
                pltpu.SemaphoreType.DMA,
                pltpu.SemaphoreType.DMA((DEV, ROWS)),
                pltpu.SemaphoreType.DMA((DEV, ROWS)),
            ],
            compiler_params=pltpu.CompilerParams(collective_id=0, has_side_effects=True, vmem_limit_bytes=40 * 2**20),
            name="exchange",
        )(pltpu.with_memory_space_constraint(ao_rows, pltpu.HBM), pltpu.with_memory_space_constraint(coeffs, pltpu.HBM))
        same = [(2, 4), (3, 5), (4, 2), (5, 3)]
        other = [(2, 5), (3, 4), (4, 3), (5, 2)]
        arrived = []
        for chunk in range(CHUNKS):
            pair = []
            for side, perm in enumerate((same, other)):
                pair.append(lax.ppermute(near[side * CHUNKS + chunk], "dev", perm))
            arrived.append(pair)
        most = pl.pallas_call(
            most_kernel,
            out_shape=sds((8, 8 * N, COLS), F32),
            in_specs=[vmem, vmem],
            out_specs=vmem,
            compiler_params=pltpu.CompilerParams(vmem_limit_bytes=12 * 2**20),
            cost_estimate=pl.CostEstimate(flops=2 * 8 * 512**3, bytes_accessed=12 * 2**20, transcendentals=0),
            name="most",
        )(g, l4)
        v = None
        for chunk in range(CHUNKS):
            operands = (*arrived[chunk], ct, l4n, most) + (() if v is None else (v,))
            v = pl.pallas_call(
                functools.partial(chunk_kernel, chunk),
                out_shape=sds((N, N, COLS), F32),
                in_specs=[vmem] * 5 + ([] if v is None else [anywhere]),
                out_specs=anywhere,
                scratch_shapes=[
                    pltpu.VMEM((2 * N, 8 * 128), BF16),
                    pltpu.VMEM((8, N, 8, 128), F32),
                    pltpu.SemaphoreType.DMA((8,)),
                ],
                input_output_aliases={} if v is None else {5: 0},
                compiler_params=pltpu.CompilerParams(vmem_limit_bytes=12 * 2**20),
                cost_estimate=pl.CostEstimate(flops=2 * 8 * 512 * 128 * 128, bytes_accessed=4 * 2**20, transcendentals=0),
            )(*operands)
        return v

    return jax.shard_map(local_transform, mesh=mesh, in_specs=(P(('frag', 'dev')), P('frag')), out_specs=P('frag', None, 'dev'), check_vma=False)
```

```python
import functools

import jax
import jax.numpy as jnp
from jax import lax
from jax.experimental import pallas as pl
from jax.experimental.pallas import tpu as pltpu
from jax.sharding import PartitionSpec as P


N = 64
DEV = 8
ROWS = N // DEV
COLS = N * N // DEV
CHUNKS = COLS // 128
EARLY = ((0, 1), (1, 1), (2, 2), (4, 4))
LATER = ((0, 4), (4, 4))
WHOLE = ((0, 8),)
BF16 = jnp.bfloat16
F32 = jnp.float32


def iota(shape, dim):
    return lax.broadcasted_iota(jnp.int32, shape, dim)


def exchange_kernel(a_hbm, c_hbm, g_ref, l4_ref, l4n_ref, ct_ref, *refs):
    near_refs = refs[:2 * CHUNKS]
    a_vm, c_vm, l_vm, b4_vm, ct_vm, send, recv, a_sem, c_sem, send_sem, recv_sem = refs[2 * CHUNKS:]
    me = lax.axis_index("dev")
    chip = me // 2
    core = me % 2

    load_c = pltpu.make_async_copy(c_hbm, c_vm, c_sem)
    load_c.start()

    def load_row(p):
        return pltpu.make_async_copy(a_hbm.at[p], a_vm.at[p], a_sem.at[p])

    def load_half(h):
        half = pl.ds(32 * h, 32)
        return pltpu.make_async_copy(a_hbm.at[0, half], a_vm.at[0, half], a_sem.at[ROWS * h])

    for h in range(2):
        load_half(h).start()

    barrier = pltpu.get_barrier_semaphore()
    for k in range(1, DEV):
        pl.semaphore_signal(barrier, inc=1, device_id={"dev": (me + k) % DEV}, device_id_type=pl.DeviceIdType.MESH)

    load_c.wait()
    c = c_vm[...]
    spread = (iota((8 * N, N), 0) // 8 == iota((8 * N, N), 1)).astype(BF16)
    nt = (((1,), (1,)), ((), ()))
    rows = lax.dot_general(spread, c, nt, preferred_element_type=F32)
    wide = (8 * N, 8 * N)
    pair = jnp.concatenate([rows, rows], axis=1)
    tiled = jnp.concatenate([pair] * 4, axis=1)
    l_vm[...] = jnp.where(iota(wide, 0) % 8 == iota(wide, 1) // N, tiled, 0.0).astype(BF16)
    cf = c.astype(F32)
    cpair = jnp.concatenate([cf, cf], axis=1)
    c4 = jnp.concatenate([cpair, cpair], axis=1)
    c44 = jnp.concatenate([c4] * 4, axis=0)
    quad = (4 * N, 4 * N)
    b4_vm[...] = jnp.where(iota(quad, 0) // N == iota(quad, 1) // N, c44, 0.0).astype(BF16)

    pl.semaphore_wait(barrier, DEV - 1)

    def group(rows, dest, src):
        part = pl.ds(*rows)
        return pltpu.make_async_remote_copy(
            src_ref=send.at[dest, part],
            dst_ref=recv.at[src, part],
            send_sem=send_sem.at[dest, rows[0]],
            recv_sem=recv_sem.at[src, rows[0]],
            device_id={"dev": dest},
            device_id_type=pl.DeviceIdType.MESH,
        )

    def start(rows, to):
        for k in range(2):
            group(rows, 2 * to + k, me).start()

    def sent(groups, to):
        for rows in groups:
            for k in range(2):
                group(rows, 2 * to + k, me).wait_send()

    low = iota((32, 8, 128), 2) < N

    def pieces(p, h, first, count, put):
        a = a_vm[p, pl.ds(32 * h, 32)].reshape(4, 8 * N, N)
        left = jnp.concatenate([a[0], a[1]], axis=1)
        right = jnp.concatenate([a[2], a[3]], axis=1)
        a4 = jnp.concatenate([left, right], axis=1)
        lhs = l_vm[pl.ds(first, 16 * count), :]
        t_one = jnp.dot(lhs, a4, preferred_element_type=F32).astype(BF16)
        half = jnp.dot(t_one, b4_vm[...], preferred_element_type=F32)
        pairs = half.reshape(count, 2, 8, 256)
        for t in range(2):
            even = pairs[:, 0, :, 128 * t:128 * t + 128]
            odd = pairs[:, 1, :, 128 * t:128 * t + 128]
            first_rows = jnp.where(low[:count], even, pltpu.roll(odd, N, 2))
            second_rows = jnp.where(low[:count], pltpu.roll(even, N, 2), odd)
            both = jnp.concatenate([first_rows, second_rows], axis=1).astype(BF16)
            for jp in range(count):
                put(jp // 4, pl.ds(32 * h + 16 * t, 16), pl.ds(128 * (jp % 4), 128), both[jp])

    def half_row(p, h):
        def put(dest, q, columns, value):
            send[dest, p, q, columns] = value

        pieces(p, h, 0, 32, put)

    def chip_piece(to):
        def put(dest, q, columns, value):
            send[2 * to + dest, 0, q, columns] = value

        for h in range(2):
            pieces(0, h, pl.multiple_of(128 * to, 128), 8, put)

    is_edge = jnp.logical_or(chip == 0, chip == 3)
    inward = jnp.where(chip < 2, 1, -1)
    partner = 2 * chip + 1 - core
    near = chip + inward
    far = chip + 2 * inward
    last = chip + 3 * inward
    outward = chip - inward
    beside = jnp.where(is_edge, near, outward)

    for h in range(2):
        load_half(h).wait()
    for later in range(1, ROWS):
        load_row(later).start()
    chip_piece(jnp.where(is_edge, near, far))
    start(EARLY[0], jnp.where(is_edge, near, far))
    chip_piece(jnp.where(is_edge, far, outward))

    @pl.when(jnp.logical_not(is_edge))
    def _():
        start(EARLY[0], outward)

    chip_piece(jnp.where(is_edge, last, near))
    chip_piece(chip)
    group(EARLY[0], partner, me).start()

    def make_row(p, carry):
        load_row(p).wait()
        for h in range(2):
            half_row(p, h)
        for rows in EARLY[1:]:
            @pl.when(p == sum(rows) - 1)
            def _():
                start(rows, beside)

                @pl.when(jnp.logical_not(is_edge))
                def _():
                    start(rows, far)

                group(rows, partner, me).start()

        return carry

    lax.fori_loop(1, ROWS, make_row, 0)

    @pl.when(is_edge)
    def _():
        for rows in LATER:
            start(rows, far)
        for rows in WHOLE:
            start(rows, last)

    for side, dest in ((0, 2 * near + core), (1, 2 * near + 1 - core)):
        for chunk in range(CHUNKS):
            near_refs[side * CHUNKS + chunk][...] = send[dest, :, :, pl.ds(128 * chunk, 128)]

    c = c_vm[...]
    rows = lax.dot_general(spread, c, nt, preferred_element_type=F32)
    widen = (iota((N, 8 * N), 0) == iota((N, 8 * N), 1) // 8).astype(BF16)
    full = jnp.dot(rows.astype(BF16), widen, preferred_element_type=F32)
    l4_ref[...] = jnp.where(iota(wide, 0) % 8 == iota(wide, 1) % 8, full, 0.0).astype(BF16)
    l4n_ref[...] = l4_ref[:, pl.ds(pl.multiple_of(128 * near, 128), 128)]
    eye = (iota((N, N), 0) == iota((N, N), 1)).astype(BF16)
    ct_vm[...] = lax.dot_general(eye, c, nt, preferred_element_type=F32).astype(BF16)
    ct_ref[...] = ct_vm[...]

    def third(src, p, first, second):
        g0 = jnp.dot(ct_vm[...], first, preferred_element_type=F32).reshape(8, 8, COLS)
        g1 = jnp.dot(ct_vm[...], second, preferred_element_type=F32).reshape(8, 8, COLS)
        at = pl.multiple_of(N * src + 8 * p, 16)
        g_ref[:, pl.ds(at, 16), :] = jnp.concatenate([g0, g1], axis=1).astype(BF16)

    def own(t, carry):
        third(me, 2 * t, send[me, 2 * t], send[me, 2 * t + 1])
        return carry

    lax.fori_loop(0, ROWS // 2, own, 0)

    def take(groups, sources):
        for rows in groups:
            for src in sources:
                group(rows, src, src).wait_recv()
            if sum(rows) % 2 == 0:
                begin = rows[0] // 2 * 2

                def body(t, carry):
                    for src in sources:
                        p = begin + 2 * t
                        third(src, p, recv[src, p], recv[src, p + 1])
                    return carry

                lax.fori_loop(0, (sum(rows) - begin) // 2, body, 0)

    take(EARLY, [partner])

    @pl.when(jnp.logical_not(is_edge))
    def _():
        g_ref[:, pl.ds(pl.multiple_of(2 * N * near, 16), 2 * N), :] = jnp.zeros((8, 2 * N, COLS), BF16)

    take(EARLY, [2 * beside, 2 * beside + 1])

    for rows in EARLY:
        group(rows, partner, me).wait_send()
    sent(EARLY, beside)

    @pl.when(is_edge)
    def _():
        take(EARLY, [2 * far, 2 * far + 1])
        take(WHOLE, [2 * last, 2 * last + 1])
        sent(LATER, far)
        sent(WHOLE, last)

    @pl.when(jnp.logical_not(is_edge))
    def _():
        take(LATER, [2 * far, 2 * far + 1])
        sent(EARLY, far)


def most_kernel(g_ref, l4_ref, v_ref):
    for ag in range(8):
        v_ref[ag] = jnp.dot(l4_ref[...], g_ref[ag], preferred_element_type=F32)


def chunk_kernel(chunk, same_ref, other_ref, ct_ref, l4n_ref, most_ref, *refs):
    v_hbm, g_vm, v_vm, v_sem = refs[-4:]
    core = lax.axis_index("dev") % 2
    for side, ref in ((core, same_ref), (1 - core, other_ref)):
        for p in range(0, ROWS, 2):
            g0 = jnp.dot(ct_ref[...], ref[p], preferred_element_type=F32).reshape(8, 8, 128)
            g1 = jnp.dot(ct_ref[...], ref[p + 1], preferred_element_type=F32).reshape(8, 8, 128)
            at = pl.multiple_of(N * side + 8 * p, 16)
            g_vm[:, pl.ds(at, 16), :] = jnp.concatenate([g0, g1], axis=1).astype(BF16)

    def put(ag):
        return pltpu.make_async_copy(v_vm.at[ag], v_hbm.at[:, pl.ds(8 * ag, 8), pl.ds(128 * chunk, 128)], v_sem.at[ag])

    for ag in range(8):
        part = jnp.dot(l4n_ref[...], g_vm[ag], preferred_element_type=F32)
        v_vm[ag] = (part + most_ref[ag, :, 128 * chunk:128 * chunk + 128]).reshape(N, 8, 128)
        put(ag).start()
    for ag in range(8):
        put(ag).wait()


def solution(mesh):
    def local_transform(ao_rows, coeffs):
        vmem = pl.BlockSpec(memory_space=pltpu.VMEM)
        anywhere = pl.BlockSpec(memory_space=pltpu.HBM)
        sds = jax.ShapeDtypeStruct
        outs = (
            sds((8, 8 * N, COLS), BF16),
            sds((8 * N, 8 * N), BF16),
            sds((8 * N, 2 * N), BF16),
            sds((N, N), BF16),
        ) + (sds((ROWS, N, 128), BF16),) * (2 * CHUNKS)
        g, l4, l4n, ct, *near = pl.pallas_call(
            exchange_kernel,
            out_shape=outs,
            in_specs=[anywhere, anywhere],
            out_specs=(vmem,) * len(outs),
            scratch_shapes=[
                pltpu.VMEM((ROWS, N, N, N), BF16),
                pltpu.VMEM((N, N), BF16),
                pltpu.VMEM((8 * N, 8 * N), BF16),
                pltpu.VMEM((4 * N, 4 * N), BF16),
                pltpu.VMEM((N, N), BF16),
                pltpu.VMEM((DEV, ROWS, N, COLS), BF16),
                pltpu.VMEM((DEV, ROWS, N, COLS), BF16),
                pltpu.SemaphoreType.DMA((ROWS + 1,)),
                pltpu.SemaphoreType.DMA,
                pltpu.SemaphoreType.DMA((DEV, ROWS)),
                pltpu.SemaphoreType.DMA((DEV, ROWS)),
            ],
            compiler_params=pltpu.CompilerParams(collective_id=0, has_side_effects=True, vmem_limit_bytes=40 * 2**20),
            name="exchange",
        )(pltpu.with_memory_space_constraint(ao_rows, pltpu.HBM), pltpu.with_memory_space_constraint(coeffs, pltpu.HBM))
        same = [(2, 4), (3, 5), (4, 2), (5, 3)]
        other = [(2, 5), (3, 4), (4, 3), (5, 2)]
        arrived = []
        for chunk in range(CHUNKS):
            pair = []
            for side, perm in enumerate((same, other)):
                pair.append(lax.ppermute(near[side * CHUNKS + chunk], "dev", perm))
            arrived.append(pair)
        most = pl.pallas_call(
            most_kernel,
            out_shape=sds((8, 8 * N, COLS), F32),
            in_specs=[vmem, vmem],
            out_specs=vmem,
            compiler_params=pltpu.CompilerParams(vmem_limit_bytes=12 * 2**20),
            cost_estimate=pl.CostEstimate(flops=2 * 8 * 512**3, bytes_accessed=12 * 2**20, transcendentals=0),
            name="most",
        )(g, l4)
        v = None
        for chunk in range(CHUNKS):
            operands = (*arrived[chunk], ct, l4n, most) + (() if v is None else (v,))
            v = pl.pallas_call(
                functools.partial(chunk_kernel, chunk),
                out_shape=sds((N, N, COLS), F32),
                in_specs=[vmem] * 5 + ([] if v is None else [anywhere]),
                out_specs=anywhere,
                scratch_shapes=[
                    pltpu.VMEM((8, 2 * N, 128), BF16),
                    pltpu.VMEM((8, N, 8, 128), F32),
                    pltpu.SemaphoreType.DMA((8,)),
                ],
                input_output_aliases={} if v is None else {5: 0},
                compiler_params=pltpu.CompilerParams(vmem_limit_bytes=12 * 2**20),
                cost_estimate=pl.CostEstimate(flops=2 * 8 * 512 * 128 * 128, bytes_accessed=4 * 2**20, transcendentals=0),
            )(*operands)
        return v

    return jax.shard_map(local_transform, mesh=mesh, in_specs=(P(('frag', 'dev')), P('frag')), out_specs=P('frag', None, 'dev'), check_vma=False)
```

```python
import functools

import jax
import jax.numpy as jnp
from jax import lax
from jax.experimental import pallas as pl
from jax.experimental.pallas import tpu as pltpu
from jax.sharding import PartitionSpec as P


N = 64
DEV = 8
ROWS = N // DEV
COLS = N * N // DEV
CHUNKS = COLS // 128
EARLY = ((0, 1), (1, 1), (2, 2), (4, 4))
LATER = ((0, 4), (4, 4))
WHOLE = ((0, 8),)
BF16 = jnp.bfloat16
F32 = jnp.float32


def iota(shape, dim):
    return lax.broadcasted_iota(jnp.int32, shape, dim)


def exchange_kernel(a_hbm, c_hbm, g_ref, l4_ref, l4n_ref, ct_ref, *refs):
    near_refs = refs[:2 * CHUNKS]
    a_vm, c_vm, l_vm, b4_vm, ct_vm, send, recv, a_sem, c_sem, send_sem, recv_sem = refs[2 * CHUNKS:]
    me = lax.axis_index("dev")
    chip = me // 2
    core = me % 2

    load_c = pltpu.make_async_copy(c_hbm, c_vm, c_sem)
    load_c.start()

    def load_row(p):
        return pltpu.make_async_copy(a_hbm.at[p], a_vm.at[p], a_sem.at[p])

    def load_half(h):
        half = pl.ds(32 * h, 32)
        return pltpu.make_async_copy(a_hbm.at[0, half], a_vm.at[0, half], a_sem.at[ROWS * h])

    for h in range(2):
        load_half(h).start()

    barrier = pltpu.get_barrier_semaphore()
    for k in range(1, DEV):
        pl.semaphore_signal(barrier, inc=1, device_id={"dev": (me + k) % DEV}, device_id_type=pl.DeviceIdType.MESH)

    load_c.wait()
    c = c_vm[...]
    nt = (((1,), (1,)), ((), ()))
    wide = (8 * N, 8 * N)

    def kron_rows(first_m, count):
        spread = (iota((8 * count, N), 0) // 8 + first_m == iota((8 * count, N), 1)).astype(BF16)
        rows = lax.dot_general(spread, c, nt, preferred_element_type=F32)
        pair = jnp.concatenate([rows, rows], axis=1)
        tiled = jnp.concatenate([pair] * 4, axis=1)
        shape = (8 * count, 8 * N)
        return jnp.where(iota(shape, 0) % 8 == iota(shape, 1) // N, tiled, 0.0).astype(BF16)

    cf = c.astype(F32)
    cpair = jnp.concatenate([cf, cf], axis=1)
    c4 = jnp.concatenate([cpair, cpair], axis=1)
    c44 = jnp.concatenate([c4] * 4, axis=0)
    quad = (4 * N, 4 * N)
    b4_vm[...] = jnp.where(iota(quad, 0) // N == iota(quad, 1) // N, c44, 0.0).astype(BF16)

    def group(rows, dest, src):
        part = pl.ds(*rows)
        return pltpu.make_async_remote_copy(
            src_ref=send.at[dest, part],
            dst_ref=recv.at[src, part],
            send_sem=send_sem.at[dest, rows[0]],
            recv_sem=recv_sem.at[src, rows[0]],
            device_id={"dev": dest},
            device_id_type=pl.DeviceIdType.MESH,
        )

    def start(rows, to):
        for k in range(2):
            group(rows, 2 * to + k, me).start()

    def sent(groups, to):
        for rows in groups:
            for k in range(2):
                group(rows, 2 * to + k, me).wait_send()

    low = iota((32, 8, 128), 2) < N

    def pieces(p, h, lhs, count, put):
        a = a_vm[p, pl.ds(32 * h, 32)].reshape(4, 8 * N, N)
        left = jnp.concatenate([a[0], a[1]], axis=1)
        right = jnp.concatenate([a[2], a[3]], axis=1)
        a4 = jnp.concatenate([left, right], axis=1)
        t_one = jnp.dot(lhs, a4, preferred_element_type=F32).astype(BF16)
        half = jnp.dot(t_one, b4_vm[...], preferred_element_type=F32)
        pairs = half.reshape(count, 2, 8, 256)
        for t in range(2):
            even = pairs[:, 0, :, 128 * t:128 * t + 128]
            odd = pairs[:, 1, :, 128 * t:128 * t + 128]
            first_rows = jnp.where(low[:count], even, pltpu.roll(odd, N, 2))
            second_rows = jnp.where(low[:count], pltpu.roll(even, N, 2), odd)
            both = jnp.concatenate([first_rows, second_rows], axis=1).astype(BF16)
            for jp in range(count):
                put(jp // 4, pl.ds(32 * h + 16 * t, 16), pl.ds(128 * (jp % 4), 128), both[jp])

    def half_row(p, h):
        def put(dest, q, columns, value):
            send[dest, p, q, columns] = value

        pieces(p, h, l_vm[...], 32, put)

    def chip_piece(to, lhs):
        def put(dest, q, columns, value):
            send[2 * to + dest, 0, q, columns] = value

        for h in range(2):
            pieces(0, h, lhs, 8, put)

    is_edge = jnp.logical_or(chip == 0, chip == 3)
    inward = jnp.where(chip < 2, 1, -1)
    partner = 2 * chip + 1 - core
    near = chip + inward
    far = chip + 2 * inward
    last = chip + 3 * inward
    outward = chip - inward
    beside = jnp.where(is_edge, near, outward)

    first_chip = jnp.where(is_edge, near, far)
    l_vm[:128, :] = kron_rows(16 * first_chip, 16)
    for h in range(2):
        load_half(h).wait()
    for later in range(1, ROWS):
        load_row(later).start()
    chip_piece(first_chip, l_vm[:128, :])
    pl.semaphore_wait(barrier, DEV - 1)
    start(EARLY[0], first_chip)

    l_vm[...] = kron_rows(0, N)

    def l_rows(to):
        return l_vm[pl.ds(pl.multiple_of(128 * to, 128), 128), :]

    second_chip = jnp.where(is_edge, far, outward)
    chip_piece(second_chip, l_rows(second_chip))

    @pl.when(jnp.logical_not(is_edge))
    def _():
        start(EARLY[0], outward)

    fourth_chip = jnp.where(is_edge, last, near)
    chip_piece(fourth_chip, l_rows(fourth_chip))
    chip_piece(chip, l_rows(chip))
    group(EARLY[0], partner, me).start()

    def make_row(p, carry):
        load_row(p).wait()
        for h in range(2):
            half_row(p, h)
        for rows in EARLY[1:]:
            @pl.when(p == sum(rows) - 1)
            def _():
                start(rows, beside)

                @pl.when(jnp.logical_not(is_edge))
                def _():
                    start(rows, far)

                group(rows, partner, me).start()

        return carry

    lax.fori_loop(1, ROWS, make_row, 0)

    @pl.when(is_edge)
    def _():
        for rows in LATER:
            start(rows, far)
        for rows in WHOLE:
            start(rows, last)

    for side, dest in ((0, 2 * near + core), (1, 2 * near + 1 - core)):
        for chunk in range(CHUNKS):
            near_refs[side * CHUNKS + chunk][...] = send[dest, :, :, pl.ds(128 * chunk, 128)]

    c = c_vm[...]
    spread = (iota((8 * N, N), 0) // 8 == iota((8 * N, N), 1)).astype(BF16)
    rows = lax.dot_general(spread, c, nt, preferred_element_type=F32)
    widen = (iota((N, 8 * N), 0) == iota((N, 8 * N), 1) // 8).astype(BF16)
    full = jnp.dot(rows.astype(BF16), widen, preferred_element_type=F32)
    l4_ref[...] = jnp.where(iota(wide, 0) % 8 == iota(wide, 1) % 8, full, 0.0).astype(BF16)
    l4n_ref[...] = l4_ref[:, pl.ds(pl.multiple_of(128 * near, 128), 128)]
    eye = (iota((N, N), 0) == iota((N, N), 1)).astype(BF16)
    ct_vm[...] = lax.dot_general(eye, c, nt, preferred_element_type=F32).astype(BF16)
    ct_ref[...] = ct_vm[...]

    def third(src, p, first, second):
        g0 = jnp.dot(ct_vm[...], first, preferred_element_type=F32).reshape(8, 8, COLS)
        g1 = jnp.dot(ct_vm[...], second, preferred_element_type=F32).reshape(8, 8, COLS)
        at = pl.multiple_of(N * src + 8 * p, 16)
        g_ref[:, pl.ds(at, 16), :] = jnp.concatenate([g0, g1], axis=1).astype(BF16)

    def own(t, carry):
        third(me, 2 * t, send[me, 2 * t], send[me, 2 * t + 1])
        return carry

    lax.fori_loop(0, ROWS // 2, own, 0)

    def take(groups, sources):
        for rows in groups:
            for src in sources:
                group(rows, src, src).wait_recv()
            if sum(rows) % 2 == 0:
                begin = rows[0] // 2 * 2

                def body(t, carry):
                    for src in sources:
                        p = begin + 2 * t
                        third(src, p, recv[src, p], recv[src, p + 1])
                    return carry

                lax.fori_loop(0, (sum(rows) - begin) // 2, body, 0)

    take(EARLY, [partner])

    @pl.when(jnp.logical_not(is_edge))
    def _():
        g_ref[:, pl.ds(pl.multiple_of(2 * N * near, 16), 2 * N), :] = jnp.zeros((8, 2 * N, COLS), BF16)

    take(EARLY, [2 * beside, 2 * beside + 1])

    for rows in EARLY:
        group(rows, partner, me).wait_send()
    sent(EARLY, beside)

    @pl.when(is_edge)
    def _():
        take(EARLY, [2 * far, 2 * far + 1])
        take(WHOLE, [2 * last, 2 * last + 1])
        sent(LATER, far)
        sent(WHOLE, last)

    @pl.when(jnp.logical_not(is_edge))
    def _():
        take(LATER, [2 * far, 2 * far + 1])
        sent(EARLY, far)


def most_kernel(g_ref, l4_ref, v_ref):
    for ag in range(8):
        v_ref[ag] = jnp.dot(l4_ref[...], g_ref[ag], preferred_element_type=F32)


def chunk_kernel(chunk, same_ref, other_ref, ct_ref, l4n_ref, most_ref, *refs):
    v_hbm, g_vm, v_vm, v_sem = refs[-4:]
    core = lax.axis_index("dev") % 2
    for side, ref in ((core, same_ref), (1 - core, other_ref)):
        for p in range(0, ROWS, 2):
            g0 = jnp.dot(ct_ref[...], ref[p], preferred_element_type=F32).reshape(8, 8, 128)
            g1 = jnp.dot(ct_ref[...], ref[p + 1], preferred_element_type=F32).reshape(8, 8, 128)
            at = pl.multiple_of(N * side + 8 * p, 16)
            g_vm[:, pl.ds(at, 16), :] = jnp.concatenate([g0, g1], axis=1).astype(BF16)

    def put(ag):
        return pltpu.make_async_copy(v_vm.at[ag], v_hbm.at[:, pl.ds(8 * ag, 8), pl.ds(128 * chunk, 128)], v_sem.at[ag])

    for ag in range(8):
        part = jnp.dot(l4n_ref[...], g_vm[ag], preferred_element_type=F32)
        v_vm[ag] = (part + most_ref[ag, :, 128 * chunk:128 * chunk + 128]).reshape(N, 8, 128)
        put(ag).start()
    for ag in range(8):
        put(ag).wait()


def solution(mesh):
    def local_transform(ao_rows, coeffs):
        vmem = pl.BlockSpec(memory_space=pltpu.VMEM)
        anywhere = pl.BlockSpec(memory_space=pltpu.HBM)
        sds = jax.ShapeDtypeStruct
        outs = (
            sds((8, 8 * N, COLS), BF16),
            sds((8 * N, 8 * N), BF16),
            sds((8 * N, 2 * N), BF16),
            sds((N, N), BF16),
        ) + (sds((ROWS, N, 128), BF16),) * (2 * CHUNKS)
        g, l4, l4n, ct, *near = pl.pallas_call(
            exchange_kernel,
            out_shape=outs,
            in_specs=[anywhere, anywhere],
            out_specs=(vmem,) * len(outs),
            scratch_shapes=[
                pltpu.VMEM((ROWS, N, N, N), BF16),
                pltpu.VMEM((N, N), BF16),
                pltpu.VMEM((8 * N, 8 * N), BF16),
                pltpu.VMEM((4 * N, 4 * N), BF16),
                pltpu.VMEM((N, N), BF16),
                pltpu.VMEM((DEV, ROWS, N, COLS), BF16),
                pltpu.VMEM((DEV, ROWS, N, COLS), BF16),
                pltpu.SemaphoreType.DMA((ROWS + 1,)),
                pltpu.SemaphoreType.DMA,
                pltpu.SemaphoreType.DMA((DEV, ROWS)),
                pltpu.SemaphoreType.DMA((DEV, ROWS)),
            ],
            compiler_params=pltpu.CompilerParams(collective_id=0, has_side_effects=True, vmem_limit_bytes=40 * 2**20),
            name="exchange",
        )(pltpu.with_memory_space_constraint(ao_rows, pltpu.HBM), pltpu.with_memory_space_constraint(coeffs, pltpu.HBM))
        same = [(2, 4), (3, 5), (4, 2), (5, 3)]
        other = [(2, 5), (3, 4), (4, 3), (5, 2)]
        arrived = []
        for chunk in range(CHUNKS):
            pair = []
            for side, perm in enumerate((same, other)):
                pair.append(lax.ppermute(near[side * CHUNKS + chunk], "dev", perm))
            arrived.append(pair)
        most = pl.pallas_call(
            most_kernel,
            out_shape=sds((8, 8 * N, COLS), F32),
            in_specs=[vmem, vmem],
            out_specs=vmem,
            compiler_params=pltpu.CompilerParams(vmem_limit_bytes=12 * 2**20),
            cost_estimate=pl.CostEstimate(flops=2 * 8 * 512**3, bytes_accessed=12 * 2**20, transcendentals=0),
            name="most",
        )(g, l4)
        v = None
        for chunk in range(CHUNKS):
            operands = (*arrived[chunk], ct, l4n, most) + (() if v is None else (v,))
            v = pl.pallas_call(
                functools.partial(chunk_kernel, chunk),
                out_shape=sds((N, N, COLS), F32),
                in_specs=[vmem] * 5 + ([] if v is None else [anywhere]),
                out_specs=anywhere,
                scratch_shapes=[
                    pltpu.VMEM((8, 2 * N, 128), BF16),
                    pltpu.VMEM((8, N, 8, 128), F32),
                    pltpu.SemaphoreType.DMA((8,)),
                ],
                input_output_aliases={} if v is None else {5: 0},
                compiler_params=pltpu.CompilerParams(vmem_limit_bytes=12 * 2**20),
                cost_estimate=pl.CostEstimate(flops=2 * 8 * 512 * 128 * 128, bytes_accessed=4 * 2**20, transcendentals=0),
            )(*operands)
        return v

    return jax.shard_map(local_transform, mesh=mesh, in_specs=(P(('frag', 'dev')), P('frag')), out_specs=P('frag', None, 'dev'), check_vma=False)
```

```python
import functools

import jax
import jax.numpy as jnp
from jax import lax
from jax.experimental import pallas as pl
from jax.experimental.pallas import tpu as pltpu
from jax.sharding import PartitionSpec as P


N = 64
DEV = 8
ROWS = N // DEV
COLS = N * N // DEV
CHUNKS = COLS // 128
EARLY = ((0, 1), (1, 1), (2, 2), (4, 4))
LATER = ((0, 4), (4, 4))
WHOLE = ((0, 8),)
BF16 = jnp.bfloat16
F32 = jnp.float32


def iota(shape, dim):
    return lax.broadcasted_iota(jnp.int32, shape, dim)


def exchange_kernel(a_hbm, c_hbm, g_ref, l4_ref, l4n_ref, ct_ref, *refs):
    near_refs = refs[:2 * CHUNKS]
    a_vm, c_vm, l_vm, b4_vm, ct_vm, send, recv, a_sem, c_sem, send_sem, recv_sem = refs[2 * CHUNKS:]
    me = lax.axis_index("dev")
    chip = me // 2
    core = me % 2

    load_c = pltpu.make_async_copy(c_hbm, c_vm, c_sem)
    load_c.start()

    def load_row(p):
        return pltpu.make_async_copy(a_hbm.at[p], a_vm.at[p], a_sem.at[p])

    def load_half(h):
        half = pl.ds(32 * h, 32)
        return pltpu.make_async_copy(a_hbm.at[0, half], a_vm.at[0, half], a_sem.at[ROWS * h])

    for h in range(2):
        load_half(h).start()

    barrier = pltpu.get_barrier_semaphore()
    for k in range(1, DEV):
        pl.semaphore_signal(barrier, inc=1, device_id={"dev": (me + k) % DEV}, device_id_type=pl.DeviceIdType.MESH)

    load_c.wait()
    c = c_vm[...]
    nt = (((1,), (1,)), ((), ()))
    wide = (8 * N, 8 * N)

    def kron_rows(first_m, count):
        spread = (iota((8 * count, N), 0) // 8 + first_m == iota((8 * count, N), 1)).astype(BF16)
        rows = lax.dot_general(spread, c, nt, preferred_element_type=F32)
        pair = jnp.concatenate([rows, rows], axis=1)
        tiled = jnp.concatenate([pair] * 4, axis=1)
        shape = (8 * count, 8 * N)
        return jnp.where(iota(shape, 0) % 8 == iota(shape, 1) // N, tiled, 0.0).astype(BF16)

    cf = c.astype(F32)
    cpair = jnp.concatenate([cf, cf], axis=1)
    c4 = jnp.concatenate([cpair, cpair], axis=1)
    c44 = jnp.concatenate([c4] * 4, axis=0)
    quad = (4 * N, 4 * N)
    b4_vm[...] = jnp.where(iota(quad, 0) // N == iota(quad, 1) // N, c44, 0.0).astype(BF16)

    def group(rows, dest, src):
        part = pl.ds(*rows)
        return pltpu.make_async_remote_copy(
            src_ref=send.at[dest, part],
            dst_ref=recv.at[src, part],
            send_sem=send_sem.at[dest, rows[0]],
            recv_sem=recv_sem.at[src, rows[0]],
            device_id={"dev": dest},
            device_id_type=pl.DeviceIdType.MESH,
        )

    def start(rows, to):
        for k in range(2):
            group(rows, 2 * to + k, me).start()

    def sent(groups, to):
        for rows in groups:
            for k in range(2):
                group(rows, 2 * to + k, me).wait_send()

    low = iota((32, 8, 128), 2) < N

    def pieces(p, h, lhs, count, put):
        a = a_vm[p, pl.ds(32 * h, 32)].reshape(4, 8 * N, N)
        left = jnp.concatenate([a[0], a[1]], axis=1)
        right = jnp.concatenate([a[2], a[3]], axis=1)
        a4 = jnp.concatenate([left, right], axis=1)
        t_one = jnp.dot(lhs, a4, preferred_element_type=F32).astype(BF16)
        half = jnp.dot(t_one, b4_vm[...], preferred_element_type=F32)
        pairs = half.reshape(count, 2, 8, 256)
        for t in range(2):
            even = pairs[:, 0, :, 128 * t:128 * t + 128]
            odd = pairs[:, 1, :, 128 * t:128 * t + 128]
            first_rows = jnp.where(low[:count], even, pltpu.roll(odd, N, 2))
            second_rows = jnp.where(low[:count], pltpu.roll(even, N, 2), odd)
            both = jnp.concatenate([first_rows, second_rows], axis=1).astype(BF16)
            for jp in range(count):
                put(jp // 4, pl.ds(32 * h + 16 * t, 16), pl.ds(128 * (jp % 4), 128), both[jp])

    def half_row(p, h):
        def put(dest, q, columns, value):
            send[dest, p, q, columns] = value

        pieces(p, h, l_vm[...], 32, put)

    def chip_piece(to, lhs):
        def put(dest, q, columns, value):
            send[2 * to + dest, 0, q, columns] = value

        for h in range(2):
            pieces(0, h, lhs, 8, put)

    is_edge = jnp.logical_or(chip == 0, chip == 3)
    inward = jnp.where(chip < 2, 1, -1)
    partner = 2 * chip + 1 - core
    near = chip + inward
    far = chip + 2 * inward
    last = chip + 3 * inward
    outward = chip - inward
    beside = jnp.where(is_edge, near, outward)

    first_chip = jnp.where(is_edge, near, far)
    l_vm[:128, :] = kron_rows(16 * first_chip, 16)
    for h in range(2):
        load_half(h).wait()
    for later in (1, 2):
        load_row(later).start()
    chip_piece(first_chip, l_vm[:128, :])
    pl.semaphore_wait(barrier, DEV - 1)
    start(EARLY[0], first_chip)

    l_vm[...] = kron_rows(0, N)

    def l_rows(to):
        return l_vm[pl.ds(pl.multiple_of(128 * to, 128), 128), :]

    second_chip = jnp.where(is_edge, far, outward)
    chip_piece(second_chip, l_rows(second_chip))

    @pl.when(jnp.logical_not(is_edge))
    def _():
        start(EARLY[0], outward)

    fourth_chip = jnp.where(is_edge, last, near)
    chip_piece(fourth_chip, l_rows(fourth_chip))
    chip_piece(chip, l_rows(chip))
    group(EARLY[0], partner, me).start()

    def make_row(p, carry):
        load_row(p).wait()

        @pl.when(p < ROWS - 2)
        def _():
            load_row(p + 2).start()

        for h in range(2):
            half_row(p, h)
        for rows in EARLY[1:]:
            @pl.when(p == sum(rows) - 1)
            def _():
                start(rows, beside)

                @pl.when(jnp.logical_not(is_edge))
                def _():
                    start(rows, far)

                group(rows, partner, me).start()

        return carry

    lax.fori_loop(1, ROWS, make_row, 0)

    @pl.when(is_edge)
    def _():
        for rows in LATER:
            start(rows, far)
        for rows in WHOLE:
            start(rows, last)

    for side, dest in ((0, 2 * near + core), (1, 2 * near + 1 - core)):
        for chunk in range(CHUNKS):
            near_refs[side * CHUNKS + chunk][...] = send[dest, :, :, pl.ds(128 * chunk, 128)]

    c = c_vm[...]
    spread = (iota((8 * N, N), 0) // 8 == iota((8 * N, N), 1)).astype(BF16)
    rows = lax.dot_general(spread, c, nt, preferred_element_type=F32)
    widen = (iota((N, 8 * N), 0) == iota((N, 8 * N), 1) // 8).astype(BF16)
    full = jnp.dot(rows.astype(BF16), widen, preferred_element_type=F32)
    l4_ref[...] = jnp.where(iota(wide, 0) % 8 == iota(wide, 1) % 8, full, 0.0).astype(BF16)
    l4n_ref[...] = l4_ref[:, pl.ds(pl.multiple_of(128 * near, 128), 128)]
    eye = (iota((N, N), 0) == iota((N, N), 1)).astype(BF16)
    ct_vm[...] = lax.dot_general(eye, c, nt, preferred_element_type=F32).astype(BF16)
    ct_ref[...] = ct_vm[...]

    def third(src, p, first, second):
        g0 = jnp.dot(ct_vm[...], first, preferred_element_type=F32).reshape(8, 8, COLS)
        g1 = jnp.dot(ct_vm[...], second, preferred_element_type=F32).reshape(8, 8, COLS)
        at = pl.multiple_of(N * src + 8 * p, 16)
        g_ref[:, pl.ds(at, 16), :] = jnp.concatenate([g0, g1], axis=1).astype(BF16)

    def own(t, carry):
        third(me, 2 * t, send[me, 2 * t], send[me, 2 * t + 1])
        return carry

    lax.fori_loop(0, ROWS // 2, own, 0)

    def take(groups, sources):
        for rows in groups:
            for src in sources:
                group(rows, src, src).wait_recv()
            if sum(rows) % 2 == 0:
                begin = rows[0] // 2 * 2

                def body(t, carry):
                    for src in sources:
                        p = begin + 2 * t
                        third(src, p, recv[src, p], recv[src, p + 1])
                    return carry

                lax.fori_loop(0, (sum(rows) - begin) // 2, body, 0)

    take(EARLY, [partner])

    @pl.when(jnp.logical_not(is_edge))
    def _():
        g_ref[:, pl.ds(pl.multiple_of(2 * N * near, 16), 2 * N), :] = jnp.zeros((8, 2 * N, COLS), BF16)

    take(EARLY, [2 * beside, 2 * beside + 1])

    for rows in EARLY:
        group(rows, partner, me).wait_send()
    sent(EARLY, beside)

    @pl.when(is_edge)
    def _():
        take(EARLY, [2 * far, 2 * far + 1])
        take(WHOLE, [2 * last, 2 * last + 1])
        sent(LATER, far)
        sent(WHOLE, last)

    @pl.when(jnp.logical_not(is_edge))
    def _():
        take(LATER, [2 * far, 2 * far + 1])
        sent(EARLY, far)


def most_kernel(g_ref, l4_ref, v_ref):
    for ag in range(8):
        v_ref[ag] = jnp.dot(l4_ref[...], g_ref[ag], preferred_element_type=F32)


def chunk_kernel(chunk, same_ref, other_ref, ct_ref, l4n_ref, most_ref, *refs):
    v_hbm, g_vm, v_vm, v_sem = refs[-4:]
    core = lax.axis_index("dev") % 2
    for side, ref in ((core, same_ref), (1 - core, other_ref)):
        for p in range(0, ROWS, 2):
            g0 = jnp.dot(ct_ref[...], ref[p], preferred_element_type=F32).reshape(8, 8, 128)
            g1 = jnp.dot(ct_ref[...], ref[p + 1], preferred_element_type=F32).reshape(8, 8, 128)
            at = pl.multiple_of(N * side + 8 * p, 16)
            g_vm[:, pl.ds(at, 16), :] = jnp.concatenate([g0, g1], axis=1).astype(BF16)

    def put(ag):
        return pltpu.make_async_copy(v_vm.at[ag], v_hbm.at[:, pl.ds(8 * ag, 8), pl.ds(128 * chunk, 128)], v_sem.at[ag])

    for ag in range(8):
        part = jnp.dot(l4n_ref[...], g_vm[ag], preferred_element_type=F32)
        v_vm[ag] = (part + most_ref[ag, :, 128 * chunk:128 * chunk + 128]).reshape(N, 8, 128)
        put(ag).start()
    for ag in range(8):
        put(ag).wait()


def solution(mesh):
    def local_transform(ao_rows, coeffs):
        vmem = pl.BlockSpec(memory_space=pltpu.VMEM)
        anywhere = pl.BlockSpec(memory_space=pltpu.HBM)
        sds = jax.ShapeDtypeStruct
        outs = (
            sds((8, 8 * N, COLS), BF16),
            sds((8 * N, 8 * N), BF16),
            sds((8 * N, 2 * N), BF16),
            sds((N, N), BF16),
        ) + (sds((ROWS, N, 128), BF16),) * (2 * CHUNKS)
        g, l4, l4n, ct, *near = pl.pallas_call(
            exchange_kernel,
            out_shape=outs,
            in_specs=[anywhere, anywhere],
            out_specs=(vmem,) * len(outs),
            scratch_shapes=[
                pltpu.VMEM((ROWS, N, N, N), BF16),
                pltpu.VMEM((N, N), BF16),
                pltpu.VMEM((8 * N, 8 * N), BF16),
                pltpu.VMEM((4 * N, 4 * N), BF16),
                pltpu.VMEM((N, N), BF16),
                pltpu.VMEM((DEV, ROWS, N, COLS), BF16),
                pltpu.VMEM((DEV, ROWS, N, COLS), BF16),
                pltpu.SemaphoreType.DMA((ROWS + 1,)),
                pltpu.SemaphoreType.DMA,
                pltpu.SemaphoreType.DMA((DEV, ROWS)),
                pltpu.SemaphoreType.DMA((DEV, ROWS)),
            ],
            compiler_params=pltpu.CompilerParams(collective_id=0, has_side_effects=True, vmem_limit_bytes=40 * 2**20),
            name="exchange",
        )(pltpu.with_memory_space_constraint(ao_rows, pltpu.HBM), pltpu.with_memory_space_constraint(coeffs, pltpu.HBM))
        same = [(2, 4), (3, 5), (4, 2), (5, 3)]
        other = [(2, 5), (3, 4), (4, 3), (5, 2)]
        arrived = []
        for chunk in range(CHUNKS):
            pair = []
            for side, perm in enumerate((same, other)):
                pair.append(lax.ppermute(near[side * CHUNKS + chunk], "dev", perm))
            arrived.append(pair)
        most = pl.pallas_call(
            most_kernel,
            out_shape=sds((8, 8 * N, COLS), F32),
            in_specs=[vmem, vmem],
            out_specs=vmem,
            compiler_params=pltpu.CompilerParams(vmem_limit_bytes=12 * 2**20),
            cost_estimate=pl.CostEstimate(flops=2 * 8 * 512**3, bytes_accessed=12 * 2**20, transcendentals=0),
            name="most",
        )(g, l4)
        v = None
        for chunk in range(CHUNKS):
            operands = (*arrived[chunk], ct, l4n, most) + (() if v is None else (v,))
            v = pl.pallas_call(
                functools.partial(chunk_kernel, chunk),
                out_shape=sds((N, N, COLS), F32),
                in_specs=[vmem] * 5 + ([] if v is None else [anywhere]),
                out_specs=anywhere,
                scratch_shapes=[
                    pltpu.VMEM((8, 2 * N, 128), BF16),
                    pltpu.VMEM((8, N, 8, 128), F32),
                    pltpu.SemaphoreType.DMA((8,)),
                ],
                input_output_aliases={} if v is None else {5: 0},
                compiler_params=pltpu.CompilerParams(vmem_limit_bytes=12 * 2**20),
                cost_estimate=pl.CostEstimate(flops=2 * 8 * 512 * 128 * 128, bytes_accessed=4 * 2**20, transcendentals=0),
            )(*operands)
        return v

    return jax.shard_map(local_transform, mesh=mesh, in_specs=(P(('frag', 'dev')), P('frag')), out_specs=P('frag', None, 'dev'), check_vma=False)
```

```python
import functools

import jax
import jax.numpy as jnp
from jax import lax
from jax.experimental import pallas as pl
from jax.experimental.pallas import tpu as pltpu
from jax.sharding import PartitionSpec as P


N = 64
DEV = 8
ROWS = N // DEV
COLS = N * N // DEV
CHUNKS = COLS // 128
EARLY = ((0, 1), (1, 1), (2, 1), (3, 1), (4, 2), (6, 2))
LATER = ((0, 4), (4, 4))
WHOLE = ((0, 8),)
BF16 = jnp.bfloat16
F32 = jnp.float32


def iota(shape, dim):
    return lax.broadcasted_iota(jnp.int32, shape, dim)


def exchange_kernel(a_hbm, c_hbm, g_ref, l4_ref, l4n_ref, ct_ref, *refs):
    near_refs = refs[:2 * CHUNKS]
    a_vm, c_vm, l_vm, b4_vm, ct_vm, send, recv, a_sem, c_sem, send_sem, recv_sem = refs[2 * CHUNKS:]
    me = lax.axis_index("dev")
    chip = me // 2
    core = me % 2

    load_c = pltpu.make_async_copy(c_hbm, c_vm, c_sem)
    load_c.start()

    def load_row(p):
        return pltpu.make_async_copy(a_hbm.at[p], a_vm.at[p], a_sem.at[p])

    def load_half(h):
        half = pl.ds(32 * h, 32)
        return pltpu.make_async_copy(a_hbm.at[0, half], a_vm.at[0, half], a_sem.at[ROWS * h])

    for h in range(2):
        load_half(h).start()

    barrier = pltpu.get_barrier_semaphore()
    for k in range(1, DEV):
        pl.semaphore_signal(barrier, inc=1, device_id={"dev": (me + k) % DEV}, device_id_type=pl.DeviceIdType.MESH)

    load_c.wait()
    load_row(1).start()
    c = c_vm[...]
    nt = (((1,), (1,)), ((), ()))
    wide = (8 * N, 8 * N)

    def kron_rows(first_m, count):
        spread = (iota((8 * count, N), 0) // 8 + first_m == iota((8 * count, N), 1)).astype(BF16)
        rows = lax.dot_general(spread, c, nt, preferred_element_type=F32)
        pair = jnp.concatenate([rows, rows], axis=1)
        tiled = jnp.concatenate([pair] * 4, axis=1)
        shape = (8 * count, 8 * N)
        return jnp.where(iota(shape, 0) % 8 == iota(shape, 1) // N, tiled, 0.0).astype(BF16)

    cf = c.astype(F32)
    cpair = jnp.concatenate([cf, cf], axis=1)
    c4 = jnp.concatenate([cpair, cpair], axis=1)
    c44 = jnp.concatenate([c4] * 4, axis=0)
    quad = (4 * N, 4 * N)
    b4_vm[...] = jnp.where(iota(quad, 0) // N == iota(quad, 1) // N, c44, 0.0).astype(BF16)

    def group(rows, dest, src):
        part = pl.ds(*rows)
        return pltpu.make_async_remote_copy(
            src_ref=send.at[dest, part],
            dst_ref=recv.at[src, part],
            send_sem=send_sem.at[dest, rows[0]],
            recv_sem=recv_sem.at[src, rows[0]],
            device_id={"dev": dest},
            device_id_type=pl.DeviceIdType.MESH,
        )

    def start(rows, to):
        for k in range(2):
            group(rows, 2 * to + k, me).start()

    def sent(groups, to):
        for rows in groups:
            for k in range(2):
                group(rows, 2 * to + k, me).wait_send()

    low = iota((32, 8, 128), 2) < N

    def pieces(p, h, lhs, count, put):
        a = a_vm[p, pl.ds(32 * h, 32)].reshape(4, 8 * N, N)
        left = jnp.concatenate([a[0], a[1]], axis=1)
        right = jnp.concatenate([a[2], a[3]], axis=1)
        a4 = jnp.concatenate([left, right], axis=1)
        t_one = jnp.dot(lhs, a4, preferred_element_type=F32).astype(BF16)
        half = jnp.dot(t_one, b4_vm[...], preferred_element_type=F32)
        pairs = half.reshape(count, 2, 8, 256)
        for t in range(2):
            even = pairs[:, 0, :, 128 * t:128 * t + 128]
            odd = pairs[:, 1, :, 128 * t:128 * t + 128]
            first_rows = jnp.where(low[:count], even, pltpu.roll(odd, N, 2))
            second_rows = jnp.where(low[:count], pltpu.roll(even, N, 2), odd)
            both = jnp.concatenate([first_rows, second_rows], axis=1).astype(BF16)
            for jp in range(count):
                put(jp // 4, pl.ds(32 * h + 16 * t, 16), pl.ds(128 * (jp % 4), 128), both[jp])

    def half_row(p, h):
        def put(dest, q, columns, value):
            send[dest, p, q, columns] = value

        pieces(p, h, l_vm[...], 32, put)

    def chip_piece(p, to, lhs):
        def put(dest, q, columns, value):
            send[2 * to + dest, p, q, columns] = value

        for h in range(2):
            pieces(p, h, lhs, 8, put)

    is_edge = jnp.logical_or(chip == 0, chip == 3)
    inward = jnp.where(chip < 2, 1, -1)
    partner = 2 * chip + 1 - core
    near = chip + inward
    far = chip + 2 * inward
    last = chip + 3 * inward
    outward = chip - inward
    beside = jnp.where(is_edge, near, outward)

    first_chip = jnp.where(is_edge, near, far)
    l_vm[:128, :] = kron_rows(16 * first_chip, 16)
    for h in range(2):
        load_half(h).wait()
    load_row(2).start()
    chip_piece(0, first_chip, l_vm[:128, :])
    pl.semaphore_wait(barrier, DEV - 1)
    start(EARLY[0], first_chip)
    load_row(1).wait()
    load_row(3).start()
    chip_piece(1, first_chip, l_vm[:128, :])
    start(EARLY[1], first_chip)

    l_vm[...] = kron_rows(0, N)
    second_chip = jnp.where(is_edge, far, outward)
    fourth_chip = jnp.where(is_edge, last, near)
    for p in range(2):
        for to in (second_chip, fourth_chip, chip):
            chip_piece(p, to, l_vm[pl.ds(pl.multiple_of(128 * to, 128), 128), :])
        group(EARLY[p], partner, me).start()

        @pl.when(jnp.logical_not(is_edge))
        def _():
            start(EARLY[p], outward)

    def make_row(p, carry):
        load_row(p).wait()

        @pl.when(p < ROWS - 2)
        def _():
            load_row(p + 2).start()

        for h in range(2):
            half_row(p, h)
        for rows in EARLY[2:]:
            @pl.when(p == sum(rows) - 1)
            def _():
                start(rows, beside)

                @pl.when(jnp.logical_not(is_edge))
                def _():
                    start(rows, far)

                group(rows, partner, me).start()

        return carry

    lax.fori_loop(2, ROWS, make_row, 0)

    @pl.when(is_edge)
    def _():
        for rows in LATER:
            start(rows, far)
        for rows in WHOLE:
            start(rows, last)

    for side, dest in ((0, 2 * near + core), (1, 2 * near + 1 - core)):
        for chunk in range(CHUNKS):
            near_refs[side * CHUNKS + chunk][...] = send[dest, :, :, pl.ds(128 * chunk, 128)]

    c = c_vm[...]
    spread = (iota((8 * N, N), 0) // 8 == iota((8 * N, N), 1)).astype(BF16)
    rows = lax.dot_general(spread, c, nt, preferred_element_type=F32)
    widen = (iota((N, 8 * N), 0) == iota((N, 8 * N), 1) // 8).astype(BF16)
    full = jnp.dot(rows.astype(BF16), widen, preferred_element_type=F32)
    l4_ref[...] = jnp.where(iota(wide, 0) % 8 == iota(wide, 1) % 8, full, 0.0).astype(BF16)
    l4n_ref[...] = l4_ref[:, pl.ds(pl.multiple_of(128 * near, 128), 128)]
    eye = (iota((N, N), 0) == iota((N, N), 1)).astype(BF16)
    ct_vm[...] = lax.dot_general(eye, c, nt, preferred_element_type=F32).astype(BF16)
    ct_ref[...] = ct_vm[...]

    def third(src, p, first, second):
        g0 = jnp.dot(ct_vm[...], first, preferred_element_type=F32).reshape(8, 8, COLS)
        g1 = jnp.dot(ct_vm[...], second, preferred_element_type=F32).reshape(8, 8, COLS)
        at = pl.multiple_of(N * src + 8 * p, 16)
        g_ref[:, pl.ds(at, 16), :] = jnp.concatenate([g0, g1], axis=1).astype(BF16)

    def own(t, carry):
        third(me, 2 * t, send[me, 2 * t], send[me, 2 * t + 1])
        return carry

    lax.fori_loop(0, ROWS // 2, own, 0)

    def take(groups, sources):
        for rows in groups:
            for src in sources:
                group(rows, src, src).wait_recv()
            if sum(rows) % 2 == 0:
                begin = rows[0] // 2 * 2

                def body(t, carry):
                    for src in sources:
                        p = begin + 2 * t
                        third(src, p, recv[src, p], recv[src, p + 1])
                    return carry

                lax.fori_loop(0, (sum(rows) - begin) // 2, body, 0)

    take(EARLY, [partner])

    @pl.when(jnp.logical_not(is_edge))
    def _():
        g_ref[:, pl.ds(pl.multiple_of(2 * N * near, 16), 2 * N), :] = jnp.zeros((8, 2 * N, COLS), BF16)

    take(EARLY, [2 * beside, 2 * beside + 1])

    for rows in EARLY:
        group(rows, partner, me).wait_send()
    sent(EARLY, beside)

    @pl.when(is_edge)
    def _():
        take(EARLY, [2 * far, 2 * far + 1])
        take(WHOLE, [2 * last, 2 * last + 1])
        sent(LATER, far)
        sent(WHOLE, last)

    @pl.when(jnp.logical_not(is_edge))
    def _():
        take(LATER, [2 * far, 2 * far + 1])
        sent(EARLY, far)


def most_kernel(g_ref, l4_ref, v_ref):
    for ag in range(8):
        v_ref[ag] = jnp.dot(l4_ref[...], g_ref[ag], preferred_element_type=F32)


def chunk_kernel(chunk, same_ref, other_ref, ct_ref, l4n_ref, most_ref, *refs):
    v_hbm, g_vm, v_vm, v_sem = refs[-4:]
    core = lax.axis_index("dev") % 2
    for side, ref in ((core, same_ref), (1 - core, other_ref)):
        for p in range(0, ROWS, 2):
            g0 = jnp.dot(ct_ref[...], ref[p], preferred_element_type=F32).reshape(8, 8, 128)
            g1 = jnp.dot(ct_ref[...], ref[p + 1], preferred_element_type=F32).reshape(8, 8, 128)
            at = pl.multiple_of(N * side + 8 * p, 16)
            g_vm[:, pl.ds(at, 16), :] = jnp.concatenate([g0, g1], axis=1).astype(BF16)

    def put(ag):
        return pltpu.make_async_copy(v_vm.at[ag], v_hbm.at[:, pl.ds(8 * ag, 8), pl.ds(128 * chunk, 128)], v_sem.at[ag])

    for ag in range(8):
        part = jnp.dot(l4n_ref[...], g_vm[ag], preferred_element_type=F32)
        v_vm[ag] = (part + most_ref[ag, :, 128 * chunk:128 * chunk + 128]).reshape(N, 8, 128)
        put(ag).start()
    for ag in range(8):
        put(ag).wait()


def solution(mesh):
    def local_transform(ao_rows, coeffs):
        vmem = pl.BlockSpec(memory_space=pltpu.VMEM)
        anywhere = pl.BlockSpec(memory_space=pltpu.HBM)
        sds = jax.ShapeDtypeStruct
        outs = (
            sds((8, 8 * N, COLS), BF16),
            sds((8 * N, 8 * N), BF16),
            sds((8 * N, 2 * N), BF16),
            sds((N, N), BF16),
        ) + (sds((ROWS, N, 128), BF16),) * (2 * CHUNKS)
        g, l4, l4n, ct, *near = pl.pallas_call(
            exchange_kernel,
            out_shape=outs,
            in_specs=[anywhere, anywhere],
            out_specs=(vmem,) * len(outs),
            scratch_shapes=[
                pltpu.VMEM((ROWS, N, N, N), BF16),
                pltpu.VMEM((N, N), BF16),
                pltpu.VMEM((8 * N, 8 * N), BF16),
                pltpu.VMEM((4 * N, 4 * N), BF16),
                pltpu.VMEM((N, N), BF16),
                pltpu.VMEM((DEV, ROWS, N, COLS), BF16),
                pltpu.VMEM((DEV, ROWS, N, COLS), BF16),
                pltpu.SemaphoreType.DMA((ROWS + 1,)),
                pltpu.SemaphoreType.DMA,
                pltpu.SemaphoreType.DMA((DEV, ROWS)),
                pltpu.SemaphoreType.DMA((DEV, ROWS)),
            ],
            compiler_params=pltpu.CompilerParams(collective_id=0, has_side_effects=True, vmem_limit_bytes=40 * 2**20),
            name="exchange",
        )(pltpu.with_memory_space_constraint(ao_rows, pltpu.HBM), pltpu.with_memory_space_constraint(coeffs, pltpu.HBM))
        same = [(2, 4), (3, 5), (4, 2), (5, 3)]
        other = [(2, 5), (3, 4), (4, 3), (5, 2)]
        arrived = []
        for chunk in range(CHUNKS):
            pair = []
            for side, perm in enumerate((same, other)):
                pair.append(lax.ppermute(near[side * CHUNKS + chunk], "dev", perm))
            arrived.append(pair)
        most = pl.pallas_call(
            most_kernel,
            out_shape=sds((8, 8 * N, COLS), F32),
            in_specs=[vmem, vmem],
            out_specs=vmem,
            compiler_params=pltpu.CompilerParams(vmem_limit_bytes=12 * 2**20),
            cost_estimate=pl.CostEstimate(flops=2 * 8 * 512**3, bytes_accessed=12 * 2**20, transcendentals=0),
            name="most",
        )(g, l4)
        v = None
        for chunk in range(CHUNKS):
            operands = (*arrived[chunk], ct, l4n, most) + (() if v is None else (v,))
            v = pl.pallas_call(
                functools.partial(chunk_kernel, chunk),
                out_shape=sds((N, N, COLS), F32),
                in_specs=[vmem] * 5 + ([] if v is None else [anywhere]),
                out_specs=anywhere,
                scratch_shapes=[
                    pltpu.VMEM((8, 2 * N, 128), BF16),
                    pltpu.VMEM((8, N, 8, 128), F32),
                    pltpu.SemaphoreType.DMA((8,)),
                ],
                input_output_aliases={} if v is None else {5: 0},
                compiler_params=pltpu.CompilerParams(vmem_limit_bytes=12 * 2**20),
                cost_estimate=pl.CostEstimate(flops=2 * 8 * 512 * 128 * 128, bytes_accessed=4 * 2**20, transcendentals=0),
            )(*operands)
        return v

    return jax.shard_map(local_transform, mesh=mesh, in_specs=(P(('frag', 'dev')), P('frag')), out_specs=P('frag', None, 'dev'), check_vma=False)
```

```python
import functools

import jax
import jax.numpy as jnp
from jax import lax
from jax.experimental import pallas as pl
from jax.experimental.pallas import tpu as pltpu
from jax.sharding import PartitionSpec as P


N = 64
DEV = 8
ROWS = N // DEV
COLS = N * N // DEV
CHUNKS = COLS // 128
EARLY = ((0, 1), (1, 1), (2, 1), (3, 1), (4, 2), (6, 2))
LATER = ((0, 4), (4, 4))
WHOLE = ((0, 8),)
BF16 = jnp.bfloat16
F32 = jnp.float32


def iota(shape, dim):
    return lax.broadcasted_iota(jnp.int32, shape, dim)


def exchange_kernel(a_hbm, c_hbm, g_ref, l4_ref, l4n_ref, ct_ref, *refs):
    near_refs = refs[:2 * CHUNKS]
    a_vm, c_vm, l_vm, b4_vm, ct_vm, send, recv, a_sem, c_sem, send_sem, recv_sem = refs[2 * CHUNKS:]
    me = lax.axis_index("dev")
    chip = me // 2
    core = me % 2

    load_c = pltpu.make_async_copy(c_hbm, c_vm, c_sem)
    load_c.start()

    def load_row(p):
        return pltpu.make_async_copy(a_hbm.at[p], a_vm.at[p], a_sem.at[p])

    def load_half(h):
        half = pl.ds(32 * h, 32)
        return pltpu.make_async_copy(a_hbm.at[0, half], a_vm.at[0, half], a_sem.at[ROWS * h])

    for h in range(2):
        load_half(h).start()

    barrier = pltpu.get_barrier_semaphore()
    for k in range(1, DEV):
        pl.semaphore_signal(barrier, inc=1, device_id={"dev": (me + k) % DEV}, device_id_type=pl.DeviceIdType.MESH)

    load_c.wait()
    load_row(1).start()
    c = c_vm[...]
    nt = (((1,), (1,)), ((), ()))
    wide = (8 * N, 8 * N)

    def kron_rows(first_m, count):
        spread = (iota((8 * count, N), 0) // 8 + first_m == iota((8 * count, N), 1)).astype(BF16)
        rows = lax.dot_general(spread, c, nt, preferred_element_type=F32)
        pair = jnp.concatenate([rows, rows], axis=1)
        tiled = jnp.concatenate([pair] * 4, axis=1)
        shape = (8 * count, 8 * N)
        return jnp.where(iota(shape, 0) % 8 == iota(shape, 1) // N, tiled, 0.0).astype(BF16)

    cf = c.astype(F32)
    cpair = jnp.concatenate([cf, cf], axis=1)
    c4 = jnp.concatenate([cpair, cpair], axis=1)
    c44 = jnp.concatenate([c4] * 4, axis=0)
    quad = (4 * N, 4 * N)
    b4_vm[...] = jnp.where(iota(quad, 0) // N == iota(quad, 1) // N, c44, 0.0).astype(BF16)

    def group(rows, dest, src):
        part = pl.ds(*rows)
        return pltpu.make_async_remote_copy(
            src_ref=send.at[dest, part],
            dst_ref=recv.at[src, part],
            send_sem=send_sem.at[dest, rows[0]],
            recv_sem=recv_sem.at[src, rows[0]],
            device_id={"dev": dest},
            device_id_type=pl.DeviceIdType.MESH,
        )

    def start(rows, to):
        for k in range(2):
            group(rows, 2 * to + k, me).start()

    def sent(groups, to):
        for rows in groups:
            for k in range(2):
                group(rows, 2 * to + k, me).wait_send()

    low = iota((32, 8, 128), 2) < N

    def pieces(p, h, lhs, count, put):
        a = a_vm[p, pl.ds(32 * h, 32)].reshape(4, 8 * N, N)
        left = jnp.concatenate([a[0], a[1]], axis=1)
        right = jnp.concatenate([a[2], a[3]], axis=1)
        a4 = jnp.concatenate([left, right], axis=1)
        t_one = jnp.dot(lhs, a4, preferred_element_type=F32).astype(BF16)
        half = jnp.dot(t_one, b4_vm[...], preferred_element_type=F32)
        pairs = half.reshape(count, 2, 8, 256)
        for t in range(2):
            even = pairs[:, 0, :, 128 * t:128 * t + 128]
            odd = pairs[:, 1, :, 128 * t:128 * t + 128]
            first_rows = jnp.where(low[:count], even, pltpu.roll(odd, N, 2))
            second_rows = jnp.where(low[:count], pltpu.roll(even, N, 2), odd)
            both = jnp.concatenate([first_rows, second_rows], axis=1).astype(BF16)
            for jp in range(count):
                put(jp // 4, pl.ds(32 * h + 16 * t, 16), pl.ds(128 * (jp % 4), 128), both[jp])

    def half_row(p, h):
        def put(dest, q, columns, value):
            send[dest, p, q, columns] = value

        pieces(p, h, l_vm[...], 32, put)

    def chip_piece(p, to, lhs):
        def put(dest, q, columns, value):
            send[2 * to + dest, p, q, columns] = value

        for h in range(2):
            pieces(p, h, lhs, 8, put)

    is_edge = jnp.logical_or(chip == 0, chip == 3)
    inward = jnp.where(chip < 2, 1, -1)
    partner = 2 * chip + 1 - core
    near = chip + inward
    far = chip + 2 * inward
    last = chip + 3 * inward
    outward = chip - inward
    beside = jnp.where(is_edge, near, outward)

    first_chip = jnp.where(is_edge, near, far)
    l_vm[:128, :] = kron_rows(16 * first_chip, 16)
    for h in range(2):
        load_half(h).wait()
    load_row(2).start()
    chip_piece(0, first_chip, l_vm[:128, :])
    pl.semaphore_wait(barrier, DEV - 1)
    start(EARLY[0], first_chip)
    load_row(1).wait()
    load_row(3).start()
    chip_piece(1, first_chip, l_vm[:128, :])
    start(EARLY[1], first_chip)

    l_vm[...] = kron_rows(0, N)
    second_chip = jnp.where(is_edge, far, outward)
    fourth_chip = jnp.where(is_edge, last, near)
    for p in range(2):
        for to in (second_chip, fourth_chip, chip):
            chip_piece(p, to, l_vm[pl.ds(pl.multiple_of(128 * to, 128), 128), :])
        group(EARLY[p], partner, me).start()

        @pl.when(jnp.logical_not(is_edge))
        def _():
            start(EARLY[p], outward)

    def make_row(p, carry):
        load_row(p).wait()

        @pl.when(p < ROWS - 2)
        def _():
            load_row(p + 2).start()

        for h in range(2):
            half_row(p, h)
        for rows in EARLY[2:]:
            @pl.when(p == sum(rows) - 1)
            def _():
                start(rows, beside)

                @pl.when(jnp.logical_not(is_edge))
                def _():
                    start(rows, far)

                group(rows, partner, me).start()

        return carry

    lax.fori_loop(2, ROWS, make_row, 0)

    @pl.when(is_edge)
    def _():
        for rows in LATER:
            start(rows, far)
        for rows in WHOLE:
            start(rows, last)

    for side, dest in ((0, 2 * near + core), (1, 2 * near + 1 - core)):
        for chunk in range(CHUNKS):
            near_refs[side * CHUNKS + chunk][...] = send[dest, :, :, pl.ds(128 * chunk, 128)]

    c = c_vm[...]
    spread = (iota((8 * N, N), 0) // 8 == iota((8 * N, N), 1)).astype(BF16)
    rows = lax.dot_general(spread, c, nt, preferred_element_type=F32)
    widen = (iota((N, 8 * N), 0) == iota((N, 8 * N), 1) // 8).astype(BF16)
    full = jnp.dot(rows.astype(BF16), widen, preferred_element_type=F32)
    l4_ref[...] = jnp.where(iota(wide, 0) % 8 == iota(wide, 1) % 8, full, 0.0).astype(BF16)
    l4n_ref[...] = l4_ref[:, pl.ds(pl.multiple_of(128 * near, 128), 128)]
    eye = (iota((N, N), 0) == iota((N, N), 1)).astype(BF16)
    ct_vm[...] = lax.dot_general(eye, c, nt, preferred_element_type=F32).astype(BF16)
    ct_ref[...] = ct_vm[...]

    def third(src, p, first, second):
        g0 = jnp.dot(ct_vm[...], first, preferred_element_type=F32).reshape(8, 8, COLS)
        g1 = jnp.dot(ct_vm[...], second, preferred_element_type=F32).reshape(8, 8, COLS)
        at = pl.multiple_of(N * src + 8 * p, 16)
        g_ref[:, pl.ds(at, 16), :] = jnp.concatenate([g0, g1], axis=1).astype(BF16)

    def own(t, carry):
        third(me, 2 * t, send[me, 2 * t], send[me, 2 * t + 1])
        return carry

    lax.fori_loop(0, ROWS // 2, own, 0)

    def take(groups, sources):
        for rows in groups:
            for src in sources:
                group(rows, src, src).wait_recv()
            if sum(rows) % 2 == 0:
                begin = rows[0] // 2 * 2

                def body(t, carry):
                    for src in sources:
                        p = begin + 2 * t
                        third(src, p, recv[src, p], recv[src, p + 1])
                    return carry

                lax.fori_loop(0, (sum(rows) - begin) // 2, body, 0)

    take(EARLY, [partner])

    @pl.when(jnp.logical_not(is_edge))
    def _():
        g_ref[:, pl.ds(pl.multiple_of(2 * N * near, 16), 2 * N), :] = jnp.zeros((8, 2 * N, COLS), BF16)

    take(EARLY, [2 * beside, 2 * beside + 1])

    for rows in EARLY:
        group(rows, partner, me).wait_send()
    sent(EARLY, beside)

    @pl.when(is_edge)
    def _():
        take(EARLY, [2 * far, 2 * far + 1])
        take(WHOLE, [2 * last, 2 * last + 1])
        sent(LATER, far)
        sent(WHOLE, last)

    @pl.when(jnp.logical_not(is_edge))
    def _():
        take(LATER, [2 * far, 2 * far + 1])
        sent(EARLY, far)


def most_kernel(g_ref, l4_ref, v_ref):
    for ag in range(8):
        v_ref[ag] = jnp.dot(l4_ref[...], g_ref[ag], preferred_element_type=F32)


def chunk_kernel(chunk, same_ref, other_ref, ct_ref, l4n_ref, most_ref, *refs):
    v_hbm, g_vm, v_vm, v_sem = refs[-4:]
    core = lax.axis_index("dev") % 2
    for side, ref in ((core, same_ref), (1 - core, other_ref)):
        for p in range(0, ROWS, 2):
            both = jnp.concatenate([ref[p], ref[p + 1]], axis=1)
            g = jnp.dot(ct_ref[...], both, preferred_element_type=F32)
            g0 = g[:, :128].reshape(8, 8, 128)
            g1 = g[:, 128:].reshape(8, 8, 128)
            at = pl.multiple_of(N * side + 8 * p, 16)
            g_vm[:, pl.ds(at, 16), :] = jnp.concatenate([g0, g1], axis=1).astype(BF16)

    def put(ag):
        return pltpu.make_async_copy(v_vm.at[ag], v_hbm.at[:, pl.ds(8 * ag, 8), pl.ds(128 * chunk, 128)], v_sem.at[ag])

    for ag in range(0, 8, 2):
        both = jnp.concatenate([g_vm[ag], g_vm[ag + 1]], axis=1)
        for m in range(2):
            part = jnp.dot(l4n_ref[256 * m:256 * m + 256, :], both, preferred_element_type=F32)
            for k in range(2):
                most = most_ref[ag + k, 256 * m:256 * m + 256, 128 * chunk:128 * chunk + 128]
                v_vm[ag + k, 32 * m:32 * m + 32] = (part[:, 128 * k:128 * k + 128] + most).reshape(N // 2, 8, 128)
        for k in range(2):
            put(ag + k).start()
    for ag in range(8):
        put(ag).wait()


def solution(mesh):
    def local_transform(ao_rows, coeffs):
        vmem = pl.BlockSpec(memory_space=pltpu.VMEM)
        anywhere = pl.BlockSpec(memory_space=pltpu.HBM)
        sds = jax.ShapeDtypeStruct
        outs = (
            sds((8, 8 * N, COLS), BF16),
            sds((8 * N, 8 * N), BF16),
            sds((8 * N, 2 * N), BF16),
            sds((N, N), BF16),
        ) + (sds((ROWS, N, 128), BF16),) * (2 * CHUNKS)
        g, l4, l4n, ct, *near = pl.pallas_call(
            exchange_kernel,
            out_shape=outs,
            in_specs=[anywhere, anywhere],
            out_specs=(vmem,) * len(outs),
            scratch_shapes=[
                pltpu.VMEM((ROWS, N, N, N), BF16),
                pltpu.VMEM((N, N), BF16),
                pltpu.VMEM((8 * N, 8 * N), BF16),
                pltpu.VMEM((4 * N, 4 * N), BF16),
                pltpu.VMEM((N, N), BF16),
                pltpu.VMEM((DEV, ROWS, N, COLS), BF16),
                pltpu.VMEM((DEV, ROWS, N, COLS), BF16),
                pltpu.SemaphoreType.DMA((ROWS + 1,)),
                pltpu.SemaphoreType.DMA,
                pltpu.SemaphoreType.DMA((DEV, ROWS)),
                pltpu.SemaphoreType.DMA((DEV, ROWS)),
            ],
            compiler_params=pltpu.CompilerParams(collective_id=0, has_side_effects=True, vmem_limit_bytes=40 * 2**20),
            name="exchange",
        )(pltpu.with_memory_space_constraint(ao_rows, pltpu.HBM), pltpu.with_memory_space_constraint(coeffs, pltpu.HBM))
        same = [(2, 4), (3, 5), (4, 2), (5, 3)]
        other = [(2, 5), (3, 4), (4, 3), (5, 2)]
        arrived = []
        for chunk in range(CHUNKS):
            pair = []
            for side, perm in enumerate((same, other)):
                pair.append(lax.ppermute(near[side * CHUNKS + chunk], "dev", perm))
            arrived.append(pair)
        most = pl.pallas_call(
            most_kernel,
            out_shape=sds((8, 8 * N, COLS), F32),
            in_specs=[vmem, vmem],
            out_specs=vmem,
            compiler_params=pltpu.CompilerParams(vmem_limit_bytes=12 * 2**20),
            cost_estimate=pl.CostEstimate(flops=2 * 8 * 512**3, bytes_accessed=12 * 2**20, transcendentals=0),
            name="most",
        )(g, l4)
        v = None
        for chunk in range(CHUNKS):
            operands = (*arrived[chunk], ct, l4n, most) + (() if v is None else (v,))
            v = pl.pallas_call(
                functools.partial(chunk_kernel, chunk),
                out_shape=sds((N, N, COLS), F32),
                in_specs=[vmem] * 5 + ([] if v is None else [anywhere]),
                out_specs=anywhere,
                scratch_shapes=[
                    pltpu.VMEM((8, 2 * N, 128), BF16),
                    pltpu.VMEM((8, N, 8, 128), F32),
                    pltpu.SemaphoreType.DMA((8,)),
                ],
                input_output_aliases={} if v is None else {5: 0},
                compiler_params=pltpu.CompilerParams(vmem_limit_bytes=12 * 2**20),
                cost_estimate=pl.CostEstimate(flops=2 * 8 * 512 * 128 * 128, bytes_accessed=4 * 2**20, transcendentals=0),
            )(*operands)
        return v

    return jax.shard_map(local_transform, mesh=mesh, in_specs=(P(('frag', 'dev')), P('frag')), out_specs=P('frag', None, 'dev'), check_vma=False)
```

```python
import functools

import jax
import jax.numpy as jnp
from jax import lax
from jax.experimental import pallas as pl
from jax.experimental.pallas import tpu as pltpu
from jax.sharding import PartitionSpec as P


N = 64
DEV = 8
ROWS = N // DEV
COLS = N * N // DEV
CHUNKS = COLS // 128
EARLY = ((0, 1), (1, 1), (2, 1), (3, 1), (4, 2), (6, 2))
LATER = ((0, 4), (4, 4))
WHOLE = ((0, 8),)
BF16 = jnp.bfloat16
F32 = jnp.float32


def iota(shape, dim):
    return lax.broadcasted_iota(jnp.int32, shape, dim)


def exchange_kernel(a_hbm, c_hbm, g_ref, l4_ref, l4n_ref, ct_ref, *refs):
    near_refs = refs[:2 * CHUNKS]
    a_vm, c_vm, l_vm, b4_vm, ct_vm, send, recv, a_sem, c_sem, send_sem, recv_sem = refs[2 * CHUNKS:]
    me = lax.axis_index("dev")
    chip = me // 2
    core = me % 2

    load_c = pltpu.make_async_copy(c_hbm, c_vm, c_sem)
    load_c.start()

    def load_row(p):
        return pltpu.make_async_copy(a_hbm.at[p], a_vm.at[p], a_sem.at[p])

    def load_half(h):
        half = pl.ds(32 * h, 32)
        return pltpu.make_async_copy(a_hbm.at[0, half], a_vm.at[0, half], a_sem.at[ROWS * h])

    for h in range(2):
        load_half(h).start()

    barrier = pltpu.get_barrier_semaphore()
    for k in range(1, DEV):
        pl.semaphore_signal(barrier, inc=1, device_id={"dev": (me + k) % DEV}, device_id_type=pl.DeviceIdType.MESH)

    load_c.wait()
    load_row(1).start()
    c = c_vm[...]
    nt = (((1,), (1,)), ((), ()))
    wide = (8 * N, 8 * N)

    def kron_rows(first_m, count):
        spread = (iota((8 * count, N), 0) // 8 + first_m == iota((8 * count, N), 1)).astype(BF16)
        rows = lax.dot_general(spread, c, nt, preferred_element_type=F32)
        pair = jnp.concatenate([rows, rows], axis=1)
        tiled = jnp.concatenate([pair] * 4, axis=1)
        shape = (8 * count, 8 * N)
        return jnp.where(iota(shape, 0) % 8 == iota(shape, 1) // N, tiled, 0.0).astype(BF16)

    cf = c.astype(F32)
    cpair = jnp.concatenate([cf, cf], axis=1)
    c4 = jnp.concatenate([cpair, cpair], axis=1)
    c44 = jnp.concatenate([c4] * 4, axis=0)
    quad = (4 * N, 4 * N)
    b4_vm[...] = jnp.where(iota(quad, 0) // N == iota(quad, 1) // N, c44, 0.0).astype(BF16)

    def group(rows, dest, src):
        part = pl.ds(*rows)
        return pltpu.make_async_remote_copy(
            src_ref=send.at[dest, part],
            dst_ref=recv.at[src, part],
            send_sem=send_sem.at[dest, rows[0]],
            recv_sem=recv_sem.at[src, rows[0]],
            device_id={"dev": dest},
            device_id_type=pl.DeviceIdType.MESH,
        )

    def start(rows, to):
        for k in range(2):
            group(rows, 2 * to + k, me).start()

    def sent(groups, to):
        for rows in groups:
            for k in range(2):
                group(rows, 2 * to + k, me).wait_send()

    low = iota((32, 8, 128), 2) < N

    def pieces(p, h, lhs, count, put):
        a = a_vm[p, pl.ds(32 * h, 32)].reshape(4, 8 * N, N)
        left = jnp.concatenate([a[0], a[1]], axis=1)
        right = jnp.concatenate([a[2], a[3]], axis=1)
        a4 = jnp.concatenate([left, right], axis=1)
        t_one = jnp.dot(lhs, a4, preferred_element_type=F32).astype(BF16)
        half = jnp.dot(t_one, b4_vm[...], preferred_element_type=F32)
        pairs = half.reshape(count, 2, 8, 256)
        for t in range(2):
            even = pairs[:, 0, :, 128 * t:128 * t + 128]
            odd = pairs[:, 1, :, 128 * t:128 * t + 128]
            first_rows = jnp.where(low[:count], even, pltpu.roll(odd, N, 2))
            second_rows = jnp.where(low[:count], pltpu.roll(even, N, 2), odd)
            both = jnp.concatenate([first_rows, second_rows], axis=1).astype(BF16)
            for jp in range(count):
                put(jp // 4, pl.ds(32 * h + 16 * t, 16), pl.ds(128 * (jp % 4), 128), both[jp])

    def half_row(p, h):
        def put(dest, q, columns, value):
            send[dest, p, q, columns] = value

        pieces(p, h, l_vm[...], 32, put)

    def chip_piece(p, to, lhs):
        def put(dest, q, columns, value):
            send[2 * to + dest, p, q, columns] = value

        for h in range(2):
            pieces(p, h, lhs, 8, put)

    is_edge = jnp.logical_or(chip == 0, chip == 3)
    inward = jnp.where(chip < 2, 1, -1)
    partner = 2 * chip + 1 - core
    near = chip + inward
    far = chip + 2 * inward
    last = chip + 3 * inward
    outward = chip - inward
    beside = jnp.where(is_edge, near, outward)

    first_chip = jnp.where(is_edge, near, far)
    l_vm[:128, :] = kron_rows(16 * first_chip, 16)
    for h in range(2):
        load_half(h).wait()
    load_row(2).start()
    chip_piece(0, first_chip, l_vm[:128, :])
    pl.semaphore_wait(barrier, DEV - 1)
    start(EARLY[0], first_chip)
    load_row(1).wait()
    load_row(3).start()
    chip_piece(1, first_chip, l_vm[:128, :])
    start(EARLY[1], first_chip)

    l_vm[...] = kron_rows(0, N)
    second_chip = jnp.where(is_edge, far, outward)
    fourth_chip = jnp.where(is_edge, last, near)
    for p in range(2):
        for to in (second_chip, fourth_chip, chip):
            chip_piece(p, to, l_vm[pl.ds(pl.multiple_of(128 * to, 128), 128), :])
        group(EARLY[p], partner, me).start()

        @pl.when(jnp.logical_not(is_edge))
        def _():
            start(EARLY[p], outward)

    def make_row(p, carry):
        load_row(p).wait()

        @pl.when(p < ROWS - 2)
        def _():
            load_row(p + 2).start()

        for h in range(2):
            half_row(p, h)
        for rows in EARLY[2:]:
            @pl.when(p == sum(rows) - 1)
            def _():
                start(rows, beside)

                @pl.when(jnp.logical_not(is_edge))
                def _():
                    start(rows, far)

                group(rows, partner, me).start()

        return carry

    lax.fori_loop(2, ROWS, make_row, 0)

    @pl.when(is_edge)
    def _():
        for rows in LATER:
            start(rows, far)
        for rows in WHOLE:
            start(rows, last)

    for side, dest in ((0, 2 * near + core), (1, 2 * near + 1 - core)):
        for chunk in range(CHUNKS):
            near_refs[side * CHUNKS + chunk][...] = send[dest, :, :, pl.ds(128 * chunk, 128)]

    c = c_vm[...]
    spread = (iota((8 * N, N), 0) // 8 == iota((8 * N, N), 1)).astype(BF16)
    rows = lax.dot_general(spread, c, nt, preferred_element_type=F32)
    widen = (iota((N, 8 * N), 0) == iota((N, 8 * N), 1) // 8).astype(BF16)
    full = jnp.dot(rows.astype(BF16), widen, preferred_element_type=F32)
    l4_ref[...] = jnp.where(iota(wide, 0) % 8 == iota(wide, 1) % 8, full, 0.0).astype(BF16)
    l4n_ref[...] = l4_ref[:, pl.ds(pl.multiple_of(128 * near, 128), 128)]
    eye = (iota((N, N), 0) == iota((N, N), 1)).astype(BF16)
    ct_vm[...] = lax.dot_general(eye, c, nt, preferred_element_type=F32).astype(BF16)
    ct_ref[...] = ct_vm[...]

    def third(src, p, first, second):
        g0 = jnp.dot(ct_vm[...], first, preferred_element_type=F32).reshape(8, 8, COLS)
        g1 = jnp.dot(ct_vm[...], second, preferred_element_type=F32).reshape(8, 8, COLS)
        at = pl.multiple_of(N * src + 8 * p, 16)
        g_ref[:, pl.ds(at, 16), :] = jnp.concatenate([g0, g1], axis=1).astype(BF16)

    def own(t, carry):
        third(me, 2 * t, send[me, 2 * t], send[me, 2 * t + 1])
        return carry

    lax.fori_loop(0, ROWS // 2, own, 0)

    def take(groups, sources):
        for rows in groups:
            for src in sources:
                group(rows, src, src).wait_recv()
            if sum(rows) % 2 == 0:
                begin = rows[0] // 2 * 2

                def body(t, carry):
                    for src in sources:
                        p = begin + 2 * t
                        third(src, p, recv[src, p], recv[src, p + 1])
                    return carry

                lax.fori_loop(0, (sum(rows) - begin) // 2, body, 0)

    take(EARLY, [partner])

    @pl.when(jnp.logical_not(is_edge))
    def _():
        g_ref[:, pl.ds(pl.multiple_of(2 * N * near, 16), 2 * N), :] = jnp.zeros((8, 2 * N, COLS), BF16)

    take(EARLY, [2 * beside, 2 * beside + 1])

    for rows in EARLY:
        group(rows, partner, me).wait_send()
    sent(EARLY, beside)

    @pl.when(is_edge)
    def _():
        take(EARLY, [2 * far, 2 * far + 1])
        take(WHOLE, [2 * last, 2 * last + 1])
        sent(LATER, far)
        sent(WHOLE, last)

    @pl.when(jnp.logical_not(is_edge))
    def _():
        take(LATER, [2 * far, 2 * far + 1])
        sent(EARLY, far)


def most_kernel(g_ref, l4_ref, v_ref):
    for ag in range(8):
        v_ref[ag] = jnp.dot(l4_ref[...], g_ref[ag], preferred_element_type=F32)


def chunk_kernel(chunk, same_ref, other_ref, ct_ref, l4n_ref, most_ref, *refs):
    v_hbm, g_vm, v_vm, v_sem = refs[-4:]
    core = lax.axis_index("dev") % 2
    for side, ref in ((core, same_ref), (1 - core, other_ref)):
        for p in range(0, ROWS, 2):
            both = jnp.concatenate([ref[p], ref[p + 1]], axis=1)
            g = jnp.dot(ct_ref[...], both, preferred_element_type=F32)
            g0 = g[:, :128].reshape(8, 8, 128)
            g1 = g[:, 128:].reshape(8, 8, 128)
            at = pl.multiple_of(N * side + 8 * p, 16)
            g_vm[:, pl.ds(at, 16), :] = jnp.concatenate([g0, g1], axis=1).astype(BF16)

    def put(m):
        part = pl.ds(16 * m, 16)
        return pltpu.make_async_copy(v_vm.at[part], v_hbm.at[part, :, pl.ds(128 * chunk, 128)], v_sem.at[m])

    for m in range(4):
        rows = slice(128 * m, 128 * m + 128)
        for ag in range(0, 8, 2):
            both = jnp.concatenate([g_vm[ag], g_vm[ag + 1]], axis=1)
            part = jnp.dot(l4n_ref[rows, :], both, preferred_element_type=F32)
            for k in range(2):
                most = most_ref[ag + k, rows, 128 * chunk:128 * chunk + 128]
                value = (part[:, 128 * k:128 * k + 128] + most).reshape(16, 8, 128)
                v_vm[16 * m:16 * m + 16, 8 * (ag + k):8 * (ag + k) + 8, :] = value
        put(m).start()
    for m in range(4):
        put(m).wait()


def solution(mesh):
    def local_transform(ao_rows, coeffs):
        vmem = pl.BlockSpec(memory_space=pltpu.VMEM)
        anywhere = pl.BlockSpec(memory_space=pltpu.HBM)
        sds = jax.ShapeDtypeStruct
        outs = (
            sds((8, 8 * N, COLS), BF16),
            sds((8 * N, 8 * N), BF16),
            sds((8 * N, 2 * N), BF16),
            sds((N, N), BF16),
        ) + (sds((ROWS, N, 128), BF16),) * (2 * CHUNKS)
        g, l4, l4n, ct, *near = pl.pallas_call(
            exchange_kernel,
            out_shape=outs,
            in_specs=[anywhere, anywhere],
            out_specs=(vmem,) * len(outs),
            scratch_shapes=[
                pltpu.VMEM((ROWS, N, N, N), BF16),
                pltpu.VMEM((N, N), BF16),
                pltpu.VMEM((8 * N, 8 * N), BF16),
                pltpu.VMEM((4 * N, 4 * N), BF16),
                pltpu.VMEM((N, N), BF16),
                pltpu.VMEM((DEV, ROWS, N, COLS), BF16),
                pltpu.VMEM((DEV, ROWS, N, COLS), BF16),
                pltpu.SemaphoreType.DMA((ROWS + 1,)),
                pltpu.SemaphoreType.DMA,
                pltpu.SemaphoreType.DMA((DEV, ROWS)),
                pltpu.SemaphoreType.DMA((DEV, ROWS)),
            ],
            compiler_params=pltpu.CompilerParams(collective_id=0, has_side_effects=True, vmem_limit_bytes=40 * 2**20),
            name="exchange",
        )(pltpu.with_memory_space_constraint(ao_rows, pltpu.HBM), pltpu.with_memory_space_constraint(coeffs, pltpu.HBM))
        same = [(2, 4), (3, 5), (4, 2), (5, 3)]
        other = [(2, 5), (3, 4), (4, 3), (5, 2)]
        arrived = []
        for chunk in range(CHUNKS):
            pair = []
            for side, perm in enumerate((same, other)):
                pair.append(lax.ppermute(near[side * CHUNKS + chunk], "dev", perm))
            arrived.append(pair)
        most = pl.pallas_call(
            most_kernel,
            out_shape=sds((8, 8 * N, COLS), F32),
            in_specs=[vmem, vmem],
            out_specs=vmem,
            compiler_params=pltpu.CompilerParams(vmem_limit_bytes=12 * 2**20),
            cost_estimate=pl.CostEstimate(flops=2 * 8 * 512**3, bytes_accessed=12 * 2**20, transcendentals=0),
            name="most",
        )(g, l4)
        v = None
        for chunk in range(CHUNKS):
            operands = (*arrived[chunk], ct, l4n, most) + (() if v is None else (v,))
            v = pl.pallas_call(
                functools.partial(chunk_kernel, chunk),
                out_shape=sds((N, N, COLS), F32),
                in_specs=[vmem] * 5 + ([] if v is None else [anywhere]),
                out_specs=anywhere,
                scratch_shapes=[
                    pltpu.VMEM((8, 2 * N, 128), BF16),
                    pltpu.VMEM((N, N, 128), F32),
                    pltpu.SemaphoreType.DMA((4,)),
                ],
                input_output_aliases={} if v is None else {5: 0},
                compiler_params=pltpu.CompilerParams(vmem_limit_bytes=12 * 2**20),
                cost_estimate=pl.CostEstimate(flops=2 * 8 * 512 * 128 * 128, bytes_accessed=4 * 2**20, transcendentals=0),
            )(*operands)
        return v

    return jax.shard_map(local_transform, mesh=mesh, in_specs=(P(('frag', 'dev')), P('frag')), out_specs=P('frag', None, 'dev'), check_vma=False)
```

```python
import functools

import jax
import jax.numpy as jnp
from jax import lax
from jax.experimental import pallas as pl
from jax.experimental.pallas import tpu as pltpu
from jax.sharding import PartitionSpec as P


N = 64
DEV = 8
ROWS = N // DEV
COLS = N * N // DEV
CHUNKS = COLS // 128
EARLY = ((0, 1), (1, 1), (2, 1), (3, 1), (4, 2), (6, 2))
LATER = ((0, 4), (4, 4))
WHOLE = ((0, 8),)
BF16 = jnp.bfloat16
F32 = jnp.float32


def iota(shape, dim):
    return lax.broadcasted_iota(jnp.int32, shape, dim)


def exchange_kernel(a_hbm, c_hbm, g_ref, l4_ref, l4n_ref, ct_ref, *refs):
    near_refs = refs[:2 * CHUNKS]
    a_vm, c_vm, l_vm, b4_vm, ct_vm, send, recv, a_sem, c_sem, send_sem, recv_sem = refs[2 * CHUNKS:]
    me = lax.axis_index("dev")
    chip = me // 2
    core = me % 2

    load_c = pltpu.make_async_copy(c_hbm, c_vm, c_sem)

    def load_row(p):
        return pltpu.make_async_copy(a_hbm.at[p], a_vm.at[p], a_sem.at[p])

    def load_half(h):
        half = pl.ds(32 * h, 32)
        return pltpu.make_async_copy(a_hbm.at[0, half], a_vm.at[0, half], a_sem.at[ROWS * h])

    load_half(0).start()
    load_c.start()
    load_half(1).start()

    barrier = pltpu.get_barrier_semaphore()
    for k in range(1, DEV):
        pl.semaphore_signal(barrier, inc=1, device_id={"dev": (me + k) % DEV}, device_id_type=pl.DeviceIdType.MESH)

    load_c.wait()
    c = c_vm[...]
    nt = (((1,), (1,)), ((), ()))
    wide = (8 * N, 8 * N)

    def kron_rows(first_m, count):
        spread = (iota((8 * count, N), 0) // 8 + first_m == iota((8 * count, N), 1)).astype(BF16)
        rows = lax.dot_general(spread, c, nt, preferred_element_type=F32)
        pair = jnp.concatenate([rows, rows], axis=1)
        tiled = jnp.concatenate([pair] * 4, axis=1)
        shape = (8 * count, 8 * N)
        return jnp.where(iota(shape, 0) % 8 == iota(shape, 1) // N, tiled, 0.0).astype(BF16)

    cf = c.astype(F32)
    cpair = jnp.concatenate([cf, cf], axis=1)
    c4 = jnp.concatenate([cpair, cpair], axis=1)
    c44 = jnp.concatenate([c4] * 4, axis=0)
    quad = (4 * N, 4 * N)
    b4_vm[...] = jnp.where(iota(quad, 0) // N == iota(quad, 1) // N, c44, 0.0).astype(BF16)

    def group(rows, dest, src):
        part = pl.ds(*rows)
        return pltpu.make_async_remote_copy(
            src_ref=send.at[dest, part],
            dst_ref=recv.at[src, part],
            send_sem=send_sem.at[dest, rows[0]],
            recv_sem=recv_sem.at[src, rows[0]],
            device_id={"dev": dest},
            device_id_type=pl.DeviceIdType.MESH,
        )

    def half(h, dest, src):
        part = pl.ds(32 * h, 32)
        return pltpu.make_async_remote_copy(
            src_ref=send.at[dest, 0, part],
            dst_ref=recv.at[src, 0, part],
            send_sem=send_sem.at[dest, ROWS * h],
            recv_sem=recv_sem.at[src, ROWS * h],
            device_id={"dev": dest},
            device_id_type=pl.DeviceIdType.MESH,
        )

    def copies(rows, dest, src):
        if rows == EARLY[0]:
            return [half(h, dest, src) for h in range(2)]
        return [group(rows, dest, src)]

    def start(rows, to):
        for k in range(2):
            for copy in copies(rows, 2 * to + k, me):
                copy.start()

    def sent(groups, to):
        for rows in groups:
            for k in range(2):
                for copy in copies(rows, 2 * to + k, me):
                    copy.wait_send()

    low = iota((32, 8, 128), 2) < N

    def pieces(p, h, lhs, count, put):
        a = a_vm[p, pl.ds(32 * h, 32)].reshape(4, 8 * N, N)
        left = jnp.concatenate([a[0], a[1]], axis=1)
        right = jnp.concatenate([a[2], a[3]], axis=1)
        a4 = jnp.concatenate([left, right], axis=1)
        t_one = jnp.dot(lhs, a4, preferred_element_type=F32).astype(BF16)
        half = jnp.dot(t_one, b4_vm[...], preferred_element_type=F32)
        pairs = half.reshape(count, 2, 8, 256)
        for t in range(2):
            even = pairs[:, 0, :, 128 * t:128 * t + 128]
            odd = pairs[:, 1, :, 128 * t:128 * t + 128]
            first_rows = jnp.where(low[:count], even, pltpu.roll(odd, N, 2))
            second_rows = jnp.where(low[:count], pltpu.roll(even, N, 2), odd)
            both = jnp.concatenate([first_rows, second_rows], axis=1).astype(BF16)
            for jp in range(count):
                put(jp // 4, pl.ds(32 * h + 16 * t, 16), pl.ds(128 * (jp % 4), 128), both[jp])

    def half_row(p, h):
        def put(dest, q, columns, value):
            send[dest, p, q, columns] = value

        pieces(p, h, l_vm[...], 32, put)

    def chip_piece(p, halves, to, lhs):
        def put(dest, q, columns, value):
            send[2 * to + dest, p, q, columns] = value

        for h in halves:
            pieces(p, h, lhs, 8, put)

    is_edge = jnp.logical_or(chip == 0, chip == 3)
    inward = jnp.where(chip < 2, 1, -1)
    partner = 2 * chip + 1 - core
    near = chip + inward
    far = chip + 2 * inward
    last = chip + 3 * inward
    outward = chip - inward
    beside = jnp.where(is_edge, near, outward)

    first_chip = jnp.where(is_edge, near, far)
    l_vm[:128, :] = kron_rows(16 * first_chip, 16)
    for h in range(2):
        load_half(h).wait()
        if h == 1:
            for later in (1, 2):
                load_row(later).start()
        chip_piece(0, (h,), first_chip, l_vm[:128, :])
        if h == 0:
            pl.semaphore_wait(barrier, DEV - 1)
        for k in range(2):
            half(h, 2 * first_chip + k, me).start()
    load_row(1).wait()
    load_row(3).start()
    chip_piece(1, range(2), first_chip, l_vm[:128, :])
    start(EARLY[1], first_chip)

    l_vm[...] = kron_rows(0, N)
    second_chip = jnp.where(is_edge, far, outward)
    fourth_chip = jnp.where(is_edge, last, near)
    for p in range(2):
        for to in (second_chip, fourth_chip, chip):
            chip_piece(p, range(2), to, l_vm[pl.ds(pl.multiple_of(128 * to, 128), 128), :])
        for copy in copies(EARLY[p], partner, me):
            copy.start()

        @pl.when(jnp.logical_not(is_edge))
        def _():
            start(EARLY[p], outward)

    def make_row(p, carry):
        load_row(p).wait()

        @pl.when(p < ROWS - 2)
        def _():
            load_row(p + 2).start()

        for h in range(2):
            half_row(p, h)
        for rows in EARLY[2:]:
            @pl.when(p == sum(rows) - 1)
            def _():
                start(rows, beside)

                @pl.when(jnp.logical_not(is_edge))
                def _():
                    start(rows, far)

                group(rows, partner, me).start()

        return carry

    lax.fori_loop(2, ROWS, make_row, 0)

    @pl.when(is_edge)
    def _():
        for rows in LATER:
            start(rows, far)
        for rows in WHOLE:
            start(rows, last)

    for side, dest in ((0, 2 * near + core), (1, 2 * near + 1 - core)):
        for chunk in range(CHUNKS):
            near_refs[side * CHUNKS + chunk][...] = send[dest, :, :, pl.ds(128 * chunk, 128)]

    c = c_vm[...]
    spread = (iota((8 * N, N), 0) // 8 == iota((8 * N, N), 1)).astype(BF16)
    rows = lax.dot_general(spread, c, nt, preferred_element_type=F32)
    widen = (iota((N, 8 * N), 0) == iota((N, 8 * N), 1) // 8).astype(BF16)
    full = jnp.dot(rows.astype(BF16), widen, preferred_element_type=F32)
    l4_ref[...] = jnp.where(iota(wide, 0) % 8 == iota(wide, 1) % 8, full, 0.0).astype(BF16)
    l4n_ref[...] = l4_ref[:, pl.ds(pl.multiple_of(128 * near, 128), 128)]
    eye = (iota((N, N), 0) == iota((N, N), 1)).astype(BF16)
    ct_vm[...] = lax.dot_general(eye, c, nt, preferred_element_type=F32).astype(BF16)
    ct_ref[...] = ct_vm[...]

    def third(src, p, first, second):
        g0 = jnp.dot(ct_vm[...], first, preferred_element_type=F32).reshape(8, 8, COLS)
        g1 = jnp.dot(ct_vm[...], second, preferred_element_type=F32).reshape(8, 8, COLS)
        at = pl.multiple_of(N * src + 8 * p, 16)
        g_ref[:, pl.ds(at, 16), :] = jnp.concatenate([g0, g1], axis=1).astype(BF16)

    def own(t, carry):
        third(me, 2 * t, send[me, 2 * t], send[me, 2 * t + 1])
        return carry

    lax.fori_loop(0, ROWS // 2, own, 0)

    def take(groups, sources):
        for rows in groups:
            for src in sources:
                for copy in copies(rows, src, src):
                    copy.wait_recv()
            if sum(rows) % 2 == 0:
                begin = rows[0] // 2 * 2

                def body(t, carry):
                    for src in sources:
                        p = begin + 2 * t
                        third(src, p, recv[src, p], recv[src, p + 1])
                    return carry

                lax.fori_loop(0, (sum(rows) - begin) // 2, body, 0)

    take(EARLY, [partner])

    @pl.when(jnp.logical_not(is_edge))
    def _():
        g_ref[:, pl.ds(pl.multiple_of(2 * N * near, 16), 2 * N), :] = jnp.zeros((8, 2 * N, COLS), BF16)

    take(EARLY, [2 * beside, 2 * beside + 1])

    for rows in EARLY:
        for copy in copies(rows, partner, me):
            copy.wait_send()
    sent(EARLY, beside)

    @pl.when(is_edge)
    def _():
        take(EARLY, [2 * far, 2 * far + 1])
        take(WHOLE, [2 * last, 2 * last + 1])
        sent(LATER, far)
        sent(WHOLE, last)

    @pl.when(jnp.logical_not(is_edge))
    def _():
        take(LATER, [2 * far, 2 * far + 1])
        sent(EARLY, far)


def most_kernel(g_ref, l4_ref, v_ref):
    for ag in range(8):
        v_ref[ag] = jnp.dot(l4_ref[...], g_ref[ag], preferred_element_type=F32)


def chunk_kernel(chunk, same_ref, other_ref, ct_ref, l4n_ref, most_ref, *refs):
    v_hbm, g_vm, v_vm, v_sem = refs[-4:]
    core = lax.axis_index("dev") % 2
    for side, ref in ((core, same_ref), (1 - core, other_ref)):
        for p in range(0, ROWS, 2):
            both = jnp.concatenate([ref[p], ref[p + 1]], axis=1)
            g = jnp.dot(ct_ref[...], both, preferred_element_type=F32)
            g0 = g[:, :128].reshape(8, 8, 128)
            g1 = g[:, 128:].reshape(8, 8, 128)
            at = pl.multiple_of(N * side + 8 * p, 16)
            g_vm[:, pl.ds(at, 16), :] = jnp.concatenate([g0, g1], axis=1).astype(BF16)

    def put(m):
        part = pl.ds(16 * m, 16)
        return pltpu.make_async_copy(v_vm.at[part], v_hbm.at[part, :, pl.ds(128 * chunk, 128)], v_sem.at[m])

    for m in range(4):
        rows = slice(128 * m, 128 * m + 128)
        for ag in range(0, 8, 2):
            both = jnp.concatenate([g_vm[ag], g_vm[ag + 1]], axis=1)
            part = jnp.dot(l4n_ref[rows, :], both, preferred_element_type=F32)
            for k in range(2):
                most = most_ref[ag + k, rows, 128 * chunk:128 * chunk + 128]
                value = (part[:, 128 * k:128 * k + 128] + most).reshape(16, 8, 128)
                v_vm[16 * m:16 * m + 16, 8 * (ag + k):8 * (ag + k) + 8, :] = value
        put(m).start()
    for m in range(4):
        put(m).wait()


def solution(mesh):
    def local_transform(ao_rows, coeffs):
        vmem = pl.BlockSpec(memory_space=pltpu.VMEM)
        anywhere = pl.BlockSpec(memory_space=pltpu.HBM)
        sds = jax.ShapeDtypeStruct
        outs = (
            sds((8, 8 * N, COLS), BF16),
            sds((8 * N, 8 * N), BF16),
            sds((8 * N, 2 * N), BF16),
            sds((N, N), BF16),
        ) + (sds((ROWS, N, 128), BF16),) * (2 * CHUNKS)
        g, l4, l4n, ct, *near = pl.pallas_call(
            exchange_kernel,
            out_shape=outs,
            in_specs=[anywhere, anywhere],
            out_specs=(vmem,) * len(outs),
            scratch_shapes=[
                pltpu.VMEM((ROWS, N, N, N), BF16),
                pltpu.VMEM((N, N), BF16),
                pltpu.VMEM((8 * N, 8 * N), BF16),
                pltpu.VMEM((4 * N, 4 * N), BF16),
                pltpu.VMEM((N, N), BF16),
                pltpu.VMEM((DEV, ROWS, N, COLS), BF16),
                pltpu.VMEM((DEV, ROWS, N, COLS), BF16),
                pltpu.SemaphoreType.DMA((ROWS + 1,)),
                pltpu.SemaphoreType.DMA,
                pltpu.SemaphoreType.DMA((DEV, ROWS + 1)),
                pltpu.SemaphoreType.DMA((DEV, ROWS + 1)),
            ],
            compiler_params=pltpu.CompilerParams(collective_id=0, has_side_effects=True, vmem_limit_bytes=40 * 2**20),
            name="exchange",
        )(pltpu.with_memory_space_constraint(ao_rows, pltpu.HBM), pltpu.with_memory_space_constraint(coeffs, pltpu.HBM))
        same = [(2, 4), (3, 5), (4, 2), (5, 3)]
        other = [(2, 5), (3, 4), (4, 3), (5, 2)]
        arrived = []
        for chunk in range(CHUNKS):
            pair = []
            for side, perm in enumerate((same, other)):
                pair.append(lax.ppermute(near[side * CHUNKS + chunk], "dev", perm))
            arrived.append(pair)
        most = pl.pallas_call(
            most_kernel,
            out_shape=sds((8, 8 * N, COLS), F32),
            in_specs=[vmem, vmem],
            out_specs=vmem,
            compiler_params=pltpu.CompilerParams(vmem_limit_bytes=12 * 2**20),
            cost_estimate=pl.CostEstimate(flops=2 * 8 * 512**3, bytes_accessed=12 * 2**20, transcendentals=0),
            name="most",
        )(g, l4)
        v = None
        for chunk in range(CHUNKS):
            operands = (*arrived[chunk], ct, l4n, most) + (() if v is None else (v,))
            v = pl.pallas_call(
                functools.partial(chunk_kernel, chunk),
                out_shape=sds((N, N, COLS), F32),
                in_specs=[vmem] * 5 + ([] if v is None else [anywhere]),
                out_specs=anywhere,
                scratch_shapes=[
                    pltpu.VMEM((8, 2 * N, 128), BF16),
                    pltpu.VMEM((N, N, 128), F32),
                    pltpu.SemaphoreType.DMA((4,)),
                ],
                input_output_aliases={} if v is None else {5: 0},
                compiler_params=pltpu.CompilerParams(vmem_limit_bytes=12 * 2**20),
                cost_estimate=pl.CostEstimate(flops=2 * 8 * 512 * 128 * 128, bytes_accessed=4 * 2**20, transcendentals=0),
            )(*operands)
        return v

    return jax.shard_map(local_transform, mesh=mesh, in_specs=(P(('frag', 'dev')), P('frag')), out_specs=P('frag', None, 'dev'), check_vma=False)
```

```python
import functools

import jax
import jax.numpy as jnp
from jax import lax
from jax.experimental import pallas as pl
from jax.experimental.pallas import tpu as pltpu
from jax.sharding import PartitionSpec as P


N = 64
DEV = 8
ROWS = N // DEV
COLS = N * N // DEV
CHUNKS = COLS // 128
EARLY = ((0, 1), (1, 1), (2, 1), (3, 1), (4, 2), (6, 2))
LATER = ((0, 2), (2, 2), (4, 2), (6, 2))
WHOLE = ((0, 2), (2, 2), (4, 2), (6, 2))
BF16 = jnp.bfloat16
F32 = jnp.float32


def iota(shape, dim):
    return lax.broadcasted_iota(jnp.int32, shape, dim)


def exchange_kernel(a_hbm, c_hbm, g_ref, l4_ref, l4n_ref, ct_ref, *refs):
    near_refs = refs[:2 * CHUNKS]
    a_vm, c_vm, l_vm, b4_vm, ct_vm, send, recv, a_sem, c_sem, send_sem, recv_sem = refs[2 * CHUNKS:]
    me = lax.axis_index("dev")
    chip = me // 2
    core = me % 2

    load_c = pltpu.make_async_copy(c_hbm, c_vm, c_sem)

    def load_row(p):
        return pltpu.make_async_copy(a_hbm.at[p], a_vm.at[p], a_sem.at[p])

    def load_half(h):
        half = pl.ds(32 * h, 32)
        return pltpu.make_async_copy(a_hbm.at[0, half], a_vm.at[0, half], a_sem.at[ROWS * h])

    load_half(0).start()
    load_c.start()
    load_half(1).start()

    barrier = pltpu.get_barrier_semaphore()
    for k in range(1, DEV):
        pl.semaphore_signal(barrier, inc=1, device_id={"dev": (me + k) % DEV}, device_id_type=pl.DeviceIdType.MESH)

    load_c.wait()
    c = c_vm[...]
    nt = (((1,), (1,)), ((), ()))
    wide = (8 * N, 8 * N)

    def kron_rows(first_m, count):
        spread = (iota((8 * count, N), 0) // 8 + first_m == iota((8 * count, N), 1)).astype(BF16)
        rows = lax.dot_general(spread, c, nt, preferred_element_type=F32)
        pair = jnp.concatenate([rows, rows], axis=1)
        tiled = jnp.concatenate([pair] * 4, axis=1)
        shape = (8 * count, 8 * N)
        return jnp.where(iota(shape, 0) % 8 == iota(shape, 1) // N, tiled, 0.0).astype(BF16)

    cf = c.astype(F32)
    cpair = jnp.concatenate([cf, cf], axis=1)
    c4 = jnp.concatenate([cpair, cpair], axis=1)
    c44 = jnp.concatenate([c4] * 4, axis=0)
    quad = (4 * N, 4 * N)
    b4_vm[...] = jnp.where(iota(quad, 0) // N == iota(quad, 1) // N, c44, 0.0).astype(BF16)

    def group(rows, dest, src):
        part = pl.ds(*rows)
        return pltpu.make_async_remote_copy(
            src_ref=send.at[dest, part],
            dst_ref=recv.at[src, part],
            send_sem=send_sem.at[dest, rows[0]],
            recv_sem=recv_sem.at[src, rows[0]],
            device_id={"dev": dest},
            device_id_type=pl.DeviceIdType.MESH,
        )

    def half(h, dest, src):
        part = pl.ds(32 * h, 32)
        return pltpu.make_async_remote_copy(
            src_ref=send.at[dest, 0, part],
            dst_ref=recv.at[src, 0, part],
            send_sem=send_sem.at[dest, ROWS * h],
            recv_sem=recv_sem.at[src, ROWS * h],
            device_id={"dev": dest},
            device_id_type=pl.DeviceIdType.MESH,
        )

    def copies(rows, dest, src):
        if rows == EARLY[0]:
            return [half(h, dest, src) for h in range(2)]
        return [group(rows, dest, src)]

    def start(rows, to):
        for k in range(2):
            for copy in copies(rows, 2 * to + k, me):
                copy.start()

    def sent(groups, to):
        for rows in groups:
            for k in range(2):
                for copy in copies(rows, 2 * to + k, me):
                    copy.wait_send()

    low = iota((32, 8, 128), 2) < N

    def pieces(p, h, lhs, count, put):
        a = a_vm[p, pl.ds(32 * h, 32)].reshape(4, 8 * N, N)
        left = jnp.concatenate([a[0], a[1]], axis=1)
        right = jnp.concatenate([a[2], a[3]], axis=1)
        a4 = jnp.concatenate([left, right], axis=1)
        t_one = jnp.dot(lhs, a4, preferred_element_type=F32).astype(BF16)
        half = jnp.dot(t_one, b4_vm[...], preferred_element_type=F32)
        pairs = half.reshape(count, 2, 8, 256)
        for t in range(2):
            even = pairs[:, 0, :, 128 * t:128 * t + 128]
            odd = pairs[:, 1, :, 128 * t:128 * t + 128]
            first_rows = jnp.where(low[:count], even, pltpu.roll(odd, N, 2))
            second_rows = jnp.where(low[:count], pltpu.roll(even, N, 2), odd)
            both = jnp.concatenate([first_rows, second_rows], axis=1).astype(BF16)
            for jp in range(count):
                put(jp // 4, pl.ds(32 * h + 16 * t, 16), pl.ds(128 * (jp % 4), 128), both[jp])

    def half_row(p, h):
        def put(dest, q, columns, value):
            send[dest, p, q, columns] = value

        pieces(p, h, l_vm[...], 32, put)

    def chip_piece(p, halves, to, lhs):
        def put(dest, q, columns, value):
            send[2 * to + dest, p, q, columns] = value

        for h in halves:
            pieces(p, h, lhs, 8, put)

    is_edge = jnp.logical_or(chip == 0, chip == 3)
    inward = jnp.where(chip < 2, 1, -1)
    partner = 2 * chip + 1 - core
    near = chip + inward
    far = chip + 2 * inward
    last = chip + 3 * inward
    outward = chip - inward
    beside = jnp.where(is_edge, near, outward)

    first_chip = jnp.where(is_edge, near, far)
    l_vm[:128, :] = kron_rows(16 * first_chip, 16)
    for h in range(2):
        load_half(h).wait()
        if h == 1:
            for later in (1, 2):
                load_row(later).start()
        chip_piece(0, (h,), first_chip, l_vm[:128, :])
        if h == 0:
            pl.semaphore_wait(barrier, DEV - 1)
        for k in range(2):
            half(h, 2 * first_chip + k, me).start()
    load_row(1).wait()
    load_row(3).start()
    chip_piece(1, range(2), first_chip, l_vm[:128, :])
    start(EARLY[1], first_chip)

    l_vm[...] = kron_rows(0, N)

    def make_row(p, carry):
        load_row(p).wait()

        @pl.when(p < ROWS - 2)
        def _():
            load_row(p + 2).start()

        for h in range(2):
            half_row(p, h)
        for rows in EARLY[2:]:
            @pl.when(p == sum(rows) - 1)
            def _():
                start(rows, beside)

                @pl.when(jnp.logical_not(is_edge))
                def _():
                    start(rows, far)

                group(rows, partner, me).start()

        return carry

    lax.fori_loop(2, 4, make_row, 0)

    second_chip = jnp.where(is_edge, far, outward)
    fourth_chip = jnp.where(is_edge, last, near)
    for p in range(2):
        for to in (second_chip, fourth_chip, chip):
            chip_piece(p, range(2), to, l_vm[pl.ds(pl.multiple_of(128 * to, 128), 128), :])
        for copy in copies(EARLY[p], partner, me):
            copy.start()

        @pl.when(jnp.logical_not(is_edge))
        def _():
            start(EARLY[p], outward)

    lax.fori_loop(4, ROWS, make_row, 0)

    @pl.when(is_edge)
    def _():
        for rows in LATER:
            start(rows, far)
        for rows in WHOLE:
            start(rows, last)

    for side, dest in ((0, 2 * near + core), (1, 2 * near + 1 - core)):
        for chunk in range(CHUNKS):
            near_refs[side * CHUNKS + chunk][...] = send[dest, :, :, pl.ds(128 * chunk, 128)]

    c = c_vm[...]
    spread = (iota((8 * N, N), 0) // 8 == iota((8 * N, N), 1)).astype(BF16)
    rows = lax.dot_general(spread, c, nt, preferred_element_type=F32)
    widen = (iota((N, 8 * N), 0) == iota((N, 8 * N), 1) // 8).astype(BF16)
    full = jnp.dot(rows.astype(BF16), widen, preferred_element_type=F32)
    l4_ref[...] = jnp.where(iota(wide, 0) % 8 == iota(wide, 1) % 8, full, 0.0).astype(BF16)
    l4n_ref[...] = l4_ref[:, pl.ds(pl.multiple_of(128 * near, 128), 128)]
    eye = (iota((N, N), 0) == iota((N, N), 1)).astype(BF16)
    ct_vm[...] = lax.dot_general(eye, c, nt, preferred_element_type=F32).astype(BF16)
    ct_ref[...] = ct_vm[...]

    def third(src, p, first, second):
        g0 = jnp.dot(ct_vm[...], first, preferred_element_type=F32).reshape(8, 8, COLS)
        g1 = jnp.dot(ct_vm[...], second, preferred_element_type=F32).reshape(8, 8, COLS)
        at = pl.multiple_of(N * src + 8 * p, 16)
        g_ref[:, pl.ds(at, 16), :] = jnp.concatenate([g0, g1], axis=1).astype(BF16)

    def own(t, carry):
        third(me, 2 * t, send[me, 2 * t], send[me, 2 * t + 1])
        return carry

    lax.fori_loop(0, ROWS // 2, own, 0)

    def take(groups, sources):
        for rows in groups:
            for src in sources:
                for copy in copies(rows, src, src):
                    copy.wait_recv()
            if sum(rows) % 2 == 0:
                begin = rows[0] // 2 * 2

                def body(t, carry):
                    for src in sources:
                        p = begin + 2 * t
                        third(src, p, recv[src, p], recv[src, p + 1])
                    return carry

                lax.fori_loop(0, (sum(rows) - begin) // 2, body, 0)

    take(EARLY, [partner])

    @pl.when(jnp.logical_not(is_edge))
    def _():
        g_ref[:, pl.ds(pl.multiple_of(2 * N * near, 16), 2 * N), :] = jnp.zeros((8, 2 * N, COLS), BF16)

    take(EARLY, [2 * beside, 2 * beside + 1])

    for rows in EARLY:
        for copy in copies(rows, partner, me):
            copy.wait_send()
    sent(EARLY, beside)

    @pl.when(is_edge)
    def _():
        take(EARLY, [2 * far, 2 * far + 1])
        take(WHOLE, [2 * last, 2 * last + 1])
        sent(LATER, far)
        sent(WHOLE, last)

    @pl.when(jnp.logical_not(is_edge))
    def _():
        take(LATER, [2 * far, 2 * far + 1])
        sent(EARLY, far)


def most_kernel(g_ref, l4_ref, v_ref):
    for ag in range(8):
        v_ref[ag] = jnp.dot(l4_ref[...], g_ref[ag], preferred_element_type=F32)


def chunk_kernel(chunk, same_ref, other_ref, ct_ref, l4n_ref, most_ref, *refs):
    v_hbm, g_vm, v_vm, v_sem = refs[-4:]
    core = lax.axis_index("dev") % 2
    for side, ref in ((core, same_ref), (1 - core, other_ref)):
        for p in range(0, ROWS, 2):
            both = jnp.concatenate([ref[p], ref[p + 1]], axis=1)
            g = jnp.dot(ct_ref[...], both, preferred_element_type=F32)
            g0 = g[:, :128].reshape(8, 8, 128)
            g1 = g[:, 128:].reshape(8, 8, 128)
            at = pl.multiple_of(N * side + 8 * p, 16)
            g_vm[:, pl.ds(at, 16), :] = jnp.concatenate([g0, g1], axis=1).astype(BF16)

    def put(m):
        part = pl.ds(16 * m, 16)
        return pltpu.make_async_copy(v_vm.at[part], v_hbm.at[part, :, pl.ds(128 * chunk, 128)], v_sem.at[m])

    for m in range(4):
        rows = slice(128 * m, 128 * m + 128)
        for ag in range(0, 8, 2):
            both = jnp.concatenate([g_vm[ag], g_vm[ag + 1]], axis=1)
            part = jnp.dot(l4n_ref[rows, :], both, preferred_element_type=F32)
            for k in range(2):
                most = most_ref[ag + k, rows, 128 * chunk:128 * chunk + 128]
                value = (part[:, 128 * k:128 * k + 128] + most).reshape(16, 8, 128)
                v_vm[16 * m:16 * m + 16, 8 * (ag + k):8 * (ag + k) + 8, :] = value
        put(m).start()
    for m in range(4):
        put(m).wait()


def solution(mesh):
    def local_transform(ao_rows, coeffs):
        vmem = pl.BlockSpec(memory_space=pltpu.VMEM)
        anywhere = pl.BlockSpec(memory_space=pltpu.HBM)
        sds = jax.ShapeDtypeStruct
        outs = (
            sds((8, 8 * N, COLS), BF16),
            sds((8 * N, 8 * N), BF16),
            sds((8 * N, 2 * N), BF16),
            sds((N, N), BF16),
        ) + (sds((ROWS, N, 128), BF16),) * (2 * CHUNKS)
        g, l4, l4n, ct, *near = pl.pallas_call(
            exchange_kernel,
            out_shape=outs,
            in_specs=[anywhere, anywhere],
            out_specs=(vmem,) * len(outs),
            scratch_shapes=[
                pltpu.VMEM((ROWS, N, N, N), BF16),
                pltpu.VMEM((N, N), BF16),
                pltpu.VMEM((8 * N, 8 * N), BF16),
                pltpu.VMEM((4 * N, 4 * N), BF16),
                pltpu.VMEM((N, N), BF16),
                pltpu.VMEM((DEV, ROWS, N, COLS), BF16),
                pltpu.VMEM((DEV, ROWS, N, COLS), BF16),
                pltpu.SemaphoreType.DMA((ROWS + 1,)),
                pltpu.SemaphoreType.DMA,
                pltpu.SemaphoreType.DMA((DEV, ROWS + 1)),
                pltpu.SemaphoreType.DMA((DEV, ROWS + 1)),
            ],
            compiler_params=pltpu.CompilerParams(collective_id=0, has_side_effects=True, vmem_limit_bytes=40 * 2**20),
            name="exchange",
        )(pltpu.with_memory_space_constraint(ao_rows, pltpu.HBM), pltpu.with_memory_space_constraint(coeffs, pltpu.HBM))
        same = [(2, 4), (3, 5), (4, 2), (5, 3)]
        other = [(2, 5), (3, 4), (4, 3), (5, 2)]
        arrived = []
        for chunk in range(CHUNKS):
            pair = []
            for side, perm in enumerate((same, other)):
                pair.append(lax.ppermute(near[side * CHUNKS + chunk], "dev", perm))
            arrived.append(pair)
        most = pl.pallas_call(
            most_kernel,
            out_shape=sds((8, 8 * N, COLS), F32),
            in_specs=[vmem, vmem],
            out_specs=vmem,
            compiler_params=pltpu.CompilerParams(vmem_limit_bytes=12 * 2**20),
            cost_estimate=pl.CostEstimate(flops=2 * 8 * 512**3, bytes_accessed=12 * 2**20, transcendentals=0),
            name="most",
        )(g, l4)
        v = None
        for chunk in range(CHUNKS):
            operands = (*arrived[chunk], ct, l4n, most) + (() if v is None else (v,))
            v = pl.pallas_call(
                functools.partial(chunk_kernel, chunk),
                out_shape=sds((N, N, COLS), F32),
                in_specs=[vmem] * 5 + ([] if v is None else [anywhere]),
                out_specs=anywhere,
                scratch_shapes=[
                    pltpu.VMEM((8, 2 * N, 128), BF16),
                    pltpu.VMEM((N, N, 128), F32),
                    pltpu.SemaphoreType.DMA((4,)),
                ],
                input_output_aliases={} if v is None else {5: 0},
                compiler_params=pltpu.CompilerParams(vmem_limit_bytes=12 * 2**20),
                cost_estimate=pl.CostEstimate(flops=2 * 8 * 512 * 128 * 128, bytes_accessed=4 * 2**20, transcendentals=0),
            )(*operands)
        return v

    return jax.shard_map(local_transform, mesh=mesh, in_specs=(P(('frag', 'dev')), P('frag')), out_specs=P('frag', None, 'dev'), check_vma=False)
```

```python
import functools

import jax
import jax.numpy as jnp
from jax import lax
from jax.experimental import pallas as pl
from jax.experimental.pallas import tpu as pltpu
from jax.sharding import PartitionSpec as P


N = 64
DEV = 8
ROWS = N // DEV
COLS = N * N // DEV
CHUNKS = COLS // 128
EARLY = ((0, 1), (1, 1), (2, 1), (3, 1), (4, 2), (6, 2))
LATER = ((0, 4), (4, 4))
WHOLE = ((0, 8),)
BF16 = jnp.bfloat16
F32 = jnp.float32


def iota(shape, dim):
    return lax.broadcasted_iota(jnp.int32, shape, dim)


def exchange_kernel(a_hbm, c_hbm, g_ref, l4_ref, l4n_ref, ct_ref, *refs):
    near_refs = refs[:2 * CHUNKS]
    a_vm, c_vm, l_vm, b4_vm, ct_vm, send, recv, a_sem, c_sem, send_sem, recv_sem = refs[2 * CHUNKS:]
    me = lax.axis_index("dev")
    chip = me // 2
    core = me % 2

    load_c = pltpu.make_async_copy(c_hbm, c_vm, c_sem)

    def load_row(p):
        return pltpu.make_async_copy(a_hbm.at[p], a_vm.at[p], a_sem.at[p])

    def load_half(h):
        half = pl.ds(32 * h, 32)
        return pltpu.make_async_copy(a_hbm.at[0, half], a_vm.at[0, half], a_sem.at[ROWS * h])

    load_half(0).start()
    load_c.start()

    barrier = pltpu.get_barrier_semaphore()
    for k in range(1, DEV):
        pl.semaphore_signal(barrier, inc=1, device_id={"dev": (me + k) % DEV}, device_id_type=pl.DeviceIdType.MESH)

    load_half(1).start()
    load_c.wait()
    c = c_vm[...]
    nt = (((1,), (1,)), ((), ()))
    wide = (8 * N, 8 * N)

    def kron_rows(first_m, count):
        spread = (iota((8 * count, N), 0) // 8 + first_m == iota((8 * count, N), 1)).astype(BF16)
        rows = lax.dot_general(spread, c, nt, preferred_element_type=F32)
        pair = jnp.concatenate([rows, rows], axis=1)
        tiled = jnp.concatenate([pair] * 4, axis=1)
        shape = (8 * count, 8 * N)
        return jnp.where(iota(shape, 0) % 8 == iota(shape, 1) // N, tiled, 0.0).astype(BF16)

    def group(rows, dest, src):
        part = pl.ds(*rows)
        return pltpu.make_async_remote_copy(
            src_ref=send.at[dest, part],
            dst_ref=recv.at[src, part],
            send_sem=send_sem.at[dest, rows[0]],
            recv_sem=recv_sem.at[src, rows[0]],
            device_id={"dev": dest},
            device_id_type=pl.DeviceIdType.MESH,
        )

    def half(h, dest, src):
        part = pl.ds(32 * h, 32)
        return pltpu.make_async_remote_copy(
            src_ref=send.at[dest, 0, part],
            dst_ref=recv.at[src, 0, part],
            send_sem=send_sem.at[dest, ROWS * h],
            recv_sem=recv_sem.at[src, ROWS * h],
            device_id={"dev": dest},
            device_id_type=pl.DeviceIdType.MESH,
        )

    def copies(rows, dest, src):
        if rows == EARLY[0]:
            return [half(h, dest, src) for h in range(2)]
        return [group(rows, dest, src)]

    def start(rows, to):
        for k in range(2):
            for copy in copies(rows, 2 * to + k, me):
                copy.start()

    def sent(groups, to):
        for rows in groups:
            for k in range(2):
                for copy in copies(rows, 2 * to + k, me):
                    copy.wait_send()

    low = iota((32, 8, 128), 2) < N

    def pieces(p, h, lhs, count, put):
        a = a_vm[p, pl.ds(32 * h, 32)].reshape(4, 8 * N, N)
        left = jnp.concatenate([a[0], a[1]], axis=1)
        right = jnp.concatenate([a[2], a[3]], axis=1)
        a4 = jnp.concatenate([left, right], axis=1)
        t_one = jnp.dot(lhs, a4, preferred_element_type=F32).astype(BF16)
        half = jnp.dot(t_one, b4_vm[...], preferred_element_type=F32)
        pairs = half.reshape(count, 2, 8, 256)
        for t in range(2):
            even = pairs[:, 0, :, 128 * t:128 * t + 128]
            odd = pairs[:, 1, :, 128 * t:128 * t + 128]
            first_rows = jnp.where(low[:count], even, pltpu.roll(odd, N, 2))
            second_rows = jnp.where(low[:count], pltpu.roll(even, N, 2), odd)
            both = jnp.concatenate([first_rows, second_rows], axis=1).astype(BF16)
            for jp in range(count):
                put(jp // 4, pl.ds(32 * h + 16 * t, 16), pl.ds(128 * (jp % 4), 128), both[jp])

    def half_row(p, h):
        def put(dest, q, columns, value):
            send[dest, p, q, columns] = value

        pieces(p, h, l_vm[...], 32, put)

    def chip_piece(p, halves, to, lhs):
        def put(dest, q, columns, value):
            send[2 * to + dest, p, q, columns] = value

        for h in halves:
            pieces(p, h, lhs, 8, put)

    is_edge = jnp.logical_or(chip == 0, chip == 3)
    inward = jnp.where(chip < 2, 1, -1)
    partner = 2 * chip + 1 - core
    near = chip + inward
    far = chip + 2 * inward
    last = chip + 3 * inward
    outward = chip - inward
    beside = jnp.where(is_edge, near, outward)

    first_chip = jnp.where(is_edge, near, far)
    l_vm[:128, :] = kron_rows(16 * first_chip, 16)
    for h in range(2):
        load_half(h).wait()
        if h == 1:
            for later in (1, 2):
                load_row(later).start()
        if h == 0:
            cf = c.astype(F32)
            cpair = jnp.concatenate([cf, cf], axis=1)
            c4 = jnp.concatenate([cpair, cpair], axis=1)
            c44 = jnp.concatenate([c4] * 4, axis=0)
            quad = (4 * N, 4 * N)
            b4_vm[...] = jnp.where(iota(quad, 0) // N == iota(quad, 1) // N, c44, 0.0).astype(BF16)
        chip_piece(0, (h,), first_chip, l_vm[:128, :])
        if h == 0:
            pl.semaphore_wait(barrier, DEV - 1)
        for k in range(2):
            half(h, 2 * first_chip + k, me).start()
    load_row(1).wait()
    load_row(3).start()
    chip_piece(1, range(2), first_chip, l_vm[:128, :])
    start(EARLY[1], first_chip)

    l_vm[...] = kron_rows(0, N)
    second_chip = jnp.where(is_edge, far, outward)
    fourth_chip = jnp.where(is_edge, last, near)

    def other_piece(i, carry):
        to = jnp.where(i % 3 == 0, second_chip, jnp.where(i % 3 == 1, fourth_chip, chip))
        chip_piece(i // 3, range(2), to, l_vm[pl.ds(pl.multiple_of(128 * to, 128), 128), :])
        return carry

    def make_row(p, carry):
        @pl.when(p == 4)
        def _():
            lax.fori_loop(0, 6, other_piece, 0)
            for rows in EARLY[:2]:
                for copy in copies(rows, partner, me):
                    copy.start()

                @pl.when(jnp.logical_not(is_edge))
                def _():
                    start(rows, outward)

        load_row(p).wait()

        @pl.when(p < ROWS - 2)
        def _():
            load_row(p + 2).start()

        for h in range(2):
            half_row(p, h)
        for rows in EARLY[2:]:
            @pl.when(p == sum(rows) - 1)
            def _():
                start(rows, beside)

                @pl.when(jnp.logical_not(is_edge))
                def _():
                    start(rows, far)

                group(rows, partner, me).start()

        return carry

    lax.fori_loop(2, ROWS, make_row, 0)

    @pl.when(is_edge)
    def _():
        for rows in LATER:
            start(rows, far)
        for rows in WHOLE:
            start(rows, last)

    for side, dest in ((0, 2 * near + core), (1, 2 * near + 1 - core)):
        for chunk in range(CHUNKS):
            near_refs[side * CHUNKS + chunk][...] = send[dest, :, :, pl.ds(128 * chunk, 128)]

    c = c_vm[...]
    spread = (iota((8 * N, N), 0) // 8 == iota((8 * N, N), 1)).astype(BF16)
    rows = lax.dot_general(spread, c, nt, preferred_element_type=F32)
    widen = (iota((N, 8 * N), 0) == iota((N, 8 * N), 1) // 8).astype(BF16)
    full = jnp.dot(rows.astype(BF16), widen, preferred_element_type=F32)
    l4_ref[...] = jnp.where(iota(wide, 0) % 8 == iota(wide, 1) % 8, full, 0.0).astype(BF16)
    l4n_ref[...] = l4_ref[:, pl.ds(pl.multiple_of(128 * near, 128), 128)]
    eye = (iota((N, N), 0) == iota((N, N), 1)).astype(BF16)
    ct_vm[...] = lax.dot_general(eye, c, nt, preferred_element_type=F32).astype(BF16)
    ct_ref[...] = ct_vm[...]

    def third(src, p, first, second):
        g0 = jnp.dot(ct_vm[...], first, preferred_element_type=F32).reshape(8, 8, COLS)
        g1 = jnp.dot(ct_vm[...], second, preferred_element_type=F32).reshape(8, 8, COLS)
        at = pl.multiple_of(N * src + 8 * p, 16)
        g_ref[:, pl.ds(at, 16), :] = jnp.concatenate([g0, g1], axis=1).astype(BF16)

    def own(t, carry):
        third(me, 2 * t, send[me, 2 * t], send[me, 2 * t + 1])
        return carry

    lax.fori_loop(0, ROWS // 2, own, 0)

    def take(groups, sources):
        for rows in groups:
            for src in sources:
                for copy in copies(rows, src, src):
                    copy.wait_recv()
            if sum(rows) % 2 == 0:
                begin = rows[0] // 2 * 2

                def body(t, carry):
                    for src in sources:
                        p = begin + 2 * t
                        third(src, p, recv[src, p], recv[src, p + 1])
                    return carry

                lax.fori_loop(0, (sum(rows) - begin) // 2, body, 0)

    take(EARLY, [partner])

    @pl.when(jnp.logical_not(is_edge))
    def _():
        g_ref[:, pl.ds(pl.multiple_of(2 * N * near, 16), 2 * N), :] = jnp.zeros((8, 2 * N, COLS), BF16)

    take(EARLY, [2 * beside, 2 * beside + 1])

    for rows in EARLY:
        for copy in copies(rows, partner, me):
            copy.wait_send()
    sent(EARLY, beside)

    @pl.when(is_edge)
    def _():
        take(EARLY, [2 * far, 2 * far + 1])
        take(WHOLE, [2 * last, 2 * last + 1])
        sent(LATER, far)
        sent(WHOLE, last)

    @pl.when(jnp.logical_not(is_edge))
    def _():
        take(LATER, [2 * far, 2 * far + 1])
        sent(EARLY, far)


def most_kernel(g_ref, l4_ref, v_ref):
    for ag in range(8):
        v_ref[ag] = jnp.dot(l4_ref[...], g_ref[ag], preferred_element_type=F32)


def chunk_kernel(chunk, same_ref, other_ref, ct_ref, l4n_ref, most_ref, *refs):
    v_hbm, g_vm, v_vm, v_sem = refs[-4:]
    core = lax.axis_index("dev") % 2
    for side, ref in ((core, same_ref), (1 - core, other_ref)):
        for p in range(0, ROWS, 2):
            both = jnp.concatenate([ref[p], ref[p + 1]], axis=1)
            g = jnp.dot(ct_ref[...], both, preferred_element_type=F32)
            g0 = g[:, :128].reshape(8, 8, 128)
            g1 = g[:, 128:].reshape(8, 8, 128)
            at = pl.multiple_of(N * side + 8 * p, 16)
            g_vm[:, pl.ds(at, 16), :] = jnp.concatenate([g0, g1], axis=1).astype(BF16)

    def put(m):
        part = pl.ds(8 * m, 8)
        return pltpu.make_async_copy(v_vm.at[part], v_hbm.at[part, :, pl.ds(128 * chunk, 128)], v_sem.at[m])

    for m in range(4):
        rows = slice(128 * m, 128 * m + 128)
        for ag in range(0, 8, 2):
            both = jnp.concatenate([g_vm[ag], g_vm[ag + 1]], axis=1)
            part = jnp.dot(l4n_ref[rows, :], both, preferred_element_type=F32)
            for k in range(2):
                most = most_ref[ag + k, rows, 128 * chunk:128 * chunk + 128]
                value = (part[:, 128 * k:128 * k + 128] + most).reshape(16, 8, 128)
                v_vm[16 * m:16 * m + 16, 8 * (ag + k):8 * (ag + k) + 8, :] = value
        put(2 * m).start()
        put(2 * m + 1).start()
    for m in range(8):
        put(m).wait()


def solution(mesh):
    def local_transform(ao_rows, coeffs):
        vmem = pl.BlockSpec(memory_space=pltpu.VMEM)
        anywhere = pl.BlockSpec(memory_space=pltpu.HBM)
        sds = jax.ShapeDtypeStruct
        outs = (
            sds((8, 8 * N, COLS), BF16),
            sds((8 * N, 8 * N), BF16),
            sds((8 * N, 2 * N), BF16),
            sds((N, N), BF16),
        ) + (sds((ROWS, N, 128), BF16),) * (2 * CHUNKS)
        g, l4, l4n, ct, *near = pl.pallas_call(
            exchange_kernel,
            out_shape=outs,
            in_specs=[anywhere, anywhere],
            out_specs=(vmem,) * len(outs),
            scratch_shapes=[
                pltpu.VMEM((ROWS, N, N, N), BF16),
                pltpu.VMEM((N, N), BF16),
                pltpu.VMEM((8 * N, 8 * N), BF16),
                pltpu.VMEM((4 * N, 4 * N), BF16),
                pltpu.VMEM((N, N), BF16),
                pltpu.VMEM((DEV, ROWS, N, COLS), BF16),
                pltpu.VMEM((DEV, ROWS, N, COLS), BF16),
                pltpu.SemaphoreType.DMA((ROWS + 1,)),
                pltpu.SemaphoreType.DMA,
                pltpu.SemaphoreType.DMA((DEV, ROWS + 1)),
                pltpu.SemaphoreType.DMA((DEV, ROWS + 1)),
            ],
            compiler_params=pltpu.CompilerParams(collective_id=0, has_side_effects=True, vmem_limit_bytes=40 * 2**20),
            name="exchange",
        )(pltpu.with_memory_space_constraint(ao_rows, pltpu.HBM), pltpu.with_memory_space_constraint(coeffs, pltpu.HBM))
        same = [(2, 4), (3, 5), (4, 2), (5, 3)]
        other = [(2, 5), (3, 4), (4, 3), (5, 2)]
        arrived = []
        for chunk in range(CHUNKS):
            pair = []
            for side, perm in enumerate((same, other)):
                pair.append(lax.ppermute(near[side * CHUNKS + chunk], "dev", perm))
            arrived.append(pair)
        most = pl.pallas_call(
            most_kernel,
            out_shape=sds((8, 8 * N, COLS), F32),
            in_specs=[vmem, vmem],
            out_specs=vmem,
            compiler_params=pltpu.CompilerParams(vmem_limit_bytes=12 * 2**20),
            cost_estimate=pl.CostEstimate(flops=2 * 8 * 512**3, bytes_accessed=12 * 2**20, transcendentals=0),
            name="most",
        )(g, l4)
        v = None
        for chunk in range(CHUNKS):
            operands = (*arrived[chunk], ct, l4n, most) + (() if v is None else (v,))
            v = pl.pallas_call(
                functools.partial(chunk_kernel, chunk),
                out_shape=sds((N, N, COLS), F32),
                in_specs=[vmem] * 5 + ([] if v is None else [anywhere]),
                out_specs=anywhere,
                scratch_shapes=[
                    pltpu.VMEM((8, 2 * N, 128), BF16),
                    pltpu.VMEM((N, N, 128), F32),
                    pltpu.SemaphoreType.DMA((8,)),
                ],
                input_output_aliases={} if v is None else {5: 0},
                compiler_params=pltpu.CompilerParams(vmem_limit_bytes=12 * 2**20),
                cost_estimate=pl.CostEstimate(flops=2 * 8 * 512 * 128 * 128, bytes_accessed=4 * 2**20, transcendentals=0),
            )(*operands)
        return v

    return jax.shard_map(local_transform, mesh=mesh, in_specs=(P(('frag', 'dev')), P('frag')), out_specs=P('frag', None, 'dev'), check_vma=False)
```

```python
import functools

import jax
import jax.numpy as jnp
from jax import lax
from jax.experimental import pallas as pl
from jax.experimental.pallas import tpu as pltpu
from jax.sharding import PartitionSpec as P


N = 64
DEV = 8
ROWS = N // DEV
COLS = N * N // DEV
CHUNKS = COLS // 128
EARLY = ((0, 1), (1, 1), (2, 1), (3, 1), (4, 2), (6, 2))
LATER = ((0, 4), (4, 4))
WHOLE = ((0, 8),)
BF16 = jnp.bfloat16
F32 = jnp.float32


def iota(shape, dim):
    return lax.broadcasted_iota(jnp.int32, shape, dim)


def exchange_kernel(a_hbm, c_hbm, g_ref, l4_ref, l4n_ref, ct_ref, *refs):
    near_refs = refs[:2 * CHUNKS]
    a_vm, c_vm, l_vm, b4_vm, ct_vm, send, recv, a_sem, c_sem, send_sem, recv_sem = refs[2 * CHUNKS:]
    me = lax.axis_index("dev")
    chip = me // 2
    core = me % 2

    load_c = pltpu.make_async_copy(c_hbm, c_vm, c_sem)

    def load_row(p):
        return pltpu.make_async_copy(a_hbm.at[p], a_vm.at[p], a_sem.at[p])

    def load_half(h):
        half = pl.ds(32 * h, 32)
        return pltpu.make_async_copy(a_hbm.at[0, half], a_vm.at[0, half], a_sem.at[ROWS * h])

    load_half(0).start()
    load_c.start()

    barrier = pltpu.get_barrier_semaphore()
    for k in range(1, DEV):
        pl.semaphore_signal(barrier, inc=1, device_id={"dev": (me + k) % DEV}, device_id_type=pl.DeviceIdType.MESH)

    load_half(1).start()
    load_c.wait()
    c = c_vm[...]
    nt = (((1,), (1,)), ((), ()))
    wide = (8 * N, 8 * N)

    def kron_rows(first_m, count):
        spread = (iota((8 * count, N), 0) // 8 + first_m == iota((8 * count, N), 1)).astype(BF16)
        rows = lax.dot_general(spread, c, nt, preferred_element_type=F32)
        pair = jnp.concatenate([rows, rows], axis=1)
        tiled = jnp.concatenate([pair] * 4, axis=1)
        shape = (8 * count, 8 * N)
        return jnp.where(iota(shape, 0) % 8 == iota(shape, 1) // N, tiled, 0.0).astype(BF16)

    def group(rows, dest, src):
        part = pl.ds(*rows)
        return pltpu.make_async_remote_copy(
            src_ref=send.at[dest, part],
            dst_ref=recv.at[src, part],
            send_sem=send_sem.at[dest, rows[0]],
            recv_sem=recv_sem.at[src, rows[0]],
            device_id={"dev": dest},
            device_id_type=pl.DeviceIdType.MESH,
        )

    def half(h, dest, src):
        part = pl.ds(32 * h, 32)
        return pltpu.make_async_remote_copy(
            src_ref=send.at[dest, 0, part],
            dst_ref=recv.at[src, 0, part],
            send_sem=send_sem.at[dest, ROWS * h],
            recv_sem=recv_sem.at[src, ROWS * h],
            device_id={"dev": dest},
            device_id_type=pl.DeviceIdType.MESH,
        )

    def copies(rows, dest, src):
        if rows == EARLY[0]:
            return [half(h, dest, src) for h in range(2)]
        return [group(rows, dest, src)]

    def start(rows, to):
        for k in range(2):
            for copy in copies(rows, 2 * to + k, me):
                copy.start()

    def sent(groups, to):
        for rows in groups:
            for k in range(2):
                for copy in copies(rows, 2 * to + k, me):
                    copy.wait_send()

    low = iota((32, 8, 128), 2) < N

    def pieces(p, h, lhs, count, put):
        a = a_vm[p, pl.ds(32 * h, 32)].reshape(4, 8 * N, N)
        left = jnp.concatenate([a[0], a[1]], axis=1)
        right = jnp.concatenate([a[2], a[3]], axis=1)
        a4 = jnp.concatenate([left, right], axis=1)
        t_one = jnp.dot(lhs, a4, preferred_element_type=F32).astype(BF16)
        half = jnp.dot(t_one, b4_vm[...], preferred_element_type=F32)
        pairs = half.reshape(count, 2, 8, 256)
        for t in range(2):
            even = pairs[:, 0, :, 128 * t:128 * t + 128]
            odd = pairs[:, 1, :, 128 * t:128 * t + 128]
            first_rows = jnp.where(low[:count], even, pltpu.roll(odd, N, 2))
            second_rows = jnp.where(low[:count], pltpu.roll(even, N, 2), odd)
            both = jnp.concatenate([first_rows, second_rows], axis=1).astype(BF16)
            for jp in range(count):
                put(jp // 4, pl.ds(32 * h + 16 * t, 16), pl.ds(128 * (jp % 4), 128), both[jp])

    def half_row(p, h):
        def put(dest, q, columns, value):
            send[dest, p, q, columns] = value

        pieces(p, h, l_vm[...], 32, put)

    def chip_piece(p, halves, to, lhs):
        def put(dest, q, columns, value):
            send[2 * to + dest, p, q, columns] = value

        for h in halves:
            pieces(p, h, lhs, 8, put)

    is_edge = jnp.logical_or(chip == 0, chip == 3)
    inward = jnp.where(chip < 2, 1, -1)
    partner = 2 * chip + 1 - core
    near = chip + inward
    far = chip + 2 * inward
    last = chip + 3 * inward
    outward = chip - inward
    beside = jnp.where(is_edge, near, outward)

    first_chip = jnp.where(is_edge, near, far)
    l_vm[:128, :] = kron_rows(16 * first_chip, 16)
    for h in range(2):
        load_half(h).wait()
        if h == 1:
            for later in (1, 2):
                load_row(later).start()
        if h == 0:
            cf = c.astype(F32)
            cpair = jnp.concatenate([cf, cf], axis=1)
            c4 = jnp.concatenate([cpair, cpair], axis=1)
            c44 = jnp.concatenate([c4] * 4, axis=0)
            quad = (4 * N, 4 * N)
            b4_vm[...] = jnp.where(iota(quad, 0) // N == iota(quad, 1) // N, c44, 0.0).astype(BF16)
        chip_piece(0, (h,), first_chip, l_vm[:128, :])
        if h == 0:
            pl.semaphore_wait(barrier, DEV - 1)
        for k in range(2):
            half(h, 2 * first_chip + k, me).start()
    load_row(1).wait()
    load_row(3).start()
    chip_piece(1, range(2), first_chip, l_vm[:128, :])
    start(EARLY[1], first_chip)

    l_vm[...] = kron_rows(0, N)
    second_chip = jnp.where(is_edge, far, outward)
    fourth_chip = jnp.where(is_edge, last, near)

    def other_piece(i, carry):
        to = jnp.where(i % 3 == 0, second_chip, jnp.where(i % 3 == 1, fourth_chip, chip))
        chip_piece(i // 3, range(2), to, l_vm[pl.ds(pl.multiple_of(128 * to, 128), 128), :])
        return carry

    def make_row(p, carry):
        @pl.when(p == 4)
        def _():
            lax.fori_loop(0, 6, other_piece, 0)
            for rows in EARLY[:2]:
                for copy in copies(rows, partner, me):
                    copy.start()

                @pl.when(jnp.logical_not(is_edge))
                def _():
                    start(rows, outward)

        load_row(p).wait()

        @pl.when(p < ROWS - 2)
        def _():
            load_row(p + 2).start()

        for h in range(2):
            half_row(p, h)
        for rows in EARLY[2:]:
            @pl.when(p == sum(rows) - 1)
            def _():
                start(rows, beside)

                @pl.when(jnp.logical_not(is_edge))
                def _():
                    start(rows, far)

                group(rows, partner, me).start()

        return carry

    lax.fori_loop(2, ROWS, make_row, 0)

    @pl.when(is_edge)
    def _():
        for rows in LATER:
            start(rows, far)
        for rows in WHOLE:
            start(rows, last)

    for side, dest in ((0, 2 * near + core), (1, 2 * near + 1 - core)):
        for chunk in range(CHUNKS):
            near_refs[side * CHUNKS + chunk][...] = send[dest, :, :, pl.ds(128 * chunk, 128)]

    c = c_vm[...]
    spread = (iota((8 * N, N), 0) // 8 == iota((8 * N, N), 1)).astype(BF16)
    rows = lax.dot_general(spread, c, nt, preferred_element_type=F32)
    widen = (iota((N, 8 * N), 0) == iota((N, 8 * N), 1) // 8).astype(BF16)
    full = jnp.dot(rows.astype(BF16), widen, preferred_element_type=F32)
    l4_ref[...] = jnp.where(iota(wide, 0) % 8 == iota(wide, 1) % 8, full, 0.0).astype(BF16)
    l4n_ref[...] = l4_ref[:, pl.ds(pl.multiple_of(128 * near, 128), 128)]
    eye = (iota((N, N), 0) == iota((N, N), 1)).astype(BF16)
    ct_vm[...] = lax.dot_general(eye, c, nt, preferred_element_type=F32).astype(BF16)
    ct_ref[...] = ct_vm[...]

    def third(src, p, first, second):
        g0 = jnp.dot(ct_vm[...], first, preferred_element_type=F32).reshape(8, 8, COLS)
        g1 = jnp.dot(ct_vm[...], second, preferred_element_type=F32).reshape(8, 8, COLS)
        at = pl.multiple_of(N * src + 8 * p, 16)
        g_ref[:, pl.ds(at, 16), :] = jnp.concatenate([g0, g1], axis=1).astype(BF16)

    def own(t, carry):
        third(me, 2 * t, send[me, 2 * t], send[me, 2 * t + 1])
        return carry

    lax.fori_loop(0, ROWS // 2, own, 0)

    def take(groups, sources):
        for rows in groups:
            for src in sources:
                for copy in copies(rows, src, src):
                    copy.wait_recv()
            if sum(rows) % 2 == 0:
                begin = rows[0] // 2 * 2

                def body(t, carry):
                    for src in sources:
                        p = begin + 2 * t
                        third(src, p, recv[src, p], recv[src, p + 1])
                    return carry

                lax.fori_loop(0, (sum(rows) - begin) // 2, body, 0)

    take(EARLY, [partner])

    @pl.when(jnp.logical_not(is_edge))
    def _():
        g_ref[:, pl.ds(pl.multiple_of(2 * N * near, 16), 2 * N), :] = jnp.zeros((8, 2 * N, COLS), BF16)

    take(EARLY, [2 * beside, 2 * beside + 1])

    for rows in EARLY:
        for copy in copies(rows, partner, me):
            copy.wait_send()
    sent(EARLY, beside)

    @pl.when(is_edge)
    def _():
        take(EARLY, [2 * far, 2 * far + 1])
        take(WHOLE, [2 * last, 2 * last + 1])
        sent(LATER, far)
        sent(WHOLE, last)

    @pl.when(jnp.logical_not(is_edge))
    def _():
        take(LATER, [2 * far, 2 * far + 1])
        sent(EARLY, far)


def most_kernel(g_ref, l4_ref, v_ref):
    for ag in range(8):
        v_ref[ag] = jnp.dot(l4_ref[...], g_ref[ag], preferred_element_type=F32)


def chunk_kernel(chunk, same_ref, other_ref, ct_ref, l4n_ref, most_ref, *refs):
    v_hbm, g_vm, v_vm, v_sem = refs[-4:]
    core = lax.axis_index("dev") % 2
    for side, ref in ((core, same_ref), (1 - core, other_ref)):
        for p in range(0, ROWS, 2):
            both = jnp.concatenate([ref[p], ref[p + 1]], axis=1)
            g = jnp.dot(ct_ref[...], both, preferred_element_type=F32)
            g0 = g[:, :128].reshape(8, 8, 128)
            g1 = g[:, 128:].reshape(8, 8, 128)
            at = pl.multiple_of(N * side + 8 * p, 16)
            g_vm[:, pl.ds(at, 16), :] = jnp.concatenate([g0, g1], axis=1).astype(BF16)

    def put(m):
        part = pl.ds(16 * m, 16)
        return pltpu.make_async_copy(v_vm.at[part], v_hbm.at[part, :, pl.ds(128 * chunk, 128)], v_sem.at[m])

    for m in range(4):
        rows = slice(128 * m, 128 * m + 128)
        for ag in range(0, 8, 2):
            both = jnp.concatenate([g_vm[ag], g_vm[ag + 1]], axis=1)
            part = jnp.dot(l4n_ref[rows, :], both, preferred_element_type=F32)
            for k in range(2):
                most = most_ref[ag + k, rows, 128 * chunk:128 * chunk + 128]
                value = (part[:, 128 * k:128 * k + 128] + most).reshape(16, 8, 128)
                v_vm[16 * m:16 * m + 16, 8 * (ag + k):8 * (ag + k) + 8, :] = value
        put(m).start()
    for m in range(4):
        put(m).wait()


def solution(mesh):
    def local_transform(ao_rows, coeffs):
        vmem = pl.BlockSpec(memory_space=pltpu.VMEM)
        anywhere = pl.BlockSpec(memory_space=pltpu.HBM)
        sds = jax.ShapeDtypeStruct
        outs = (
            sds((8, 8 * N, COLS), BF16),
            sds((8 * N, 8 * N), BF16),
            sds((8 * N, 2 * N), BF16),
            sds((N, N), BF16),
        ) + (sds((ROWS, N, 128), BF16),) * (2 * CHUNKS)
        g, l4, l4n, ct, *near = pl.pallas_call(
            exchange_kernel,
            out_shape=outs,
            in_specs=[anywhere, anywhere],
            out_specs=(vmem,) * len(outs),
            scratch_shapes=[
                pltpu.VMEM((ROWS, N, N, N), BF16),
                pltpu.VMEM((N, N), BF16),
                pltpu.VMEM((8 * N, 8 * N), BF16),
                pltpu.VMEM((4 * N, 4 * N), BF16),
                pltpu.VMEM((N, N), BF16),
                pltpu.VMEM((DEV, ROWS, N, COLS), BF16),
                pltpu.VMEM((DEV, ROWS, N, COLS), BF16),
                pltpu.SemaphoreType.DMA((ROWS + 1,)),
                pltpu.SemaphoreType.DMA,
                pltpu.SemaphoreType.DMA((DEV, ROWS + 1)),
                pltpu.SemaphoreType.DMA((DEV, ROWS + 1)),
            ],
            compiler_params=pltpu.CompilerParams(collective_id=0, has_side_effects=True, vmem_limit_bytes=40 * 2**20),
            name="exchange",
        )(pltpu.with_memory_space_constraint(ao_rows, pltpu.HBM), pltpu.with_memory_space_constraint(coeffs, pltpu.HBM))
        same = [(2, 4), (3, 5), (4, 2), (5, 3)]
        other = [(2, 5), (3, 4), (4, 3), (5, 2)]
        arrived = []
        for chunk in range(CHUNKS):
            pair = []
            for side, perm in enumerate((same, other)):
                pair.append(lax.ppermute(near[side * CHUNKS + chunk], "dev", perm))
            arrived.append(pair)
        most = pl.pallas_call(
            most_kernel,
            out_shape=sds((8, 8 * N, COLS), F32),
            in_specs=[vmem, vmem],
            out_specs=vmem,
            compiler_params=pltpu.CompilerParams(vmem_limit_bytes=12 * 2**20),
            cost_estimate=pl.CostEstimate(flops=2 * 8 * 512**3, bytes_accessed=12 * 2**20, transcendentals=0),
            name="most",
        )(g, l4)
        v = None
        for chunk in range(CHUNKS):
            operands = (*arrived[chunk], ct, l4n, most) + (() if v is None else (v,))
            v = pl.pallas_call(
                functools.partial(chunk_kernel, chunk),
                out_shape=sds((N, N, COLS), F32),
                in_specs=[vmem] * 5 + ([] if v is None else [anywhere]),
                out_specs=anywhere,
                scratch_shapes=[
                    pltpu.VMEM((8, 2 * N, 128), BF16),
                    pltpu.VMEM((N, N, 128), F32),
                    pltpu.SemaphoreType.DMA((4,)),
                ],
                input_output_aliases={} if v is None else {5: 0},
                compiler_params=pltpu.CompilerParams(vmem_limit_bytes=12 * 2**20),
                cost_estimate=pl.CostEstimate(flops=2 * 8 * 512 * 128 * 128, bytes_accessed=4 * 2**20, transcendentals=0),
            )(*operands)
        return v

    return jax.shard_map(local_transform, mesh=mesh, in_specs=(P(('frag', 'dev')), P('frag')), out_specs=P('frag', None, 'dev'), check_vma=False)
```
